256 devices in a mesh: rep: 1, dp: 256 (over x, y, z, core).
Axes of the slice: x: 4, y: 4, z: 8, core: 2. Of those that a mesh axis runs over, the one named last changes fastest.
Arguments:
- x: bfloat16 [256, 2048, 768], P(('rep', 'dp'))
- dy: bfloat16 [256, 2048, 768], P(('rep', 'dp'))
- wq: bfloat16 [1, 768, 768], P(None, 'dp')
- wk: bfloat16 [1, 768, 128], P(None, 'dp')
- wv: bfloat16 [1, 768, 128], P(None, 'dp')
- wo: bfloat16 [1, 768, 768], P(None, 'dp')
- w_gate: bfloat16 [1, 768, 2048], P(None, 'dp')
- w_up: bfloat16 [1, 768, 2048], P(None, 'dp')
- w_down: bfloat16 [1, 2048, 768], P(None, 'dp')
Outputs:
- output 1: bfloat16 [256, 2048, 768], P(('rep', 'dp'))
- output 2: bfloat16 [1, 768, 768], P('rep', 'dp')
- output 3: bfloat16 [1, 768, 128], P('rep', 'dp')
- output 4: bfloat16 [1, 768, 128], P('rep', 'dp')
- output 5: bfloat16 [1, 768, 768], P('rep', 'dp')
- output 6: bfloat16 [1, 768, 2048], P('rep', 'dp')
- output 7: bfloat16 [1, 768, 2048], P('rep', 'dp')
- output 8: bfloat16 [1, 2048, 768], P('rep', 'dp')
All inputs are finite; a program needn't handle non-finite values.
Results may differ from the reference program's by a relative error of at most 0.024.
Values are sent between devices in bfloat16 or wider.
A program may use at most 768 MiB of HBM per device.

```python
import jax
import jax.numpy as jnp
from jax import lax

SEQUENCES = 256
TOKENS = 2048
D = 768
HEADS = 6
KV_HEADS = 1
HEAD = 128
FF = 2048
LAYERS = 1
THETA = 10000
NAMES = ("wq", "wk", "wv", "wo", "w_gate", "w_up", "w_down")
SHAPES = {
    "wq": (LAYERS, D, HEADS * HEAD),
    "wk": (LAYERS, D, KV_HEADS * HEAD),
    "wv": (LAYERS, D, KV_HEADS * HEAD),
    "wo": (LAYERS, HEADS * HEAD, D),
    "w_gate": (LAYERS, D, FF),
    "w_up": (LAYERS, D, FF),
    "w_down": (LAYERS, FF, D),
}


def bump(key, n, height):
    away = (jnp.arange(n, dtype=jnp.int32) - jax.random.randint(key, (), 0, n, jnp.int32)) % n
    return jnp.where(away < n // 8, height, 1.0)


def together(key, own, strength):
    shared = jax.random.normal(key, own.shape[1:], jnp.float32)
    return (own + strength * shared) * lax.rsqrt(1 + strength * strength)


def setup_inputs(seed: int = 0, part: int = 0) -> dict:
    kx, kdy, ka, kb, kz, kf, kh, kl, *keys = jax.random.split(jax.random.key(seed), 8 + 3 * len(NAMES))
    kx, kdy, ka, kb = (jax.random.fold_in(k, part) for k in (kx, kdy, ka, kb))
    kw, km, kv = (keys[i::3] for i in range(3))
    shape = (SEQUENCES, TOKENS, D)
    much_x, much_dy = jax.random.uniform(kz, (2,), jnp.float32, 0.0, 1.0)
    loud = 2.0 ** jax.random.uniform(jax.random.fold_in(kz, 1), (), jnp.float32, -1.0, 2.0)
    layers = 2.0 ** jax.random.uniform(kl, (LAYERS, 1, 1), jnp.float32, -1.0, 1.0)
    times = {"wq": 1.0, "wk": 1.0, "wv": 2.0, "wo": layers, "w_gate": 1.0, "w_up": bump(kh, FF, 4.0), "w_down": layers}
    x = together(ka, jax.random.normal(kx, shape, jnp.float32), much_x) * bump(kf, D, 4.0)
    dy = together(kb, jax.random.normal(kdy, shape, jnp.float32), much_dy)
    drawn = {"x": x.astype(jnp.bfloat16), "dy": (loud * dy * (SEQUENCES * TOKENS) ** -0.5).astype(jnp.bfloat16)}
    for key, name in zip(kw, NAMES, strict=True):
        drawn[name] = (jax.random.normal(key, SHAPES[name], jnp.float32) * SHAPES[name][1] ** -0.5 * times[name]).astype(jnp.bfloat16)
    return drawn


def matmul(a, w):
    return jnp.dot(a, w, preferred_element_type=jnp.float32).astype(jnp.bfloat16)


def normed(h):
    wide = h.astype(jnp.float32)
    scale = lax.rsqrt(jnp.mean(wide**2, -1, keepdims=True) + 1e-6)
    return (wide * scale).astype(jnp.bfloat16)


def turned(t, theta):
    half = t.shape[-1] // 2
    angle = jnp.arange(t.shape[0], dtype=jnp.float32)[:, None] * theta ** (-jnp.arange(half, dtype=jnp.float32) / half)
    cos, sin = jnp.cos(angle)[:, None], jnp.sin(angle)[:, None]
    a, b = t[..., :half].astype(jnp.float32), t[..., half:].astype(jnp.float32)
    return jnp.concatenate([a * cos - b * sin, b * cos + a * sin], -1).astype(jnp.bfloat16)


def seen_by(q, k, v):
    tokens, kv = q.shape[0], k.shape[1]
    q = q.reshape(tokens, kv, -1, q.shape[-1])
    scores = jnp.einsum("tgsd,ugd->gstu", q.astype(jnp.float32), k.astype(jnp.float32)) * q.shape[-1] ** -0.5
    place = jnp.arange(tokens)
    weights = jax.nn.softmax(jnp.where(place[:, None] >= place, scores, -jnp.inf), -1).astype(jnp.bfloat16)
    return jnp.einsum("gstu,ugd->tgsd", weights.astype(jnp.float32), v.astype(jnp.float32)).astype(jnp.bfloat16).reshape(tokens, -1)


def layer(h, w):
    a = normed(h)
    q, k = (turned(matmul(a, w[name]).reshape(h.shape[0], -1, HEAD), THETA) for name in ("wq", "wk"))
    h = h + matmul(seen_by(q, k, matmul(a, w["wv"]).reshape(h.shape[0], -1, HEAD)), w["wo"])
    b = normed(h)
    gate = jnp.dot(b, w["w_gate"], preferred_element_type=jnp.float32)
    up = jnp.dot(b, w["w_up"], preferred_element_type=jnp.float32)
    return h + matmul((jax.nn.silu(gate) * up).astype(jnp.bfloat16), w["w_down"])


def stack(weights, h):
    return lax.scan(lambda h, w: (layer(h, w), None), h, weights)[0]


def reference(x, dy, wq, wk, wv, wo, w_gate, w_up, w_down):
    weights = dict(zip(NAMES, (wq, wk, wv, wo, w_gate, w_up, w_down), strict=True))

    def take(so_far, sequence):
        h, by_y = sequence
        _, back = jax.vjp(stack, weights, h)
        by_weights, by_h = back(by_y)
        return jax.tree.map(lambda total, term: total + term.astype(jnp.float32), so_far, by_weights), by_h

    none_yet = {name: jnp.zeros(w.shape, jnp.float32) for name, w in weights.items()}
    by_weights, by_x = lax.scan(take, none_yet, (x, dy))
    return (by_x, *(by_weights[name].astype(jnp.bfloat16) for name in NAMES))
```

```python
import functools

import jax
import jax.numpy as jnp
import numpy as np
from jax import lax
from jax.experimental import pallas as pl
from jax.experimental.pallas import tpu as pltpu
from jax.sharding import PartitionSpec as P


F32, BF = jnp.float32, jnp.bfloat16
X, Y, Z, C = 4, 4, 8, 2
LINE = Z * C
DMA = pltpu.SemaphoreType.DMA


def place():
    me = lax.axis_index("dp")
    return me // (LINE * Y), lax.rem(me // LINE, Y), lax.rem(me, LINE), lax.rem(me, C)


def device(x, y, slot):
    return {"dp": (x * Y + y) * LINE + slot}


def on(a, k, n=4):
    return lax.rem(a + k, n)


def remote(src, dst, sems, where):
    send, recv = sems
    return pltpu.make_async_remote_copy(src_ref=src, dst_ref=dst, send_sem=send, recv_sem=recv, device_id=where, device_id_type=pl.DeviceIdType.MESH)


def start(copies):
    for cp in copies:
        cp.start()


def landed(copies):
    for cp in copies:
        cp.wait_recv()


def left(copies):
    for cp in copies:
        cp.wait_send()


def greet():
    x, y, slot, _ = place()
    who = [device(x, y, on(slot, k, LINE)) for k in range(1, LINE)]
    for k in (1, 3):
        who += [device(on(x, k), y, slot), device(x, on(y, k), slot)]
    barrier = pltpu.get_barrier_semaphore()
    for d in who:
        pl.semaphore_signal(barrier, inc=1, device_id=d, device_id_type=pl.DeviceIdType.MESH)
    pl.semaphore_wait(barrier, len(who))


def cols(first, size):
    return pl.ds(pl.multiple_of(first, 128), size)


def pair(sems, *index):
    return sems[0].at[index], sems[1].at[index]


class Ring:
    def __init__(self, along_x):
        x, y, slot, c = place()
        self.at = x if along_x else y
        self.to = lambda k: device(on(x, k), y, slot) if along_x else device(x, on(y, k), slot)


class Gather:
    def __init__(self, arrays, pieces):
        self.arrays, self.pieces = arrays, pieces

    def scratch(self):
        A, P = len(self.arrays), len(self.pieces)
        both = lambda *s: [DMA(s), DMA(s)]
        wide = [n if whole else n // 2 for _, n, _, whole in self.arrays]
        return dict(
            blocks=[pltpu.VMEM((LINE, a[0], w), BF) for a, w in zip(self.arrays, wide)],
            rows=[pltpu.VMEM((3 * LINE, w) if a[0] == 3 else (8, 128), BF) for a, w in zip(self.arrays, wide)],
            tall=pltpu.VMEM((3 * LINE, max(wide)), F32),
            own=DMA((sum(len(a[2]) for a in self.arrays),)), put=DMA((P,)), line=[DMA((LINE, sum(len(a[2]) for a in self.arrays))), DMA((A,))],
            near=both(P, 2), far=both(P, 2), near2=both(P, 2), far2=both(P, 2), over=both(P, 4),
        )

    def outs(self):
        return [jax.ShapeDtypeStruct((X, Y, 3 * LINE, a[1]) if a[0] == 3 else (X, Y, LINE, a[0], a[1]), BF) for a in self.arrays]

    def bind(self, ins, outs, s):
        self.ins, self.res, self.s = ins, outs, s
        self.spot = place()
        return self

    def _line(self):
        x, y, slot, c = self.spot
        copies, own, n = [], [], 0
        for i, (r, width, parts, whole) in enumerate(self.arrays):
            for first, w in parts:
                src = self.ins[n].at[0]
                part = lambda core: src if whole else src.at[:, cols(core * (width // 2), width // 2)]
                dst = self.s["blocks"][i].at[slot]
                dst = dst.at[:, pl.ds(first, w)] if whole else dst
                own.append(pltpu.make_async_copy(part(c), dst, self.s["own"].at[n]))
                for k in range(1, LINE):
                    to = on(slot, k, LINE)
                    copies.append(remote(part(on(to, 0, C)), dst, (self.s["line"][0].at[k, n], self.s["line"][1].at[i]), device(x, y, to)))
                n += 1
        return copies, own

    def down(self):
        copies, own = self._line()
        start(copies)
        start(own)

    def lay(self):
        for cp in self._line()[1]:
            cp.wait()
        for i, b in enumerate(self.s["blocks"]):
            some = b.at[pl.ds(0, LINE - 1)]
            pltpu.make_async_copy(some, some, self.s["line"][1].at[i]).wait()
        tall = self.s["tall"]
        for i, b in enumerate(self.s["blocks"]):
            if self.arrays[i][0] == 3:
                w = b.shape[2]
                for d in range(LINE):
                    tall[3 * d : 3 * d + 3, :w] = b[d].astype(F32)
                self.s["rows"][i][...] = tall[:, :w].astype(BF)

    def _view(self, i, lo, w, xs, ys, core, rows=slice(None)):
        at = cols(core * (self.arrays[i][1] // 2) + lo, w)
        return self.res[i].at[xs, ys, rows, at] if self.arrays[i][0] == 3 else self.res[i].at[xs, ys, rows, :, at]

    def _half(self, i, k):
        n = 24 if self.arrays[i][0] == 3 else 8
        return slice(k * n, k * n + n)

    def _put(self):
        x, y, _, c = self.spot
        out = []
        for p, (i, lo, w, colour) in enumerate(self.pieces):
            r, n, _, whole = self.arrays[i]
            at = cols(c * (n // 2) + lo, w) if whole else pl.ds(lo, w)
            src = self.s["rows"][i].at[:, at] if r == 3 else self.s["blocks"][i].at[:, :, at]
            out.append((p, i, lo, w, colour, src))
        return out

    def _near(self, relay):
        x, y, _, c = self.spot
        copies = []
        for p, i, lo, w, colour, src in self._put():
            ring = Ring(colour == 1)
            for n, k in enumerate((1, 3)):
                if relay:
                    back = (on(x, 4 - k), y) if colour == 1 else (x, on(y, 4 - k))
                    v = self._view(i, lo, w, *back, c, self._half(i, n))
                    copies.append(remote(v, v, pair(self.s["near2"], p, n), ring.to(k)))
                else:
                    copies.append(remote(src, self._view(i, lo, w, x, y, c), pair(self.s["near"], p, n), ring.to(k)))
        return copies

    def _own_rows(self):
        x, y, _, c = self.spot
        return [pltpu.make_async_copy(src, self._view(i, lo, w, x, y, c), self.s["put"].at[p]) for p, i, lo, w, colour, src in self._put()]

    def near(self):
        start(self._near(False))
        start(self._own_rows())

    def near2(self):
        landed(self._near(False))
        start(self._near(True))

    def _strip(self, i, lo, w, colour, k, core, half=slice(None)):
        x, y, _, _ = self.spot
        return self._view(i, lo, w, on(x, k), half, core) if colour == 0 else self._view(i, lo, w, half, on(y, k), core)

    def _far(self, relay):
        c, copies = self.spot[3], []
        for p, (i, lo, w, colour) in enumerate(self.pieces):
            ring = Ring(colour == 0)
            for n, k in enumerate((1, 3)):
                v = self._strip(i, lo, w, colour, 4 - k if relay else 0, c, slice(2 * n, 2 * n + 2) if relay else slice(None))
                copies.append(remote(v, v, pair(self.s["far2" if relay else "far"], p, n), ring.to(k)))
        return copies

    def _over(self, ks):
        x, y, slot, c = self.spot
        copies = []
        for k in ks:
            for p, (i, lo, w, colour) in enumerate(self.pieces):
                v = self._strip(i, lo, w, colour, k, c)
                copies.append(remote(v, v, pair(self.s["over"], p, k), device(x, y, slot + 1 - 2 * c)))
        return copies

    def far(self):
        for cp in self._own_rows():
            cp.wait()
        landed(self._near(True))
        start(self._far(False))
        start(self._over([0]))

    def far2(self):
        landed(self._far(False))
        start(self._far(True))
        start(self._over([1, 3]))

    def over(self):
        landed(self._far(True))
        start(self._over([2]))

    def finish(self):
        landed(self._over(range(4)))
        for copies in (self._line()[0], self._near(False), self._near(True), self._far(False), self._far(True), self._over(range(4))):
            left(copies)

    def steps(self):
        return [self.down, self.lay, self.near, self.near2, self.far, self.far2, self.over, self.finish]


class Scatter:
    def __init__(self, arrays, pieces, in_vmem=False):
        self.arrays, self.pieces, self.in_vmem = arrays, pieces, in_vmem

    def scratch(self):
        P = len(self.pieces)
        both = lambda *s: [DMA(s), DMA(s)]
        per = lambda *lead: [pltpu.VMEM((*lead, self._m(i), 8, w), BF) for i, lo, w, _ in self.pieces]
        half = [pltpu.VMEM((2, 2, self._m(i), 8, w), BF) for i, lo, w, _ in self.pieces]
        return dict(
            own=per(X, Y), other=per(X, Y), h1=half, f1=per(2, 4), t=per(4),
            h2=[pltpu.VMEM((2, self._m(i) // 2, 8, w), BF) for i, lo, w, _ in self.pieces], f2=per(2),
            zs=[pltpu.VMEM((LINE, a[0], a[1] // 2), BF) for a in self.arrays], zr=[pltpu.VMEM((LINE, a[0], a[1] // 2), BF) for a in self.arrays],
            get=DMA((P,)), over=both(P), a=both(P, 2), a2=both(P, 2), b=both(P, 2), b2=both(P, 2),
            line=[DMA((LINE, len(self.arrays))), DMA((len(self.arrays),))],
        )

    def _m(self, i):
        return 6 if self.arrays[i][0] == 3 else LINE

    def outs(self):
        return [jax.ShapeDtypeStruct((1, a[0], w), BF) for a in self.arrays for _, w in a[2]]

    def bind(self, ins, outs, s):
        self.ins, self.res, self.s = ins, outs, s
        self.spot = place()
        return self

    def _each(self):
        return [(p, i, lo, w, colour) for p, (i, lo, w, colour) in enumerate(self.pieces)]

    def _view(self, i, lo, w, core):
        return self.ins[i].at[:, :, :, :, cols(core * (self.arrays[i][1] // 2) + lo, w)]

    def _over(self):
        x, y, slot, c = self.spot
        return [remote(self._view(i, lo, w, 1 - c), self.s["other"][p], pair(self.s["over"], p), device(x, y, slot + 1 - 2 * c))
                for p, i, lo, w, colour in self._each()]

    def _get(self):
        return [pltpu.make_async_copy(self._view(i, lo, w, self.spot[3]), self.s["own"][p], self.s["get"].at[p]) for p, i, lo, w, colour in self._each()]

    def down(self):
        start(self._over())
        if not self.in_vmem:
            start(self._get())

    def _target(self, p, colour, k):
        x, y, _, _ = self.spot
        own = self.s["own"][p]
        return own.at[on(x, k)] if colour == 0 else own.at[:, on(y, k)]

    def _a(self):
        copies = []
        for p, i, lo, w, colour in self._each():
            for n, k in enumerate((1, 3)):
                copies.append(remote(self._target(p, colour, 2).at[pl.ds(2 * n, 2)], self.s["h1"][p].at[n], pair(self.s["a"], p, n), Ring(colour == 0).to(k)))
        return copies

    def _a2(self):
        return [remote(self._target(p, colour, k), self.s["f1"][p].at[n], pair(self.s["a2"], p, n), Ring(colour == 0).to(k))
                for p, i, lo, w, colour in self._each() for n, k in enumerate((1, 3))]

    def _of(self, copies, p):
        return [copies[2 * p], copies[2 * p + 1]]

    def near(self):
        over, a = self._over(), self._a()
        get = None if self.in_vmem else self._get()
        for p, i, lo, w, colour in self._each():
            if get:
                get[p].wait()
            over[p].wait_recv()
            own, other = self.s["own"][p], self.s["other"][p]
            mine = self._view(i, lo, w, self.spot[3]) if self.in_vmem else own

            def add(n, _):
                at = n // Y, lax.rem(n, Y)
                own[at] = (mine[at].astype(F32) + other[at].astype(F32)).astype(BF)

            lax.fori_loop(0, X * Y, add, None)
            start(self._of(a, p))

    def near2(self):
        a, a2 = self._a(), self._a2()
        for p, i, lo, w, colour in self._each():
            landed(self._of(a, p))
            for n, k in enumerate((1, 3)):
                to, h = self._target(p, colour, k), self.s["h1"][p]
                for q in range(2):
                    to[2 * n + q] = (to[2 * n + q].astype(F32) + h[n, q].astype(F32)).astype(BF)
            start(self._of(a2, p))

    def _b(self):
        copies = []
        x, y, _, _ = self.spot
        for p, i, lo, w, colour in self._each():
            ring, h = Ring(colour == 1), self._m(i) // 2
            for n, k in enumerate((1, 3)):
                copies.append(remote(self.s["t"][p].at[on(ring.at, 2), pl.ds(n * h, h)], self.s["h2"][p].at[n], pair(self.s["b"], p, n), ring.to(k)))
        return copies

    def _b2(self):
        copies = []
        for p, i, lo, w, colour in self._each():
            ring = Ring(colour == 1)
            copies += [remote(self.s["t"][p].at[on(ring.at, k)], self.s["f2"][p].at[n], pair(self.s["b2"], p, n), ring.to(k)) for n, k in enumerate((1, 3))]
        return copies

    def far(self):
        a2, b = self._a2(), self._b()
        for p, i, lo, w, colour in self._each():
            landed(self._of(a2, p))
            own, f, t = self._target(p, colour, 0), self.s["f1"][p], self.s["t"][p]

            def add(n, _):
                t[n] = (own[n].astype(F32) + f[0, n].astype(F32) + f[1, n].astype(F32)).astype(BF)

            lax.fori_loop(0, 4, add, None)
            start(self._of(b, p))

    def far2(self):
        b, b2 = self._b(), self._b2()
        for p, i, lo, w, colour in self._each():
            landed(self._of(b, p))
            ring, h, t = Ring(colour == 1), self._m(i) // 2, self.s["t"][p]
            for n, k in enumerate((1, 3)):
                at = on(ring.at, k), pl.ds(n * h, h)
                t[at] = (t[at].astype(F32) + self.s["h2"][p][n].astype(F32)).astype(BF)
            start(self._of(b2, p))

    def _line(self):
        x, y, slot, c = self.spot
        copies = []
        for k in range(1, LINE):
            to = on(slot, k, LINE)
            for i in range(len(self.arrays)):
                copies.append(remote(self.s["zs"][i].at[to], self.s["zr"][i].at[slot], (self.s["line"][0].at[k, i], self.s["line"][1].at[i]), device(x, y, to)))
        return copies

    def line(self):
        b2, slot = self._b2(), self.spot[2]
        for p, i, lo, w, colour in self._each():
            landed(self._of(b2, p))
            f = self.s["f2"][p]
            total = self.s["t"][p][Ring(colour == 1).at].astype(F32) + f[0].astype(F32) + f[1].astype(F32)
            zs = self.s["zs"][i]
            if self.arrays[i][0] == 3:
                total = total.reshape(3 * LINE, w)
                for d in range(LINE):
                    zs[d, :, lo : lo + w] = total[3 * d : 3 * d + 3].astype(BF)
            else:
                zs[:, :, lo : lo + w] = total.astype(BF)
        start(self._line())
        for zs, zr in zip(self.s["zs"], self.s["zr"]):
            zr[slot] = zs[slot]

    def finish(self):
        n = 0
        for i, (r, width, parts, _) in enumerate(self.arrays):
            zr = self.s["zr"][i]
            some = zr.at[pl.ds(0, LINE - 1)]
            pltpu.make_async_copy(some, some, self.s["line"][1].at[i]).wait()
            sums = []
            for core in range(C):
                total = zr[core].astype(F32)
                for k in range(1, Z):
                    total += zr[C * k + core].astype(F32)
                sums.append(total.astype(BF))
            whole = jnp.concatenate(sums, axis=1)
            for first, w in parts:
                self.res[n][0] = whole[:, first : first + w]
                n += 1
        for copies in (self._over(), self._a(), self._a2(), self._b(), self._b2(), self._line()):
            left(copies)

    def steps(self):
        return [self.down, self.near, self.near2, self.far, self.far2, self.line, self.finish]


QKV = ([(3, 1024, [(0, 768), (768, 128), (896, 128)], True)], [(0, 0, 256, 0), (0, 256, 256, 1)])
REST = (
    [(3, 768, [(0, 768)], False), (3, 2048, [(0, 2048)], False), (3, 2048, [(0, 2048)], False), (8, 768, [(0, 768)], False)],
    [(1, 0, 1024, 0), (2, 0, 1024, 1), (0, 0, 384, 0), (3, 0, 128, 0), (3, 128, 256, 1)],
)


HEAD, THETA = 128, 10000
G = 6
TB = 512
NT = 4
BLOCKS = NT * (NT + 1) // 2
NEG = -1e30
HIDDEN = 2 * NEG
LOG2E = 1.4426950408889634
VMEM = 56 * 2**20
EPS = 1e-6


def mm(a, b):
    return lax.dot_general(a, b, (((1,), (0,)), ((), ())), preferred_element_type=F32)


def mm_t(a, b):
    return lax.dot_general(a, b, (((1,), (1,)), ((), ())), preferred_element_type=F32)


def norm(h):
    scale = lax.rsqrt(jnp.mean(h * h, -1, keepdims=True) + EPS)
    return (h * scale).astype(BF), scale


def norm_back(h, g):
    scale = lax.rsqrt(jnp.mean(h * h, -1, keepdims=True) + EPS)
    return scale * (g - h * (scale * scale * jnp.mean(g * h, -1, keepdims=True)))


def turn_tables(tokens):
    half = HEAD // 2
    freq = np.float64(THETA) ** (-np.arange(half) / half)
    freq = np.concatenate([freq, freq])
    far = 128.0 * np.arange(tokens // 128)[:, None] * freq
    near = np.arange(128.0)[:, None] * freq
    return [jnp.asarray(t.astype(np.float32)) for t in (np.cos(far), np.sin(far), np.cos(near), np.sin(near))]


def turners(tables, n):
    ca, sa, cb, sb = tables
    row = pl.ds(n, 1)
    fc, fs = ca[row, :], sa[row, :]
    cos = fc * cb[...] - fs * sb[...]
    sin = fs * cb[...] + fc * sb[...]
    lane = lax.broadcasted_iota(jnp.int32, sin.shape, 1)
    return cos, jnp.where(lane < HEAD // 2, -sin, sin)


def swap(t):
    return pltpu.roll(t, HEAD // 2, 1)


def whole(shape):
    return pl.BlockSpec(shape, lambda *_: (0,) * len(shape))


def stage(n, plan):
    for at, todo in plan.items():

        @pl.when(n == at)
        def _():
            for do in todo:
                do()


def block_of(m):
    i = sum((m >= (r * (r + 1)) // 2).astype(jnp.int32) for r in range(1, NT))
    return i, m - (i * (i + 1)) // 2


def _front(x_ref, ca, sa, cb, sb, wq, wk, wv, wo, wg, wu, wd, q_ref, k_ref, v_ref, at_ref, o_ref, lse_ref, *rest, gq, gr):
    outs, (vt_s, top_s, mix_s, w_s, w_sem, sq, sr) = rest[:5], rest[5:]
    n = pl.program_id(0)
    gq.bind((wq, wk, wv), outs[:1], sq)
    gr.bind((wo, wg, wu, wd), outs[1:], sr)

    def weights():
        cp = pltpu.make_async_copy(outs[0], w_s, w_sem)
        cp.start()
        cp.wait()

    stage(n, {
        0: [greet, gq.down, gr.down, gq.lay, gq.near, gq.near2, gq.far, gr.lay, gr.near, gq.far2, gq.over, gq.finish, weights, gr.near2],
        2: [gr.far],
        8: [gr.far2],
        11: [gr.over],
    })

    @pl.when(n < NT)
    def _():
        a, _ = norm(x_ref[...].astype(F32))
        at_ref[:, pl.ds(pl.multiple_of(n * TB, TB), TB)] = a.T
        y = mm(a, w_s[...].reshape(a.shape[1], -1)).astype(BF)
        for i in range(TB // HEAD):
            here, rows = slice(HEAD * i, HEAD * i + HEAD), pl.ds(n * TB + HEAD * i, HEAD)
            cos, sin = turners((ca, sa, cb, sb), n * (TB // HEAD) + i)
            for h in range(G + 1):
                t = y[here, HEAD * h : HEAD * h + HEAD].astype(F32)
                t = (t * cos + swap(t) * sin).astype(BF)
                if h < G:
                    q_ref[h, rows, :] = t
                else:
                    k_ref[rows, :] = t
        v = y[:, (G + 1) * HEAD :]
        v_ref[pl.ds(n * TB, TB), :] = v
        vt_s[n] = jnp.concatenate([v.T, jnp.ones((8, TB), BF)], axis=0)

    i, j = block_of(n - NT)
    e = HEAD**-0.5 * LOG2E

    @pl.when((n >= NT) & (j == 0))
    def _():
        top_s[...] = jnp.full(top_s.shape, NEG, F32)
        mix_s[...] = jnp.zeros(mix_s.shape, F32)

    def block(masked):
        k = k_ref[pl.ds(j * TB, TB), :]
        scores = [mm_t(k, q_ref[h, pl.ds(i * TB, TB), :]) for h in range(G)]
        weights, keeps = [], []
        for h, s in enumerate(scores):
            if masked:
                s = jnp.where(lax.broadcasted_iota(jnp.int32, s.shape, 0) <= lax.broadcasted_iota(jnp.int32, s.shape, 1), s, HIDDEN)
            old = top_s[h : h + 1, :]
            top = jnp.maximum(old, s.max(axis=0, keepdims=True))
            top_s[h : h + 1, :] = top
            weights.append(jnp.exp2((s - top) * e).astype(BF))
            keeps.append(jnp.exp2((old - top) * e))
        for h in range(G):
            mix_s[h] = mix_s[h] * keeps[h] + mm(vt_s[j], weights[h])

    @pl.when((n >= NT) & (j < i))
    def _():
        block(False)

    @pl.when((n >= NT) & (j == i))
    def _():
        block(True)
        rows = pl.ds(pl.multiple_of(i * TB, TB), TB)
        for h in range(G):
            total = mix_s[h, HEAD : HEAD + 1, :]
            o_ref[h, rows, :] = (mix_s[h, :HEAD, :] * (1 / total)).T.astype(BF)
            lse_ref[h : h + 1, rows] = top_s[h : h + 1, :] * HEAD**-0.5 + jnp.log(total)

    stage(n, {NT + BLOCKS - 1: [gr.finish]})


def front(x, tables, weights, gq, gr):
    T, D = x.shape
    hbm = pl.BlockSpec(memory_space=pltpu.HBM)
    mine = [(G, T, HEAD), (T, HEAD), (T, HEAD), (D, T), (G, T, HEAD)]
    return pl.pallas_call(
        functools.partial(_front, gq=gq, gr=gr),
        grid=(NT + BLOCKS,),
        in_specs=[pl.BlockSpec((TB, D), lambda n: (jnp.minimum(n, NT - 1), 0)), *(whole(t.shape) for t in tables)] + [hbm] * len(weights),
        out_specs=[whole(s) for s in mine] + [whole((8, T))] + [hbm] * 5,
        out_shape=[jax.ShapeDtypeStruct(s, BF) for s in mine] + [jax.ShapeDtypeStruct((8, T), F32)] + gq.outs() + gr.outs(),
        scratch_shapes=[pltpu.VMEM((NT, HEAD + 8, TB), BF), pltpu.VMEM((8, TB), F32), pltpu.VMEM((G, HEAD + 8, TB), F32),
                        pltpu.VMEM((X, Y, 3 * LINE, 1024), BF), DMA(()), gq.scratch(), gr.scratch()],
        compiler_params=pltpu.CompilerParams(dimension_semantics=("arbitrary",), vmem_limit_bytes=VMEM, collective_id=1, has_side_effects=True),
        name="front",
    )(x, *tables, *weights)


def _back(q_ref, k_ref, v_ref, do_ref, lse_ref, delta_ref, at_ref, x_ref, dh_ref, w_ref, ca, sa, cb, sb, go, gg, gu, gd,
          dx_ref, *rest, sq, sr):
    outs, (dq_s, dk_s, dv_s, d_s, acc, dw_s, rq, rr) = rest[:7], rest[7:]
    n = pl.program_id(0)
    sq.bind((dw_s,), outs[:3], rq)
    sr.bind((go, gg, gu, gd), outs[3:], rr)
    stage(n, {0: [greet, sr.down], 2: [sr.near], 4: [sr.near2], 8: [sr.far], 9: [sr.far2]})
    i, j = block_of(n)
    scale = HEAD**-0.5
    e = scale * LOG2E
    rows = lambda b: pl.ds(pl.multiple_of(b * TB, TB), TB)

    @pl.when(n == 0)
    def _():
        dk_s[...] = jnp.zeros_like(dk_s)
        dv_s[...] = jnp.zeros_like(dv_s)
        acc[...] = jnp.zeros_like(acc)

    @pl.when((n < BLOCKS) & (j == 0))
    def _():
        dq_s[...] = jnp.zeros_like(dq_s)

    def block(masked):
        k, v = k_ref[rows(j), :], v_ref[rows(j), :]
        kt = k.T
        qs = [q_ref[h, rows(i), :] for h in range(G)]
        dos = [do_ref[h, rows(i), :] for h in range(G)]
        scores = [mm_t(k, q) for q in qs]
        dps = [mm_t(v, do) for do in dos]
        for h in range(G):
            p = jnp.exp2(scores[h] * e - lse_ref[h : h + 1, rows(i)] * LOG2E)
            if masked:
                p = jnp.where(lax.broadcasted_iota(jnp.int32, p.shape, 0) <= lax.broadcasted_iota(jnp.int32, p.shape, 1), p, 0.0)
            ds = (p * (dps[h] - delta_ref[h : h + 1, rows(i)])).astype(BF)
            dv_s[j] += mm(p.astype(BF), dos[h])
            dk_s[j] += mm(ds, qs[h])
            dq_s[h] += mm(kt, ds)

    def turn_back(t, b, r):
        cos, sin = turners((ca, sa, cb, sb), b * (TB // HEAD) + r)
        t = t[HEAD * r : HEAD * r + HEAD].astype(F32)
        return (t * cos - swap(t) * sin).astype(BF)

    @pl.when((n < BLOCKS) & (j < i))
    def _():
        block(False)

    @pl.when((n < BLOCKS) & (j == i))
    def _():
        block(True)
        for h in range(G):
            dq = (dq_s[h] * scale).T.astype(BF)
            for r in range(TB // HEAD):
                d_s[i, HEAD * r : HEAD * r + HEAD, HEAD * h : HEAD * h + HEAD] = turn_back(dq, i, r)
        acc[:, : G * HEAD] += mm(at_ref[:, rows(i)], d_s[i, :, : G * HEAD])

    def last():
        for b in range(NT):
            dk = (dk_s[b] * scale).astype(BF)
            for r in range(TB // HEAD):
                d_s[b, HEAD * r : HEAD * r + HEAD, G * HEAD : (G + 1) * HEAD] = turn_back(dk, b, r)
            d_s[b, :, (G + 1) * HEAD :] = dv_s[b].astype(BF)
            acc[:, G * HEAD :] += mm(at_ref[:, rows(b)], d_s[b, :, G * HEAD :])
        dw_s[...] = acc[...].astype(BF).reshape(dw_s.shape)

    stage(n, {BLOCKS: [last, sq.down, sr.line], BLOCKS + 1: [sq.near], BLOCKS + 2: [sq.near2], BLOCKS + 3: [sr.finish, sq.far]})

    @pl.when(n >= BLOCKS)
    def _():
        da = mm_t(d_s[n - BLOCKS], w_ref[...])
        dx_ref[...] = (dh_ref[...].astype(F32) + norm_back(x_ref[...].astype(F32), da)).astype(BF)

    stage(n, {BLOCKS + NT - 1: [sq.far2, sq.line, sq.finish]})


def back(q, k, v, do, lse, delta, at, x, dh, w, tables, grads, sq, sr):
    T, D = x.shape
    hbm = pl.BlockSpec(memory_space=pltpu.HBM)
    late = pl.BlockSpec((TB, D), lambda n: (jnp.maximum(n - BLOCKS, 0), 0))
    outs = sq.outs() + sr.outs()
    ins = (q, k, v, do, lse, delta, at)
    return pl.pallas_call(
        functools.partial(_back, sq=sq, sr=sr),
        grid=(BLOCKS + NT,),
        in_specs=[whole(a.shape) for a in ins] + [late, late, whole(w.shape), *(whole(t.shape) for t in tables)] + [hbm] * len(grads),
        out_specs=[late] + [whole(o.shape) for o in outs],
        out_shape=[jax.ShapeDtypeStruct((T, D), BF)] + outs,
        scratch_shapes=[pltpu.VMEM((G, HEAD, TB), F32), pltpu.VMEM((NT, TB, HEAD), F32), pltpu.VMEM((NT, TB, HEAD), F32),
                        pltpu.VMEM((NT, TB, 1024), BF), pltpu.VMEM(w.shape, F32), pltpu.VMEM((X, Y, 6, 8, 1024), BF), sq.scratch(), sr.scratch()],
        compiler_params=pltpu.CompilerParams(dimension_semantics=("arbitrary",), vmem_limit_bytes=63 * 2**20, collective_id=2, has_side_effects=True),
        name="back",
    )(*ins, x, dh, w, *tables, *grads)


def _middle(x_ref, dy_ref, o_ref, wo_ref, wg_ref, wu_ref, wd_ref,
            dh_ref, do_ref, delta_ref, dwo_ref, dwg_ref, dwu_ref, dwd_ref,
            h_s, b_s, bt_s, dy_s, db_s, o_s, ao, ag, au, ad, *, tb, nj, nt, strip):
    j, t = pl.program_id(0), pl.program_id(1)
    D = x_ref.shape[1]
    fj = wg_ref.shape[1]

    @pl.when(j == 0)
    def _():
        o = jnp.concatenate([o_ref[h] for h in range(6)], axis=1)
        o_s[t] = o
        h = (x_ref[...].astype(F32) + mm(o, wo_ref[...]).astype(BF).astype(F32)).astype(BF)
        h_s[t] = h
        b, _ = norm(h.astype(F32))
        b_s[t] = b
        bt_s[t] = b.T
        dy_s[t] = dy_ref[...]

    @pl.when(t == 0)
    def _():
        ag[...] = jnp.zeros_like(ag)
        au[...] = jnp.zeros_like(au)
        ad[...] = jnp.zeros_like(ad)

    b, bt, dy = b_s[t], bt_s[t], dy_s[t]
    db = None
    for s in range(0, fj, strip):
        cols = slice(s, s + strip)
        wg, wu, wd = wg_ref[:, cols], wu_ref[:, cols], wd_ref[cols, :]
        gate, up, dact = mm(b, wg), mm(b, wu), mm_t(dy, wd).astype(BF).astype(F32)
        sig = 1 / (1 + jnp.exp(-gate))
        silu = gate * sig
        act = (silu * up).astype(BF)
        dup = (dact * silu).astype(BF)
        dgate = (dact * up * (sig + silu * (1 - sig))).astype(BF)
        ad[cols, :] += mm(act.T, dy)
        ag[:, cols] += mm(bt, dgate)
        au[:, cols] += mm(bt, dup)
        part = mm_t(dgate, wg) + mm_t(dup, wu)
        db = part if db is None else db + part

    @pl.when(j == 0)
    def _():
        db_s[t] = db

    @pl.when(j > 0)
    def _():
        db_s[t] += db

    @pl.when(t == nt - 1)
    def _():
        dwg_ref[...] = ag[...].astype(BF)
        dwu_ref[...] = au[...].astype(BF)
        dwd_ref[...] = ad[...].astype(BF)

    @pl.when(j == nj - 1)
    def _():
        dh = (dy.astype(F32) + norm_back(h_s[t].astype(F32), db_s[t]).astype(BF).astype(F32)).astype(BF)
        dh_ref[...] = dh
        do = mm_t(dh, wo_ref[...]).astype(BF)
        o = o_s[t]
        prod = do.astype(F32) * o.astype(F32)
        for h in range(6):
            at = slice(HEAD * h, HEAD * h + HEAD)
            do_ref[h] = do[:, at]
        delta_ref[...] = jnp.concatenate([prod[:, HEAD * h : HEAD * h + HEAD].sum(-1, keepdims=True) for h in range(6)]
                                         + [jnp.zeros((tb, 2), F32)], axis=1).T
        part = mm(o.T, dh)

        @pl.when(t == 0)
        def _():
            ao[...] = part

        @pl.when(t > 0)
        def _():
            ao[...] += part

        @pl.when(t == nt - 1)
        def _():
            dwo_ref[...] = ao[...].astype(BF)


def middle(x, dy, o, wo, wg, wu, wd, tb=512, nj=4, strip=512):
    T, D = x.shape
    F = wg.shape[1]
    nt, fj = T // tb, F // nj
    early = lambda j, t: jnp.where(j == 0, t, nt - 1)
    late = lambda j, t: jnp.where(j == nj - 1, t, 0)
    return pl.pallas_call(
        functools.partial(_middle, tb=tb, nj=nj, nt=nt, strip=strip),
        grid=(nj, nt),
        in_specs=[pl.BlockSpec((tb, D), lambda j, t: (early(j, t), 0)), pl.BlockSpec((tb, D), lambda j, t: (early(j, t), 0)),
                  pl.BlockSpec((6, tb, HEAD), lambda j, t: (0, early(j, t), 0)), whole(wo.shape),
                  pl.BlockSpec((D, fj), lambda j, t: (0, j)), pl.BlockSpec((D, fj), lambda j, t: (0, j)), pl.BlockSpec((fj, D), lambda j, t: (j, 0))],
        out_specs=[pl.BlockSpec((tb, D), lambda j, t: (late(j, t), 0)), pl.BlockSpec((6, tb, HEAD), lambda j, t: (0, late(j, t), 0)),
                   pl.BlockSpec((8, tb), lambda j, t: (0, late(j, t))), whole(wo.shape),
                   pl.BlockSpec((D, fj), lambda j, t: (0, j)), pl.BlockSpec((D, fj), lambda j, t: (0, j)), pl.BlockSpec((fj, D), lambda j, t: (j, 0))],
        out_shape=[jax.ShapeDtypeStruct((T, D), BF), jax.ShapeDtypeStruct((6, T, HEAD), BF), jax.ShapeDtypeStruct((8, T), F32),
                   *(jax.ShapeDtypeStruct(a.shape, BF) for a in (wo, wg, wu, wd))],
        scratch_shapes=[pltpu.VMEM((nt, tb, D), BF), pltpu.VMEM((nt, tb, D), BF), pltpu.VMEM((nt, D, tb), BF), pltpu.VMEM((nt, tb, D), BF),
                        pltpu.VMEM((nt, tb, D), F32), pltpu.VMEM((nt, tb, D), BF),
                        pltpu.VMEM(wo.shape, F32), pltpu.VMEM((D, fj), F32), pltpu.VMEM((D, fj), F32), pltpu.VMEM((fj, D), F32)],
        compiler_params=pltpu.CompilerParams(dimension_semantics=("arbitrary", "arbitrary"), vmem_limit_bytes=63 * 2**20), name="middle",
    )(x, dy, o, wo, wg, wu, wd)


def solution(mesh):
    gq, gr, sq, sr = Gather(*QKV), Gather(*REST), Scatter(*QKV, in_vmem=True), Scatter(*REST)

    def step(x, dy, *weights):
        x, dy = x[0], dy[0]
        T, D = x.shape
        tables = turn_tables(T)
        q, k, v, at, o, lse, w, *rest = front(x, tables, weights, gq, gr)
        rest = [a.reshape(D, -1) for a in rest[:3]] + [rest[3].reshape(-1, D)]
        dh, do, delta, *grads = middle(x, dy, o, *rest)
        grads = [g.reshape(X, Y, g.shape[0] // (8 * X * Y), 8, -1) for g in grads]
        dx, *by_w = back(q, k, v, do, lse, delta, at, x, dh, w.reshape(D, -1), tables, grads, sq, sr)
        return (dx[None], *by_w)

    states, cut = P(("rep", "dp"), None, None), P(None, "dp", None)
    return jax.shard_map(
        step,
        mesh=mesh,
        in_specs=(states, states) + (cut,) * 7,
        out_specs=(states,) + (P("rep", "dp", None),) * 7,
        check_vma=False,
    )
```

```python
import functools

import jax
import jax.numpy as jnp
import numpy as np
from jax import lax
from jax.experimental import pallas as pl
from jax.experimental.pallas import tpu as pltpu
from jax.sharding import PartitionSpec as P


F32, BF = jnp.float32, jnp.bfloat16
X, Y, Z, C = 4, 4, 8, 2
LINE = Z * C
DMA = pltpu.SemaphoreType.DMA


def place():
    me = lax.axis_index("dp")
    return me // (LINE * Y), lax.rem(me // LINE, Y), lax.rem(me, LINE), lax.rem(me, C)


def device(x, y, slot):
    return {"dp": (x * Y + y) * LINE + slot}


def on(a, k, n=4):
    return lax.rem(a + k, n)


def remote(src, dst, sems, where):
    send, recv = sems
    return pltpu.make_async_remote_copy(src_ref=src, dst_ref=dst, send_sem=send, recv_sem=recv, device_id=where, device_id_type=pl.DeviceIdType.MESH)


def start(copies):
    for cp in copies:
        cp.start()


def landed(copies):
    for cp in copies:
        cp.wait_recv()


def left(copies):
    for cp in copies:
        cp.wait_send()


def peers():
    x, y, slot, _ = place()
    who = [device(x, y, on(slot, k, LINE)) for k in range(1, LINE)]
    for k in (1, 3):
        who += [device(on(x, k), y, slot), device(x, on(y, k), slot)]
    return who


def hello():
    for d in peers():
        pl.semaphore_signal(pltpu.get_barrier_semaphore(), inc=1, device_id=d, device_id_type=pl.DeviceIdType.MESH)


def meet():
    pl.semaphore_wait(pltpu.get_barrier_semaphore(), len(peers()))


def cols(first, size):
    return pl.ds(pl.multiple_of(first, 128), size)


def pair(sems, *index):
    return sems[0].at[index], sems[1].at[index]


class Ring:
    def __init__(self, along_x):
        x, y, slot, c = place()
        self.at = x if along_x else y
        self.to = lambda k: device(on(x, k), y, slot) if along_x else device(x, on(y, k), slot)


class Gather:
    def __init__(self, arrays, pieces, in_vmem=False):
        self.arrays, self.pieces, self.in_vmem = arrays, pieces, in_vmem

    def scratch(self):
        A, P = len(self.arrays), len(self.pieces)
        both = lambda *s: [DMA(s), DMA(s)]
        wide = [n if whole else n // 2 for _, n, _, whole in self.arrays]
        return dict(
            blocks=[pltpu.VMEM((LINE, a[0], w), BF) for a, w in zip(self.arrays, wide)],
            rows=[pltpu.VMEM((3 * LINE, w) if a[0] == 3 else (8, 128), BF) for a, w in zip(self.arrays, wide)],
            tall=pltpu.VMEM((3 * LINE, max(wide)), F32),
            own=DMA((sum(len(a[2]) for a in self.arrays),)), put=DMA((P,)), line=[DMA((LINE, sum(len(a[2]) for a in self.arrays))), DMA((A,))],
            near=both(P, 2), far=both(P, 2), near2=both(P, 2), far2=both(P, 2), over=both(P, 4),
        )

    def outs(self):
        return [jax.ShapeDtypeStruct((X, Y, 3 * LINE, a[1]) if a[0] == 3 else (X, Y, LINE, a[0], a[1]), BF) for a in self.arrays]

    def bind(self, ins, outs, s):
        self.ins, self.res, self.s = ins, outs, s
        self.spot = place()
        return self

    def _line(self):
        x, y, slot, c = self.spot
        copies, own, n = [], [], 0
        for i, (r, width, parts, whole) in enumerate(self.arrays):
            for first, w in parts:
                src = self.ins[n].at[0]
                part = lambda core: src if whole else src.at[:, cols(core * (width // 2), width // 2)]
                dst = self.s["blocks"][i].at[slot]
                dst = dst.at[:, pl.ds(first, w)] if whole else dst
                own.append(pltpu.make_async_copy(part(c), dst, self.s["own"].at[n]))
                for k in range(1, LINE):
                    to = on(slot, k, LINE)
                    copies.append(remote(part(on(to, 0, C)), dst, (self.s["line"][0].at[k, n], self.s["line"][1].at[i]), device(x, y, to)))
                n += 1
        return copies, own

    def down(self):
        copies, own = self._line()
        start(copies)
        start(own)

    def lay(self):
        for cp in self._line()[1]:
            cp.wait()
        for i, b in enumerate(self.s["blocks"]):
            some = b.at[pl.ds(0, LINE - 1)]
            pltpu.make_async_copy(some, some, self.s["line"][1].at[i]).wait()
        tall = self.s["tall"]
        for i, b in enumerate(self.s["blocks"]):
            if self.arrays[i][0] == 3:
                w = b.shape[2]
                for d in range(LINE):
                    tall[3 * d : 3 * d + 3, :w] = b[d].astype(F32)
                self.s["rows"][i][...] = tall[:, :w].astype(BF)

    def _view(self, i, lo, w, xs, ys, core, rows=slice(None)):
        at = cols(core * (self.arrays[i][1] // 2) + lo, w)
        if rows == slice(LINE, None) and self.arrays[i][0] == 3:
            rows = pl.ds(LINE, 2 * LINE)
        return self.res[i].at[xs, ys, rows, at] if self.arrays[i][0] == 3 else self.res[i].at[xs, ys, rows, :, at]

    def _half(self, i, k):
        n = LINE if self.arrays[i][0] == 3 else LINE // 2
        return slice(n, None) if k else slice(n)

    def _put(self):
        x, y, _, c = self.spot
        out = []
        for p, (i, lo, w, colour) in enumerate(self.pieces):
            r, n, _, whole = self.arrays[i]
            at = cols(c * (n // 2) + lo, w) if whole else pl.ds(lo, w)
            src = self.s["rows"][i].at[:, at] if r == 3 else self.s["blocks"][i].at[:, :, at]
            out.append((p, i, lo, w, colour, src))
        return out

    def _near(self, relay):
        x, y, _, c = self.spot
        copies = []
        for p, i, lo, w, colour, src in self._put():
            ring = Ring(colour == 1)
            for n, k in enumerate((1, 3)):
                if relay:
                    back = (on(x, 4 - k), y) if colour == 1 else (x, on(y, 4 - k))
                    v = self._view(i, lo, w, *back, c, self._half(i, n))
                    copies.append(remote(v, v, pair(self.s["near2"], p, n), ring.to(k)))
                else:
                    copies.append(remote(src, self._view(i, lo, w, x, y, c), pair(self.s["near"], p, n), ring.to(k)))
        return copies

    def _own_rows(self):
        x, y, _, c = self.spot
        return [pltpu.make_async_copy(src, self._view(i, lo, w, x, y, c), self.s["put"].at[p]) for p, i, lo, w, colour, src in self._put()]

    def near(self):
        start(self._near(False))
        if self.in_vmem:
            x, y, _, c = self.spot
            for rows, res in zip(self.s["rows"], self.res):
                n = rows.shape[1] // 2
                res[x, y, :, cols(c * n, n)] = rows[:, cols(c * n, n)]
        else:
            start(self._own_rows())

    def near2(self):
        landed(self._near(False))
        start(self._near(True))

    def _strip(self, i, lo, w, colour, k, core, half=slice(None)):
        x, y, _, _ = self.spot
        return self._view(i, lo, w, on(x, k), half, core) if colour == 0 else self._view(i, lo, w, half, on(y, k), core)

    def _far(self, relay):
        c, copies = self.spot[3], []
        for p, (i, lo, w, colour) in enumerate(self.pieces):
            ring = Ring(colour == 0)
            for n, k in enumerate((1, 3)):
                v = self._strip(i, lo, w, colour, 4 - k if relay else 0, c, slice(2 * n, 2 * n + 2) if relay else slice(None))
                copies.append(remote(v, v, pair(self.s["far2" if relay else "far"], p, n), ring.to(k)))
        return copies

    def _over(self, ks):
        x, y, slot, c = self.spot
        copies = []
        for k in ks:
            for p, (i, lo, w, colour) in enumerate(self.pieces):
                v = self._strip(i, lo, w, colour, k, c)
                copies.append(remote(v, v, pair(self.s["over"], p, k), device(x, y, slot + 1 - 2 * c)))
        return copies

    def far(self):
        if not self.in_vmem:
            for cp in self._own_rows():
                cp.wait()
        landed(self._near(True))
        start(self._far(False))
        start(self._over([0]))

    def far2(self):
        landed(self._far(False))
        start(self._far(True))
        start(self._over([1, 3]))

    def over(self):
        landed(self._far(True))
        start(self._over([2]))

    def finish(self):
        landed(self._over(range(4)))
        for copies in (self._line()[0], self._near(False), self._near(True), self._far(False), self._far(True), self._over(range(4))):
            left(copies)

    def steps(self):
        return [self.down, self.lay, self.near, self.near2, self.far, self.far2, self.over, self.finish]


class Scatter:
    def __init__(self, arrays, pieces, in_vmem=False):
        self.arrays, self.pieces, self.in_vmem = arrays, pieces, in_vmem

    def scratch(self):
        P = len(self.pieces)
        both = lambda *s: [DMA(s), DMA(s)]
        per = lambda *lead: [pltpu.VMEM((*lead, self._m(i), LINE, w), BF) for i, lo, w, _ in self.pieces]
        half = [pltpu.VMEM((2, 2, self._m(i), LINE, w), BF) for i, lo, w, _ in self.pieces]
        return dict(
            own=per(X, Y), other=per(X, Y), h1=half, f1=per(2, 4), t=per(4),
            h2=per(), f2=per(2),
            zs=[pltpu.VMEM((LINE, a[0], a[1] // 2), BF) for a in self.arrays], zr=[pltpu.VMEM((LINE, a[0], a[1] // 2), BF) for a in self.arrays],
            get=DMA((P,)), over=both(P), a=both(P, 2), a2=both(P, 2), b=both(P, 2), b2=both(P, 2),
            line=[DMA((LINE, len(self.arrays))), DMA((len(self.arrays),))],
        )

    def _m(self, i):
        return 3 if self.arrays[i][0] == 3 else LINE // 2

    def _parts(self, i):
        h = self._m(i) // 2
        return pl.ds(0, h), pl.ds(h, self._m(i) - h)

    def outs(self):
        return [jax.ShapeDtypeStruct((1, a[0], w), BF) for a in self.arrays for _, w in a[2]]

    def bind(self, ins, outs, s):
        self.ins, self.res, self.s = ins, outs, s
        self.spot = place()
        return self

    def _each(self):
        return [(p, i, lo, w, colour) for p, (i, lo, w, colour) in enumerate(self.pieces)]

    def _view(self, i, lo, w, core):
        return self.ins[i].at[:, :, :, :, cols(core * (self.arrays[i][1] // 2) + lo, w)]

    def _over(self):
        x, y, slot, c = self.spot
        return [remote(self._view(i, lo, w, 1 - c), self.s["other"][p], pair(self.s["over"], p), device(x, y, slot + 1 - 2 * c))
                for p, i, lo, w, colour in self._each()]

    def _get(self):
        return [pltpu.make_async_copy(self._view(i, lo, w, self.spot[3]), self.s["own"][p], self.s["get"].at[p]) for p, i, lo, w, colour in self._each()]

    def down(self):
        start(self._over())
        if not self.in_vmem:
            start(self._get())

    def _target(self, p, colour, k):
        x, y, _, _ = self.spot
        own = self.s["own"][p]
        return own.at[on(x, k)] if colour == 0 else own.at[:, on(y, k)]

    def _a(self):
        copies = []
        for p, i, lo, w, colour in self._each():
            for n, k in enumerate((1, 3)):
                copies.append(remote(self._target(p, colour, 2).at[pl.ds(2 * n, 2)], self.s["h1"][p].at[n], pair(self.s["a"], p, n), Ring(colour == 0).to(k)))
        return copies

    def _a2(self):
        return [remote(self._target(p, colour, k), self.s["f1"][p].at[n], pair(self.s["a2"], p, n), Ring(colour == 0).to(k))
                for p, i, lo, w, colour in self._each() for n, k in enumerate((1, 3))]

    def _of(self, copies, p):
        return [copies[2 * p], copies[2 * p + 1]]

    def near(self):
        over, a = self._over(), self._a()
        get = None if self.in_vmem else self._get()
        for p, i, lo, w, colour in self._each():
            if get:
                get[p].wait()
            over[p].wait_recv()
            own, other = self.s["own"][p], self.s["other"][p]
            mine = self._view(i, lo, w, self.spot[3]) if self.in_vmem else own

            def add(n, _):
                at = n // Y, lax.rem(n, Y)
                own[at] = (mine[at].astype(F32) + other[at].astype(F32)).astype(BF)

            lax.fori_loop(0, X * Y, add, None)
            start(self._of(a, p))

    def near2(self):
        a, a2 = self._a(), self._a2()
        for p, i, lo, w, colour in self._each():
            landed(self._of(a, p))
            for n, k in enumerate((1, 3)):
                to, h = self._target(p, colour, k), self.s["h1"][p]
                for q in range(2):
                    to[2 * n + q] = (to[2 * n + q].astype(F32) + h[n, q].astype(F32)).astype(BF)
            start(self._of(a2, p))

    def _b(self):
        copies = []
        x, y, _, _ = self.spot
        for p, i, lo, w, colour in self._each():
            ring = Ring(colour == 1)
            for n, (k, part) in enumerate(zip((1, 3), self._parts(i))):
                copies.append(remote(self.s["t"][p].at[on(ring.at, 2), part], self.s["h2"][p].at[part], pair(self.s["b"], p, n), ring.to(k)))
        return copies

    def _b2(self):
        copies = []
        for p, i, lo, w, colour in self._each():
            ring = Ring(colour == 1)
            copies += [remote(self.s["t"][p].at[on(ring.at, k)], self.s["f2"][p].at[n], pair(self.s["b2"], p, n), ring.to(k)) for n, k in enumerate((1, 3))]
        return copies

    def far(self):
        a2, b = self._a2(), self._b()
        for p, i, lo, w, colour in self._each():
            landed(self._of(a2, p))
            own, f, t = self._target(p, colour, 0), self.s["f1"][p], self.s["t"][p]

            def add(n, _):
                t[n] = (own[n].astype(F32) + f[0, n].astype(F32) + f[1, n].astype(F32)).astype(BF)

            lax.fori_loop(0, 4, add, None)
            start(self._of(b, p))

    def far2(self):
        b, b2 = self._b(), self._b2()
        for p, i, lo, w, colour in self._each():
            landed(self._of(b, p))
            ring, t = Ring(colour == 1), self.s["t"][p]
            for k, part in zip((1, 3), self._parts(i)):
                at = on(ring.at, k), part
                t[at] = (t[at].astype(F32) + self.s["h2"][p][part].astype(F32)).astype(BF)
            start(self._of(b2, p))

    def _line(self):
        x, y, slot, c = self.spot
        copies = []
        for k in range(1, LINE):
            to = on(slot, k, LINE)
            for i in range(len(self.arrays)):
                copies.append(remote(self.s["zs"][i].at[to], self.s["zr"][i].at[slot], (self.s["line"][0].at[k, i], self.s["line"][1].at[i]), device(x, y, to)))
        return copies

    def line(self):
        b2, slot = self._b2(), self.spot[2]
        for p, i, lo, w, colour in self._each():
            landed(self._of(b2, p))
            f = self.s["f2"][p]
            total = self.s["t"][p][Ring(colour == 1).at].astype(F32) + f[0].astype(F32) + f[1].astype(F32)
            zs = self.s["zs"][i]
            if self.arrays[i][0] == 3:
                total = total.reshape(3 * LINE, w)
                for d in range(LINE):
                    zs[d, :, lo : lo + w] = total[3 * d : 3 * d + 3].astype(BF)
            else:
                zs[:, :, lo : lo + w] = total.reshape(LINE, -1, w).astype(BF)
        start(self._line())
        for zs, zr in zip(self.s["zs"], self.s["zr"]):
            zr[slot] = zs[slot]

    def finish(self):
        n = 0
        for i, (r, width, parts, _) in enumerate(self.arrays):
            zr = self.s["zr"][i]
            some = zr.at[pl.ds(0, LINE - 1)]
            pltpu.make_async_copy(some, some, self.s["line"][1].at[i]).wait()
            sums = []
            for core in range(C):
                total = zr[core].astype(F32)
                for k in range(1, Z):
                    total += zr[C * k + core].astype(F32)
                sums.append(total.astype(BF))
            whole = jnp.concatenate(sums, axis=1)
            for first, w in parts:
                self.res[n][0] = whole[:, first : first + w]
                n += 1
        for copies in (self._over(), self._a(), self._a2(), self._b(), self._b2(), self._line()):
            left(copies)

    def steps(self):
        return [self.down, self.near, self.near2, self.far, self.far2, self.line, self.finish]


QKV = ([(3, 1024, [(0, 768), (768, 128), (896, 128)], True)], [(0, 0, 256, 0), (0, 256, 256, 1)])
REST = (
    [(3, 768, [(0, 768)], False), (3, 2048, [(0, 2048)], False), (3, 2048, [(0, 2048)], False), (8, 768, [(0, 768)], False)],
    [(1, 0, 1024, 0), (2, 0, 1024, 1), (0, 0, 384, 0), (3, 0, 128, 0), (3, 128, 256, 1)],
)


HEAD, THETA = 128, 10000
G = 6
TB = 512
NT = 4
BLOCKS = NT * (NT + 1) // 2
NEG = -1e30
HIDDEN = 2 * NEG
LOG2E = 1.4426950408889634
VMEM = 56 * 2**20
EPS = 1e-6


def mm(a, b):
    return lax.dot_general(a, b, (((1,), (0,)), ((), ())), preferred_element_type=F32)


def mm_t(a, b):
    return lax.dot_general(a, b, (((1,), (1,)), ((), ())), preferred_element_type=F32)


def norm(h):
    scale = lax.rsqrt(jnp.mean(h * h, -1, keepdims=True) + EPS)
    return (h * scale).astype(BF), scale


def norm_back(h, g):
    scale = lax.rsqrt(jnp.mean(h * h, -1, keepdims=True) + EPS)
    return scale * (g - h * (scale * scale * jnp.mean(g * h, -1, keepdims=True)))


def turn_tables(tokens):
    half = HEAD // 2
    freq = np.float64(THETA) ** (-np.arange(half) / half)
    freq = np.concatenate([freq, freq])
    far = 128.0 * np.arange(tokens // 128)[:, None] * freq
    near = np.arange(128.0)[:, None] * freq
    return [jnp.asarray(t.astype(np.float32)) for t in (np.cos(far), np.sin(far), np.cos(near), np.sin(near))]


def turners(tables, n):
    ca, sa, cb, sb = tables
    row = pl.ds(n, 1)
    fc, fs = ca[row, :], sa[row, :]
    cos = fc * cb[...] - fs * sb[...]
    sin = fs * cb[...] + fc * sb[...]
    lane = lax.broadcasted_iota(jnp.int32, sin.shape, 1)
    return cos, jnp.where(lane < HEAD // 2, -sin, sin)


def swap(t):
    return pltpu.roll(t, HEAD // 2, 1)


def whole(shape):
    return pl.BlockSpec(shape, lambda *_: (0,) * len(shape))


def stage(n, plan):
    for at, todo in plan.items():

        @pl.when(n == at)
        def _():
            for do in todo:
                do()


def block_of(m):
    i = sum((m >= (r * (r + 1)) // 2).astype(jnp.int32) for r in range(1, NT))
    return i, m - (i * (i + 1)) // 2


def _front(x_ref, ca, sa, cb, sb, wq, wk, wv, wo, wg, wu, wd, q_ref, k_ref, v_ref, at_ref, o_ref, lse_ref, *rest, gq, gr):
    outs, (x_s, vt_s, top_s, mix_s, w_s, sems, sq, sr) = rest[:5], rest[5:]
    n = pl.program_id(0)
    gq.bind((wq, wk, wv), (w_s,), sq)
    gr.bind((wo, wg, wu, wd), outs[1:], sr)
    fetch = pltpu.make_async_copy(x_ref, x_s, sems.at[0])
    keep = pltpu.make_async_copy(w_s, outs[0], sems.at[1])

    def normed(first, last):
        for b in range(first, last):
            rows = slice(b * TB, b * TB + TB)
            a, _ = norm(x_s[rows, :].astype(F32))
            x_s[rows, :] = a
            at_ref[:, rows] = a.T

    def early():
        fetch.wait()
        normed(0, NT // 2)

    def late():
        normed(NT // 2, NT)

    stage(n, {
        0: [fetch.start, hello, early, meet, gq.down, gr.down, late, gq.lay, gq.near, gq.near2, gq.far, gr.lay, gq.far2, gr.near, gq.over, gq.finish, keep.start],
        1: [gr.near2],
        3: [gr.far],
        9: [gr.far2],
        12: [gr.over],
    })

    @pl.when(n < NT)
    def _():
        a = x_s[pl.ds(pl.multiple_of(n * TB, TB), TB), :]
        y = mm(a, w_s[...].reshape(a.shape[1], -1)).astype(BF)
        for i in range(TB // HEAD):
            here, rows = slice(HEAD * i, HEAD * i + HEAD), pl.ds(n * TB + HEAD * i, HEAD)
            cos, sin = turners((ca, sa, cb, sb), n * (TB // HEAD) + i)
            for h in range(G + 1):
                t = y[here, HEAD * h : HEAD * h + HEAD].astype(F32)
                t = (t * cos + swap(t) * sin).astype(BF)
                if h < G:
                    q_ref[h, rows, :] = t
                else:
                    k_ref[rows, :] = t
        v = y[:, (G + 1) * HEAD :]
        v_ref[pl.ds(n * TB, TB), :] = v
        vt_s[n] = jnp.concatenate([v.T, jnp.ones((8, TB), BF)], axis=0)

    i, j = block_of(n - NT)
    e = HEAD**-0.5 * LOG2E

    @pl.when((n >= NT) & (j == 0))
    def _():
        top_s[...] = jnp.full(top_s.shape, NEG, F32)
        mix_s[...] = jnp.zeros(mix_s.shape, F32)

    def block(masked):
        k = k_ref[pl.ds(j * TB, TB), :]
        scores = [mm_t(k, q_ref[h, pl.ds(i * TB, TB), :]) for h in range(G)]
        weights, keeps = [], []
        for h, s in enumerate(scores):
            if masked:
                s = jnp.where(lax.broadcasted_iota(jnp.int32, s.shape, 0) <= lax.broadcasted_iota(jnp.int32, s.shape, 1), s, HIDDEN)
            old = top_s[h : h + 1, :]
            top = jnp.maximum(old, s.max(axis=0, keepdims=True))
            top_s[h : h + 1, :] = top
            weights.append(jnp.exp2((s - top) * e).astype(BF))
            keeps.append(jnp.exp2((old - top) * e))
        for h in range(G):
            mix_s[h] = mix_s[h] * keeps[h] + mm(vt_s[j], weights[h])

    @pl.when((n >= NT) & (j < i))
    def _():
        block(False)

    @pl.when((n >= NT) & (j == i))
    def _():
        block(True)
        rows = pl.ds(pl.multiple_of(i * TB, TB), TB)
        for h in range(G):
            total = mix_s[h, HEAD : HEAD + 1, :]
            o_ref[h, rows, :] = (mix_s[h, :HEAD, :] * (1 / total)).T.astype(BF)
            lse_ref[h : h + 1, rows] = top_s[h : h + 1, :] * HEAD**-0.5 + jnp.log(total)

    stage(n, {NT + BLOCKS - 1: [gr.finish, keep.wait]})


def front(x, tables, weights, gq, gr):
    T, D = x.shape
    hbm = pl.BlockSpec(memory_space=pltpu.HBM)
    mine = [(G, T, HEAD), (T, HEAD), (T, HEAD), (D, T), (G, T, HEAD)]
    return pl.pallas_call(
        functools.partial(_front, gq=gq, gr=gr),
        grid=(NT + BLOCKS,),
        in_specs=[hbm, *(whole(t.shape) for t in tables)] + [hbm] * len(weights),
        out_specs=[whole(s) for s in mine] + [whole((8, T))] + [hbm] * 5,
        out_shape=[jax.ShapeDtypeStruct(s, BF) for s in mine] + [jax.ShapeDtypeStruct((8, T), F32)] + gq.outs() + gr.outs(),
        scratch_shapes=[pltpu.VMEM((T, D), BF), pltpu.VMEM((NT, HEAD + 8, TB), BF), pltpu.VMEM((8, TB), F32), pltpu.VMEM((G, HEAD + 8, TB), F32),
                        pltpu.VMEM((X, Y, 3 * LINE, 1024), BF), DMA((2,)), gq.scratch(), gr.scratch()],
        compiler_params=pltpu.CompilerParams(dimension_semantics=("arbitrary",), vmem_limit_bytes=VMEM, collective_id=1, has_side_effects=True),
        name="front",
    )(x, *tables, *weights)


def _back(q_ref, k_ref, v_ref, do_ref, lse_ref, delta_ref, at_ref, x_ref, dh_ref, w_ref, ca, sa, cb, sb, go, gg, gu, gd,
          dx_ref, *rest, sq, sr):
    outs, (dq_s, dk_s, dv_s, d_s, acc, dw_s, rq, rr) = rest[:7], rest[7:]
    n = pl.program_id(0)
    sq.bind((dw_s,), outs[:3], rq)
    sr.bind((go, gg, gu, gd), outs[3:], rr)
    stage(n, {0: [hello], 1: [meet, sr.down], 3: [sr.near], 5: [sr.near2], 9: [sr.far]})
    i, j = block_of(n)
    scale = HEAD**-0.5
    e = scale * LOG2E
    rows = lambda b: pl.ds(pl.multiple_of(b * TB, TB), TB)

    @pl.when(n == 0)
    def _():
        dk_s[...] = jnp.zeros_like(dk_s)
        dv_s[...] = jnp.zeros_like(dv_s)
        acc[...] = jnp.zeros_like(acc)

    @pl.when((n < BLOCKS) & (j == 0))
    def _():
        dq_s[...] = jnp.zeros_like(dq_s)

    def block(masked):
        k, v = k_ref[rows(j), :], v_ref[rows(j), :]
        kt = k.T
        qs = [q_ref[h, rows(i), :] for h in range(G)]
        dos = [do_ref[h, rows(i), :] for h in range(G)]
        scores = [mm_t(k, q) for q in qs]
        dps = [mm_t(v, do) for do in dos]
        for h in range(G):
            p = jnp.exp2(scores[h] * e - lse_ref[h : h + 1, rows(i)] * LOG2E)
            if masked:
                p = jnp.where(lax.broadcasted_iota(jnp.int32, p.shape, 0) <= lax.broadcasted_iota(jnp.int32, p.shape, 1), p, 0.0)
            ds = (p * (dps[h] - delta_ref[h : h + 1, rows(i)])).astype(BF)
            dv_s[j] += mm(p.astype(BF), dos[h])
            dk_s[j] += mm(ds, qs[h])
            dq_s[h] += mm(kt, ds)

    def turn_back(t, b, r):
        cos, sin = turners((ca, sa, cb, sb), b * (TB // HEAD) + r)
        t = t[HEAD * r : HEAD * r + HEAD].astype(F32)
        return (t * cos - swap(t) * sin).astype(BF)

    @pl.when((n < BLOCKS) & (j < i))
    def _():
        block(False)

    @pl.when((n < BLOCKS) & (j == i))
    def _():
        block(True)
        for h in range(G):
            dq = (dq_s[h] * scale).T.astype(BF)
            for r in range(TB // HEAD):
                d_s[i, HEAD * r : HEAD * r + HEAD, HEAD * h : HEAD * h + HEAD] = turn_back(dq, i, r)
        acc[:, : G * HEAD] += mm(at_ref[:, rows(i)], d_s[i, :, : G * HEAD])

    def last():
        for b in range(NT):
            dk = (dk_s[b] * scale).astype(BF)
            for r in range(TB // HEAD):
                d_s[b, HEAD * r : HEAD * r + HEAD, G * HEAD : (G + 1) * HEAD] = turn_back(dk, b, r)
            d_s[b, :, (G + 1) * HEAD :] = dv_s[b].astype(BF)
            acc[:, G * HEAD :] += mm(at_ref[:, rows(b)], d_s[b, :, G * HEAD :])
        dw_s[...] = acc[...].astype(BF).reshape(dw_s.shape)

    stage(n, {BLOCKS: [sr.far2, last, sq.down, sr.line], BLOCKS + 1: [sq.near], BLOCKS + 2: [sq.near2], BLOCKS + 3: [sq.far]})

    @pl.when(n >= BLOCKS)
    def _():
        da = mm_t(d_s[n - BLOCKS], w_ref[...])
        dx_ref[...] = (dh_ref[...].astype(F32) + norm_back(x_ref[...].astype(F32), da)).astype(BF)

    stage(n, {BLOCKS + NT - 1: [sq.far2, sr.finish, sq.line, sq.finish]})


def back(q, k, v, do, lse, delta, at, x, dh, w, tables, grads, sq, sr):
    T, D = x.shape
    hbm = pl.BlockSpec(memory_space=pltpu.HBM)
    late = pl.BlockSpec((TB, D), lambda n: (jnp.maximum(n - BLOCKS, 0), 0))
    outs = sq.outs() + sr.outs()
    ins = (q, k, v, do, lse, delta, at)
    return pl.pallas_call(
        functools.partial(_back, sq=sq, sr=sr),
        grid=(BLOCKS + NT,),
        in_specs=[whole(a.shape) for a in ins] + [late, late, whole(w.shape), *(whole(t.shape) for t in tables)] + [hbm] * len(grads),
        out_specs=[late] + [whole(o.shape) for o in outs],
        out_shape=[jax.ShapeDtypeStruct((T, D), BF)] + outs,
        scratch_shapes=[pltpu.VMEM((G, HEAD, TB), F32), pltpu.VMEM((NT, TB, HEAD), F32), pltpu.VMEM((NT, TB, HEAD), F32),
                        pltpu.VMEM((NT, TB, 1024), BF), pltpu.VMEM(w.shape, F32), pltpu.VMEM((X, Y, 3, LINE, 1024), BF), sq.scratch(), sr.scratch()],
        compiler_params=pltpu.CompilerParams(dimension_semantics=("arbitrary",), vmem_limit_bytes=63 * 2**20, collective_id=2, has_side_effects=True),
        name="back",
    )(*ins, x, dh, w, *tables, *grads)


def _middle(x_ref, dy_ref, o_ref, wo_ref, wg_ref, wu_ref, wd_ref,
            dh_ref, do_ref, delta_ref, dwo_ref, dwg_ref, dwu_ref, dwd_ref,
            h_s, b_s, bt_s, db_s, ao, ag, au, ad, *, tb, nj, nt, strip):
    j, t = pl.program_id(0), pl.program_id(1)
    fj = wg_ref.shape[1]

    @pl.when(j == 0)
    def _():
        o = jnp.concatenate([o_ref[h] for h in range(G)], axis=1)
        h = (x_ref[...].astype(F32) + mm(o, wo_ref[...]).astype(BF).astype(F32)).astype(BF)
        h_s[t] = h
        b, _ = norm(h.astype(F32))
        b_s[t] = b
        bt_s[t] = b.T

    @pl.when(t == 0)
    def _():
        ag[...] = jnp.zeros_like(ag)
        au[...] = jnp.zeros_like(au)
        ad[...] = jnp.zeros_like(ad)

    dy = dy_ref[...]
    b, bt = b_s[t], bt_s[t]

    def into(cols):
        wg, wu, wd = wg_ref[:, cols], wu_ref[:, cols], wd_ref[cols, :]
        return mm(b, wg), mm(b, wu), mm_t(dy, wd)

    def point(gate, up, dact):
        dact = dact.astype(BF).astype(F32)
        sig = 0.5 + 0.5 * jnp.tanh(0.5 * gate)
        silu = gate * sig
        return (silu * up).astype(BF), (dact * up * (sig + silu * (1 - sig))).astype(BF), (dact * silu).astype(BF)

    dbs = []

    def out(cols, act, dgate, dup):
        dbs.append(mm_t(dgate, wg_ref[:, cols]) + mm_t(dup, wu_ref[:, cols]))
        ag[:, cols] += mm(bt, dgate)
        au[:, cols] += mm(bt, dup)
        ad[cols, :] += mm(act.T, dy)

    strips = [slice(s, s + strip) for s in range(0, fj, strip)]
    ahead = into(strips[0])
    for n, c in enumerate(strips):
        now, ahead = ahead, into(strips[n + 1]) if n + 1 < len(strips) else None
        out(c, *point(*now))
    db = sum(dbs[1:], dbs[0])

    @pl.when(j == 0)
    def _():
        db_s[t] = db

    @pl.when(j > 0)
    def _():
        db_s[t] += db

    @pl.when(t == nt - 1)
    def _():
        dwg_ref[...] = ag[...].astype(BF)
        dwu_ref[...] = au[...].astype(BF)
        dwd_ref[...] = ad[...].astype(BF)

    @pl.when(j == nj - 1)
    def _():
        dh = (dy.astype(F32) + norm_back(h_s[t].astype(F32), db_s[t]).astype(BF).astype(F32)).astype(BF)
        dh_ref[...] = dh
        do = mm_t(dh, wo_ref[...]).astype(BF)
        o = jnp.concatenate([o_ref[h] for h in range(G)], axis=1)
        prod = do.astype(F32) * o.astype(F32)
        for h in range(G):
            do_ref[h] = do[:, HEAD * h : HEAD * h + HEAD]
        delta_ref[...] = jnp.concatenate([prod[:, HEAD * h : HEAD * h + HEAD].sum(-1, keepdims=True) for h in range(G)]
                                         + [jnp.zeros((tb, 8 - G), F32)], axis=1).T
        part = mm(o.T, dh)

        @pl.when(t == 0)
        def _():
            ao[...] = part

        @pl.when(t > 0)
        def _():
            ao[...] += part

        @pl.when(t == nt - 1)
        def _():
            dwo_ref[...] = ao[...].astype(BF)


def middle(x, dy, o, wo, wg, wu, wd, tb=1024, nj=4, strip=256):
    T, D = x.shape
    F = wg.shape[1]
    nt, fj = T // tb, F // nj
    early = lambda j, t: jnp.where(j == 0, t, nt - 1)
    late = lambda j, t: jnp.where(j == nj - 1, t, 0)
    ends = lambda j, t: jnp.where(j == 0, t, jnp.where(j == nj - 1, t, nt - 1))
    once = dict(pipeline_mode=pl.Buffered(1))
    return pl.pallas_call(
        functools.partial(_middle, tb=tb, nj=nj, nt=nt, strip=strip),
        grid=(nj, nt),
        in_specs=[pl.BlockSpec((tb, D), lambda j, t: (early(j, t), 0)), pl.BlockSpec((tb, D), lambda j, t: (t, 0)),
                  pl.BlockSpec((G, tb, HEAD), lambda j, t: (0, ends(j, t), 0)), pl.BlockSpec(wo.shape, lambda j, t: (0, 0), **once),
                  pl.BlockSpec((D, fj), lambda j, t: (0, j)), pl.BlockSpec((D, fj), lambda j, t: (0, j)), pl.BlockSpec((fj, D), lambda j, t: (j, 0))],
        out_specs=[pl.BlockSpec((tb, D), lambda j, t: (late(j, t), 0)), pl.BlockSpec((G, tb, HEAD), lambda j, t: (0, late(j, t), 0)),
                   pl.BlockSpec((8, tb), lambda j, t: (0, late(j, t))), pl.BlockSpec(wo.shape, lambda j, t: (0, 0), **once),
                   pl.BlockSpec((D, fj), lambda j, t: (0, j)), pl.BlockSpec((D, fj), lambda j, t: (0, j)), pl.BlockSpec((fj, D), lambda j, t: (j, 0))],
        out_shape=[jax.ShapeDtypeStruct((T, D), BF), jax.ShapeDtypeStruct((G, T, HEAD), BF), jax.ShapeDtypeStruct((8, T), F32),
                   *(jax.ShapeDtypeStruct(a.shape, BF) for a in (wo, wg, wu, wd))],
        scratch_shapes=[pltpu.VMEM((nt, tb, D), BF), pltpu.VMEM((nt, tb, D), BF), pltpu.VMEM((nt, D, tb), BF),
                        pltpu.VMEM((nt, tb, D), F32),
                        pltpu.VMEM(wo.shape, F32), pltpu.VMEM((D, fj), F32), pltpu.VMEM((D, fj), F32), pltpu.VMEM((fj, D), F32)],
        compiler_params=pltpu.CompilerParams(dimension_semantics=("arbitrary", "arbitrary"), vmem_limit_bytes=67043328), name="middle",
    )(x, dy, o, wo, wg, wu, wd)


def _hand_over(*refs):
    half = len(refs) // 2
    for src, dst in zip(refs[:half], refs[half:]):
        dst[...] = src[...]


def hand_over(dx, small):
    T, D = dx.shape[1:]
    specs = [pl.BlockSpec((1, TB, D), lambda n: (0, n, 0))] + [whole(a.shape) for a in small]
    return pl.pallas_call(
        _hand_over, grid=(NT,), in_specs=specs, out_specs=specs, out_shape=[jax.ShapeDtypeStruct(a.shape, BF) for a in (dx, *small)],
        compiler_params=pltpu.CompilerParams(dimension_semantics=("arbitrary",)), name="hand_over",
    )(dx, *small)


def solution(mesh):
    gq, gr, sq, sr = Gather(*QKV, in_vmem=True), Gather(*REST), Scatter(*QKV, in_vmem=True), Scatter(*REST)

    def step(x, dy, *weights):
        x, dy = x[0], dy[0]
        T, D = x.shape
        tables = turn_tables(T)
        q, k, v, at, o, lse, w, *rest = front(x, tables, weights, gq, gr)
        rest = [a.reshape(D, -1) for a in rest[:3]] + [rest[3].reshape(-1, D)]
        dh, do, delta, *grads = middle(x, dy, o, *rest)
        grads = [g.reshape(X, Y, -1, LINE, g.shape[1]) for g in grads]
        dx, *by_w = back(q, k, v, do, lse, delta, at, x, dh, w.reshape(D, -1), tables, grads, sq, sr)
        return hand_over(dx[None], by_w)

    states, cut = P(("rep", "dp"), None, None), P(None, "dp", None)
    return jax.shard_map(
        step,
        mesh=mesh,
        in_specs=(states, states) + (cut,) * 7,
        out_specs=(states,) + (P("rep", "dp", None),) * 7,
        check_vma=False,
    )
```

```python
import functools

import jax
import jax.numpy as jnp
import numpy as np
from jax import lax
from jax.experimental import pallas as pl
from jax.experimental.pallas import tpu as pltpu
from jax.sharding import PartitionSpec as P


F32, BF = jnp.float32, jnp.bfloat16
X, Y, Z, C = 4, 4, 8, 2
LINE = Z * C
DMA = pltpu.SemaphoreType.DMA
ALL = slice(None)
BOTH = ((0, 1), (1, 3))


def place():
    me = lax.axis_index("dp")
    return me // (LINE * Y), lax.rem(me // LINE, Y), lax.rem(me, LINE), lax.rem(me, C)


def device(x, y, slot):
    return {"dp": (x * Y + y) * LINE + slot}


def on(a, k, n=4):
    return lax.rem(a + k, n)


def remote(src, dst, sems, where):
    send, recv = sems
    return pltpu.make_async_remote_copy(src_ref=src, dst_ref=dst, send_sem=send, recv_sem=recv, device_id=where, device_id_type=pl.DeviceIdType.MESH)


def start(copies):
    for cp in copies:
        cp.start()


def landed(copies):
    for cp in copies:
        cp.wait_recv()


def left(copies):
    for cp in copies:
        cp.wait_send()


def peers():
    x, y, slot, _ = place()
    who = [device(x, y, on(slot, k, LINE)) for k in range(1, LINE)]
    for _, k in BOTH:
        who += [device(on(x, k), y, slot), device(x, on(y, k), slot)]
    return who


def hello():
    for d in peers():
        pl.semaphore_signal(pltpu.get_barrier_semaphore(), inc=1, device_id=d, device_id_type=pl.DeviceIdType.MESH)


def meet():
    pl.semaphore_wait(pltpu.get_barrier_semaphore(), len(peers()))


def cols(first, size):
    return pl.ds(pl.multiple_of(first, 128), size)


def pair(sems, *index):
    return sems[0].at[index], sems[1].at[index]


class Ring:
    def __init__(self, along_x):
        x, y, slot, c = place()
        self.at = x if along_x else y
        self.to = lambda k: device(on(x, k), y, slot) if along_x else device(x, on(y, k), slot)


class Gather:
    def __init__(self, arrays, pieces, in_vmem=False):
        self.arrays, self.pieces, self.in_vmem = arrays, pieces, in_vmem

    def scratch(self):
        A, P = len(self.arrays), len(self.pieces)
        both = lambda *s: [DMA(s), DMA(s)]
        wide = [n if whole else n // 2 for _, n, _, whole in self.arrays]
        return dict(
            blocks=[pltpu.VMEM((LINE, a[0], w), BF) for a, w in zip(self.arrays, wide)],
            rows=[pltpu.VMEM((3 * LINE, w) if a[0] == 3 else (8, 128), BF) for a, w in zip(self.arrays, wide)],
            tall=pltpu.VMEM((3 * LINE, max(wide)), F32),
            own=DMA((sum(len(a[2]) for a in self.arrays),)), put=DMA((P,)), line=[DMA((LINE, sum(len(a[2]) for a in self.arrays))), DMA((A,))],
            near=both(P, 2), far=both(P, 2), near2=both(P, 2), far2=both(P, 2), over=both(P, 4),
        )

    def outs(self):
        return [jax.ShapeDtypeStruct((X, Y, 3 * LINE, a[1]) if a[0] == 3 else (X, Y, LINE, a[0], a[1]), BF) for a in self.arrays]

    def bind(self, ins, outs, s):
        self.ins, self.res, self.s = ins, outs, s
        self.spot = place()
        return self

    def _parts(self, slot, core):
        out = []
        for i, (r, width, parts, whole) in enumerate(self.arrays):
            for first, w in parts:
                src, dst = self.ins[len(out)].at[0], self.s["blocks"][i].at[slot]
                half = width // 2
                out.append((len(out), i, src, dst.at[:, pl.ds(first, w)]) if whole else (len(out), i, src.at[:, cols(core * half, half)], dst))
        return out

    def _line(self, do):
        x, y, slot, _ = self.spot

        def each(k, _):
            to = on(slot, k, LINE)
            do([remote(src, dst, (self.s["line"][0].at[k, n], self.s["line"][1].at[i]), device(x, y, to))
                for n, i, src, dst in self._parts(slot, lax.rem(to, C))])

        lax.fori_loop(1, LINE, each, None)

    def _own(self):
        _, _, slot, c = self.spot
        return [pltpu.make_async_copy(src, dst, self.s["own"].at[n]) for n, i, src, dst in self._parts(slot, c)]

    def down(self):
        self._line(start)
        start(self._own())

    def lay(self):
        for cp in self._own():
            cp.wait()
        for i, b in enumerate(self.s["blocks"]):
            some = b.at[pl.ds(0, LINE - 1)]
            pltpu.make_async_copy(some, some, self.s["line"][1].at[i]).wait()
        tall = self.s["tall"]
        for i, b in enumerate(self.s["blocks"]):
            if self.arrays[i][0] == 3:
                w = b.shape[2]
                for d in range(LINE):
                    tall[3 * d : 3 * d + 3, :w] = b[d].astype(F32)
                self.s["rows"][i][...] = tall[:, :w].astype(BF)

    def _view(self, i, lo, w, xs, ys, core, rows=ALL):
        at = cols(core * (self.arrays[i][1] // 2) + lo, w)
        if rows == slice(LINE, None) and self.arrays[i][0] == 3:
            rows = pl.ds(LINE, 2 * LINE)
        return self.res[i].at[xs, ys, rows, at] if self.arrays[i][0] == 3 else self.res[i].at[xs, ys, rows, :, at]

    def _half(self, i, k):
        n = LINE if self.arrays[i][0] == 3 else LINE // 2
        return slice(n, None) if k else slice(n)

    def _put(self):
        x, y, _, c = self.spot
        out = []
        for p, (i, lo, w, colour) in enumerate(self.pieces):
            r, n, _, whole = self.arrays[i]
            at = cols(c * (n // 2) + lo, w) if whole else pl.ds(lo, w)
            src = self.s["rows"][i].at[:, at] if r == 3 else self.s["blocks"][i].at[:, :, at]
            out.append((p, i, lo, w, colour, src))
        return out

    def _near(self, relay):
        x, y, _, c = self.spot
        copies = []
        for p, i, lo, w, colour, src in self._put():
            ring = Ring(colour == 1)
            for n, k in BOTH:
                if relay:
                    back = (on(x, 4 - k), y) if colour == 1 else (x, on(y, 4 - k))
                    v = self._view(i, lo, w, *back, c, self._half(i, n))
                    copies.append(remote(v, v, pair(self.s["near2"], p, n), ring.to(k)))
                else:
                    copies.append(remote(src, self._view(i, lo, w, x, y, c), pair(self.s["near"], p, n), ring.to(k)))
        return copies

    def _own_rows(self):
        x, y, _, c = self.spot
        return [pltpu.make_async_copy(src, self._view(i, lo, w, x, y, c), self.s["put"].at[p]) for p, i, lo, w, colour, src in self._put()]

    def near(self):
        start(self._near(False))
        if self.in_vmem:
            x, y, _, c = self.spot
            for rows, res in zip(self.s["rows"], self.res):
                n = rows.shape[1] // 2
                res[x, y, :, cols(c * n, n)] = rows[:, cols(c * n, n)]
        else:
            start(self._own_rows())

    def near2(self):
        landed(self._near(False))
        start(self._near(True))

    def _strip(self, i, lo, w, colour, k, core, half=ALL):
        x, y, _, _ = self.spot
        return self._view(i, lo, w, on(x, k), half, core) if colour == 0 else self._view(i, lo, w, half, on(y, k), core)

    def _far(self, relay):
        c, copies = self.spot[3], []
        for p, (i, lo, w, colour) in enumerate(self.pieces):
            ring = Ring(colour == 0)
            for n, k in BOTH:
                v = self._strip(i, lo, w, colour, 4 - k if relay else 0, c, slice(2 * n, 2 * n + 2) if relay else ALL)
                copies.append(remote(v, v, pair(self.s["far2" if relay else "far"], p, n), ring.to(k)))
        return copies

    def _over(self, ks):
        x, y, slot, c = self.spot
        copies = []
        for k in ks:
            for p, (i, lo, w, colour) in enumerate(self.pieces):
                v = self._strip(i, lo, w, colour, k, c)
                copies.append(remote(v, v, pair(self.s["over"], p, k), device(x, y, slot + 1 - 2 * c)))
        return copies

    def far(self):
        if not self.in_vmem:
            for cp in self._own_rows():
                cp.wait()
        landed(self._near(True))
        start(self._far(False))
        start(self._over([0]))

    def far2(self):
        landed(self._far(False))
        start(self._far(True))
        start(self._over([1, 3]))

    def over(self):
        landed(self._far(True))
        start(self._over([2]))

    def finish(self):
        landed(self._over(range(4)))
        self._line(left)
        for copies in (self._near(False), self._near(True), self._far(False), self._far(True), self._over(range(4))):
            left(copies)

    def steps(self):
        return [self.down, self.lay, self.near, self.near2, self.far, self.far2, self.over, self.finish]


class Scatter:
    def __init__(self, arrays, pieces, in_vmem=False):
        self.arrays, self.pieces, self.in_vmem = arrays, pieces, in_vmem

    def scratch(self):
        P = len(self.pieces)
        both = lambda *s: [DMA(s), DMA(s)]
        per = lambda *lead: [pltpu.VMEM((*lead, self._m(i), LINE, w), BF) for i, lo, w, _ in self.pieces]
        half = [pltpu.VMEM((2, 2, self._m(i), LINE, w), BF) for i, lo, w, _ in self.pieces]
        return dict(
            own=per(X, Y), other=per(X, Y), h1=half, f1=per(2, 4), t=per(4),
            h2=per(), f2=per(2),
            zs=[pltpu.VMEM((LINE, a[0], a[1] // 2), BF) for a in self.arrays], zr=[pltpu.VMEM((LINE, a[0], a[1] // 2), BF) for a in self.arrays],
            get=DMA((P,)), over=both(P), a=both(P, 2), a2=both(P, 2), b=both(P, 2), b2=both(P, 2),
            line=[DMA((LINE, len(self.arrays))), DMA((len(self.arrays),))],
        )

    def _m(self, i):
        return 3 if self.arrays[i][0] == 3 else LINE // 2

    def _parts(self, i):
        h = self._m(i) // 2
        return pl.ds(0, h), pl.ds(h, self._m(i) - h)

    def outs(self):
        return [jax.ShapeDtypeStruct((1, a[0], w), BF) for a in self.arrays for _, w in a[2]]

    def bind(self, ins, outs, s):
        self.ins, self.res, self.s = ins, outs, s
        self.spot = place()
        return self

    def _each(self):
        return [(p, i, lo, w, colour) for p, (i, lo, w, colour) in enumerate(self.pieces)]

    def _view(self, i, lo, w, core):
        return self.ins[i].at[:, :, :, :, cols(core * (self.arrays[i][1] // 2) + lo, w)]

    def _over(self):
        x, y, slot, c = self.spot
        return [remote(self._view(i, lo, w, 1 - c), self.s["other"][p], pair(self.s["over"], p), device(x, y, slot + 1 - 2 * c))
                for p, i, lo, w, colour in self._each()]

    def _get(self):
        return [pltpu.make_async_copy(self._view(i, lo, w, self.spot[3]), self.s["own"][p], self.s["get"].at[p]) for p, i, lo, w, colour in self._each()]

    def down(self):
        start(self._over())
        if not self.in_vmem:
            start(self._get())

    def _target(self, p, colour, k):
        x, y, _, _ = self.spot
        own = self.s["own"][p]
        return own.at[on(x, k)] if colour == 0 else own.at[:, on(y, k)]

    def _a(self):
        copies = []
        for p, i, lo, w, colour in self._each():
            for n, k in BOTH:
                copies.append(remote(self._target(p, colour, 2).at[pl.ds(2 * n, 2)], self.s["h1"][p].at[n], pair(self.s["a"], p, n), Ring(colour == 0).to(k)))
        return copies

    def _a2(self):
        return [remote(self._target(p, colour, k), self.s["f1"][p].at[n], pair(self.s["a2"], p, n), Ring(colour == 0).to(k))
                for p, i, lo, w, colour in self._each() for n, k in BOTH]

    def _of(self, copies, p):
        return [copies[2 * p], copies[2 * p + 1]]

    def near(self):
        over, a = self._over(), self._a()
        get = None if self.in_vmem else self._get()
        for p, i, lo, w, colour in self._each():
            if get:
                get[p].wait()
            over[p].wait_recv()
            own, other = self.s["own"][p], self.s["other"][p]
            mine = self._view(i, lo, w, self.spot[3]) if self.in_vmem else own

            def add(n, _):
                at = n // Y, lax.rem(n, Y)
                own[at] = (mine[at].astype(F32) + other[at].astype(F32)).astype(BF)

            lax.fori_loop(0, X * Y, add, None)
            start(self._of(a, p))

    def near2(self):
        a, a2 = self._a(), self._a2()
        for p, i, lo, w, colour in self._each():
            landed(self._of(a, p))
            for n, k in BOTH:
                to, h = self._target(p, colour, k), self.s["h1"][p]
                for q in range(2):
                    to[2 * n + q] = (to[2 * n + q].astype(F32) + h[n, q].astype(F32)).astype(BF)
            start(self._of(a2, p))

    def _b(self):
        copies = []
        x, y, _, _ = self.spot
        for p, i, lo, w, colour in self._each():
            ring = Ring(colour == 1)
            for (n, k), part in zip(BOTH, self._parts(i)):
                copies.append(remote(self.s["t"][p].at[on(ring.at, 2), part], self.s["h2"][p].at[part], pair(self.s["b"], p, n), ring.to(k)))
        return copies

    def _b2(self):
        copies = []
        for p, i, lo, w, colour in self._each():
            ring = Ring(colour == 1)
            copies += [remote(self.s["t"][p].at[on(ring.at, k)], self.s["f2"][p].at[n], pair(self.s["b2"], p, n), ring.to(k)) for n, k in BOTH]
        return copies

    def far(self):
        a2, b = self._a2(), self._b()
        for p, i, lo, w, colour in self._each():
            landed(self._of(a2, p))
            own, f, t = self._target(p, colour, 0), self.s["f1"][p], self.s["t"][p]

            def add(n, _):
                t[n] = (own[n].astype(F32) + f[0, n].astype(F32) + f[1, n].astype(F32)).astype(BF)

            lax.fori_loop(0, 4, add, None)
            start(self._of(b, p))

    def far2(self):
        b, b2 = self._b(), self._b2()
        for p, i, lo, w, colour in self._each():
            landed(self._of(b, p))
            ring, t = Ring(colour == 1), self.s["t"][p]
            for (_, k), part in zip(BOTH, self._parts(i)):
                at = on(ring.at, k), part
                t[at] = (t[at].astype(F32) + self.s["h2"][p][part].astype(F32)).astype(BF)
            start(self._of(b2, p))

    def _line(self, do):
        x, y, slot, _ = self.spot

        def each(k, _):
            to = on(slot, k, LINE)
            do([remote(zs.at[to], zr.at[slot], (self.s["line"][0].at[k, i], self.s["line"][1].at[i]), device(x, y, to))
                for i, (zs, zr) in enumerate(zip(self.s["zs"], self.s["zr"]))])

        lax.fori_loop(1, LINE, each, None)

    def line(self):
        b2, slot = self._b2(), self.spot[2]
        for p, i, lo, w, colour in self._each():
            landed(self._of(b2, p))
            f = self.s["f2"][p]
            total = self.s["t"][p][Ring(colour == 1).at].astype(F32) + f[0].astype(F32) + f[1].astype(F32)
            zs = self.s["zs"][i]
            if self.arrays[i][0] == 3:
                total = total.reshape(3 * LINE, w)
                for d in range(LINE):
                    zs[d, :, lo : lo + w] = total[3 * d : 3 * d + 3].astype(BF)
            else:
                zs[:, :, lo : lo + w] = total.reshape(LINE, -1, w).astype(BF)
        self._line(start)
        for zs, zr in zip(self.s["zs"], self.s["zr"]):
            zr[slot] = zs[slot]

    def finish(self):
        n = 0
        for i, (r, width, parts, _) in enumerate(self.arrays):
            zr = self.s["zr"][i]
            some = zr.at[pl.ds(0, LINE - 1)]
            pltpu.make_async_copy(some, some, self.s["line"][1].at[i]).wait()
            sums = []
            for core in range(C):
                total = zr[core].astype(F32)
                for k in range(1, Z):
                    total += zr[C * k + core].astype(F32)
                sums.append(total.astype(BF))
            whole = jnp.concatenate(sums, axis=1)
            for first, w in parts:
                self.res[n][0] = whole[:, first : first + w]
                n += 1
        self._line(left)
        for copies in (self._over(), self._a(), self._a2(), self._b(), self._b2()):
            left(copies)

    def steps(self):
        return [self.down, self.near, self.near2, self.far, self.far2, self.line, self.finish]


QKV = ([(3, 1024, [(0, 768), (768, 128), (896, 128)], True)], [(0, 0, 256, 0), (0, 256, 256, 1)])
REST = (
    [(3, 768, [(0, 768)], False), (3, 2048, [(0, 2048)], False), (3, 2048, [(0, 2048)], False), (8, 768, [(0, 768)], False)],
    [(1, 0, 1024, 0), (2, 0, 1024, 1), (0, 0, 384, 0), (3, 0, 128, 0), (3, 128, 256, 1)],
)


HEAD, THETA = 128, 10000
NAMES = ("wq", "wk", "wv", "wo", "w_gate", "w_up", "w_down")
G = 6
TB = 512
NT = 4
BLOCKS = NT * (NT + 1) // 2
NEG = -1e30
HIDDEN = 2 * NEG
LOG2E = 1.4426950408889634
VMEM = 56 * 2**20
EPS = 1e-6


def mm(a, b):
    return lax.dot_general(a, b, (((1,), (0,)), ((), ())), preferred_element_type=F32)


def mm_t(a, b):
    return lax.dot_general(a, b, (((1,), (1,)), ((), ())), preferred_element_type=F32)


def norm(h):
    scale = lax.rsqrt(jnp.mean(h * h, -1, keepdims=True) + EPS)
    return (h * scale).astype(BF), scale


def norm_back(h, g):
    scale = lax.rsqrt(jnp.mean(h * h, -1, keepdims=True) + EPS)
    return scale * (g - h * (scale * scale * jnp.mean(g * h, -1, keepdims=True)))


def turn_tables(tokens):
    half = HEAD // 2
    freq = np.float64(THETA) ** (-np.arange(half) / half)
    freq = np.concatenate([freq, freq])
    far = 128.0 * np.arange(tokens // 128)[:, None] * freq
    near = np.arange(128.0)[:, None] * freq
    return [jnp.asarray(t.astype(np.float32)) for t in (np.cos(far), np.sin(far), np.cos(near), np.sin(near))]


def turners(tables, n):
    ca, sa, cb, sb = tables
    row = pl.ds(n, 1)
    fc, fs = ca[row, :], sa[row, :]
    cos = fc * cb[...] - fs * sb[...]
    sin = fs * cb[...] + fc * sb[...]
    lane = lax.broadcasted_iota(jnp.int32, sin.shape, 1)
    return cos, jnp.where(lane < HEAD // 2, -sin, sin)


def swap(t):
    return pltpu.roll(t, HEAD // 2, 1)


def whole(shape):
    return pl.BlockSpec(shape, lambda *_: (0,) * len(shape))


def stage(n, plan):
    for at, todo in plan.items():

        @pl.when(n == at)
        def _():
            for do in todo:
                do()


def block_of(m):
    i = sum((m >= (r * (r + 1)) // 2).astype(jnp.int32) for r in range(1, NT))
    return i, m - (i * (i + 1)) // 2


def rows(b, size=TB, first=0):
    return pl.ds(pl.multiple_of(b * TB + first, HEAD), size)


def wait(copies):
    for cp in copies:
        cp.wait()


HALVES = ((0, 0), (TB // 2, TB // 2))


def masked(s, key, query):
    return lax.broadcasted_iota(jnp.int32, s.shape, 0) + key <= lax.broadcasted_iota(jnp.int32, s.shape, 1) + query


def _front(x_ref, ca, sa, cb, sb, *rest, gq, gr):
    weights, rest = rest[: len(NAMES)], rest[len(NAMES) :]
    lse_ref, hbm, (outs, (ours, vt_s, top_s, mix_s, w_s, sems, o_sem, sq, sr)) = rest[0], rest[1:6], (rest[6:11], rest[11:])
    q_s, k_s, v_s, at_s, o_s, x_s = ours
    n = pl.program_id(0)
    gq.bind(weights[:3], (w_s,), sq)
    gr.bind(weights[3:], outs[1:], sr)
    fetch = pltpu.make_async_copy(x_ref, x_s, sems.at[5])
    keep = [pltpu.make_async_copy(a, b, sems.at[m]) for m, (a, b) in enumerate(zip((q_s, k_s, v_s, at_s, w_s), (*hbm[:4], outs[0])))]
    o_out = lambda b: pltpu.make_async_copy(o_s.at[:, rows(b)], hbm[4].at[:, rows(b)], o_sem.at[b])

    def normed(first, last):
        for b in range(first, last):
            at = slice(b * TB, b * TB + TB)
            a, _ = norm(x_s[at, :].astype(F32))
            x_s[at, :] = a
            at_s[:, at] = a.T

    def early():
        fetch.wait()
        normed(0, NT // 2)

    def late():
        normed(NT // 2, NT)

    def keep_all():
        start(keep)

    stage(n, {
        0: [fetch.start, hello, early, meet, gq.down, gr.down, late, gq.lay, gq.near, gq.near2, gr.lay, gr.near, gq.far, gq.far2, gr.near2, gq.over,
            gq.finish, gr.far],
        NT: [keep_all],
        8: [gr.far2],
        12: [gr.over],
    })

    @pl.when(n < NT)
    def _():
        a = x_s[rows(n), :]
        y = mm(a, w_s[...].reshape(a.shape[1], -1)).astype(BF)
        for i in range(TB // HEAD):
            here, there = slice(HEAD * i, HEAD * i + HEAD), rows(n, HEAD, HEAD * i)
            cos, sin = turners((ca, sa, cb, sb), n * (TB // HEAD) + i)
            for h in range(G + 1):
                t = y[here, HEAD * h : HEAD * h + HEAD].astype(F32)
                t = (t * cos + swap(t) * sin).astype(BF)
                if h < G:
                    q_s[h, there, :] = t
                else:
                    k_s[there, :] = t
        v = y[:, (G + 1) * HEAD :]
        v_s[rows(n), :] = v
        vt_s[n] = jnp.concatenate([v.T, jnp.ones((8, TB), BF)], axis=0)

    i, j = block_of(n - NT)
    e = HEAD**-0.5 * LOG2E

    @pl.when((n >= NT) & (j == 0))
    def _():
        top_s[...] = jnp.full(top_s.shape, NEG, F32)
        mix_s[...] = jnp.zeros(mix_s.shape, F32)

    def block(key, keys, query, mask):
        k = k_s[rows(j, keys, key), :]
        scores = [mm_t(k, q_s[h, rows(i, TB - query, query), :]) for h in range(G)]
        weights, keeps = [], []
        for h, s in enumerate(scores):
            if mask:
                s = jnp.where(masked(s, key, query), s, HIDDEN)
            old = top_s[h : h + 1, query:]
            top = jnp.maximum(old, s.max(axis=0, keepdims=True))
            top_s[h : h + 1, query:] = top
            weights.append(jnp.exp2((s - top) * e).astype(BF))
            keeps.append(jnp.exp2((old - top) * e))
        for h in range(G):
            mix_s[h, :, query:] = mix_s[h, :, query:] * keeps[h] + mm(vt_s[j, :, key : key + keys], weights[h])

    @pl.when((n >= NT) & (j < i))
    def _():
        block(0, TB, 0, False)

    @pl.when((n >= NT) & (j == i))
    def _():
        for key, query in HALVES:
            block(key, TB // 2, query, True)
        for h in range(G):
            total = mix_s[h, HEAD : HEAD + 1, :]
            o_s[h, rows(i), :] = (mix_s[h, :HEAD, :] * (1 / total)).T.astype(BF)
            lse_ref[h : h + 1, rows(i)] = top_s[h : h + 1, :] * HEAD**-0.5 + jnp.log(total)
        o_out(i).start()

    def finish():
        gr.finish()
        wait(keep)
        wait([o_out(b) for b in range(NT)])

    stage(n, {NT + BLOCKS - 1: [finish]})


def front(x, tables, weights, gq, gr):
    T, D = x.shape
    hbm = pl.BlockSpec(memory_space=pltpu.HBM)
    mine = [(G, T, HEAD), (T, HEAD), (T, HEAD), (D, T), (G, T, HEAD)]
    return pl.pallas_call(
        functools.partial(_front, gq=gq, gr=gr),
        grid=(NT + BLOCKS,),
        in_specs=[hbm, *(whole(t.shape) for t in tables)] + [hbm] * len(weights),
        out_specs=[whole((8, T))] + [hbm] * (len(mine) + 5),
        out_shape=[jax.ShapeDtypeStruct((8, T), F32)] + [jax.ShapeDtypeStruct(s, BF) for s in mine] + gq.outs() + gr.outs(),
        scratch_shapes=[[pltpu.VMEM(s, BF) for s in (*mine, (T, D))], pltpu.VMEM((NT, HEAD + 8, TB), BF), pltpu.VMEM((8, TB), F32),
                        pltpu.VMEM((G, HEAD + 8, TB), F32), pltpu.VMEM((X, Y, 3 * LINE, 1024), BF), DMA((6,)), DMA((NT,)), gq.scratch(), gr.scratch()],
        compiler_params=pltpu.CompilerParams(dimension_semantics=("arbitrary",), vmem_limit_bytes=VMEM, collective_id=1, has_side_effects=True),
        name="front",
    )(x, *tables, *weights)


def _back(lse_ref, delta_ref, x_ref, dh_ref, ca, sa, cb, sb, *rest, sq, sr):
    hbm, w_hbm, grads, dx_ref, outs, rest = rest[:5], rest[5], rest[6:10], rest[10], rest[11:18], rest[18:]
    ours, w_s, sems, w_sem, dq_s, dk_s, dv_s, d_s, acc, dw_s, rq, rr = rest
    q_s, do_s, k_s, v_s, at_s = ours
    n = pl.program_id(0)
    sq.bind((dw_s,), outs[:3], rq)
    sr.bind(grads, outs[3:], rr)

    def fetch(b):
        at = [(ALL, rows(b)), (ALL, rows(b)), (rows(b),), (rows(b),), (ALL, rows(b))]
        return [pltpu.make_async_copy(src.at[a], dst.at[a], sems.at[m, b]) for m, (src, dst, a) in enumerate(zip(hbm, ours, at))]

    w_in = pltpu.make_async_copy(w_hbm, w_s, w_sem)

    def fetch_all():
        for b in range(NT):
            start(fetch(b))
        w_in.start()

    i, j = block_of(n)
    stage(n, {0: [hello, fetch_all]})

    @pl.when((n < BLOCKS) & (j == 0))
    def _():
        wait(fetch(i))

    stage(n, {1: [meet, sr.down], 3: [sr.near], 5: [sr.near2], 9: [sr.far]})
    scale = HEAD**-0.5
    e = scale * LOG2E

    @pl.when(n == 0)
    def _():
        dk_s[...] = jnp.zeros_like(dk_s)
        dv_s[...] = jnp.zeros_like(dv_s)
        acc[...] = jnp.zeros_like(acc)

    @pl.when((n < BLOCKS) & (j == 0))
    def _():
        dq_s[...] = jnp.zeros_like(dq_s)

    def block(key, keys, query, mask):
        here, there = rows(j, keys, key), rows(i, TB - query, query)
        k, v = k_s[here, :], v_s[here, :]
        kt = k.T
        qs = [q_s[h, there, :] for h in range(G)]
        dos = [do_s[h, there, :] for h in range(G)]
        scores = [mm_t(k, q) for q in qs]
        dps = [mm_t(v, do) for do in dos]
        for h in range(G):
            p = jnp.exp2(scores[h] * e - lse_ref[h : h + 1, there] * LOG2E)
            if mask:
                p = jnp.where(masked(p, key, query), p, 0.0)
            ds = (p * (dps[h] - delta_ref[h : h + 1, there])).astype(BF)
            dv_s[j, key : key + keys] += mm(p.astype(BF), dos[h])
            dk_s[j, key : key + keys] += mm(ds, qs[h])
            dq_s[h, :, query:] += mm(kt, ds)

    def turn_back(t, b, r):
        cos, sin = turners((ca, sa, cb, sb), b * (TB // HEAD) + r)
        t = t[HEAD * r : HEAD * r + HEAD].astype(F32)
        return (t * cos - swap(t) * sin).astype(BF)

    @pl.when((n < BLOCKS) & (j < i))
    def _():
        block(0, TB, 0, False)

    @pl.when((n < BLOCKS) & (j == i))
    def _():
        for key, query in HALVES:
            block(key, TB // 2, query, True)
        for h in range(G):
            dq = (dq_s[h] * scale).T.astype(BF)
            for r in range(TB // HEAD):
                d_s[i, HEAD * r : HEAD * r + HEAD, HEAD * h : HEAD * h + HEAD] = turn_back(dq, i, r)
        acc[:, : G * HEAD] += mm(at_s[:, rows(i)], d_s[i, :, : G * HEAD])

    def last():
        for b in range(NT):
            dk = (dk_s[b] * scale).astype(BF)
            for r in range(TB // HEAD):
                d_s[b, HEAD * r : HEAD * r + HEAD, G * HEAD : (G + 1) * HEAD] = turn_back(dk, b, r)
            d_s[b, :, (G + 1) * HEAD :] = dv_s[b].astype(BF)
            acc[:, G * HEAD :] += mm(at_s[:, rows(b)], d_s[b, :, G * HEAD :])
        dw_s[...] = acc[...].astype(BF).reshape(dw_s.shape)

    stage(n, {BLOCKS: [sr.far2, last, sq.down, w_in.wait], BLOCKS + 1: [sq.near], BLOCKS + 2: [sr.line, sq.near2], BLOCKS + 3: [sq.far]})

    @pl.when(n >= BLOCKS)
    def _():
        da = mm_t(d_s[n - BLOCKS], w_s[...])
        dx_ref[...] = (dh_ref[...].astype(F32) + norm_back(x_ref[...].astype(F32), da)).astype(BF)

    stage(n, {BLOCKS + NT - 1: [sq.far2, sr.finish, sq.line, sq.finish]})


def back(q, k, v, do, lse, delta, at, x, dh, w, tables, grads, sq, sr):
    T, D = x.shape
    hbm = pl.BlockSpec(memory_space=pltpu.HBM)
    late = pl.BlockSpec((TB, D), lambda n: (jnp.maximum(n - BLOCKS, 0), 0))
    outs = sq.outs() + sr.outs()
    ins = (q, do, k, v, at)
    return pl.pallas_call(
        functools.partial(_back, sq=sq, sr=sr),
        grid=(BLOCKS + NT,),
        in_specs=[whole(lse.shape), whole(delta.shape), late, late, *(whole(t.shape) for t in tables)] + [hbm] * (len(ins) + 1 + len(grads)),
        out_specs=[late] + [whole(o.shape) for o in outs],
        out_shape=[jax.ShapeDtypeStruct((T, D), BF)] + outs,
        scratch_shapes=[[pltpu.VMEM(a.shape, BF) for a in ins], pltpu.VMEM(w.shape, BF), DMA((len(ins), NT)), DMA(()),
                        pltpu.VMEM((G, HEAD, TB), F32), pltpu.VMEM((NT, TB, HEAD), F32), pltpu.VMEM((NT, TB, HEAD), F32),
                        pltpu.VMEM((NT, TB, 1024), BF), pltpu.VMEM(w.shape, F32), pltpu.VMEM((X, Y, 3, LINE, 1024), BF), sq.scratch(), sr.scratch()],
        compiler_params=pltpu.CompilerParams(dimension_semantics=("arbitrary",), vmem_limit_bytes=63 * 2**20, collective_id=2, has_side_effects=True),
        name="back",
    )(lse, delta, x, dh, *tables, *ins, w, *grads)


def _middle(x_ref, dy_ref, o_ref, wo_ref, wg_ref, wu_ref, wd_ref,
            dh_ref, do_ref, delta_ref, dwo_ref, dwg_ref, dwu_ref, dwd_ref,
            h_s, b_s, bt_s, db_s, ao, ag, au, ad, *, tb, nj, nt, strip):
    j, t = pl.program_id(0), pl.program_id(1)
    fj = wg_ref.shape[1]

    def halves(do):
        lax.fori_loop(0, tb // TB, lambda r, _: do(rows(r)), None)

    @pl.when(j == 0)
    def _():
        @halves
        def _(at):
            o = jnp.concatenate([o_ref[h, at, :] for h in range(G)], axis=1)
            h = (x_ref[at, :].astype(F32) + mm(o, wo_ref[...]).astype(BF).astype(F32)).astype(BF)
            h_s[t, at, :] = h
            b, _ = norm(h.astype(F32))
            b_s[t, at, :] = b
            bt_s[t, :, at] = b.T

    @pl.when(t == 0)
    def _():
        ag[...] = jnp.zeros_like(ag)
        au[...] = jnp.zeros_like(au)
        ad[...] = jnp.zeros_like(ad)

    dy = dy_ref[...]
    b, bt = b_s[t], bt_s[t]

    def into(cols):
        wg, wu, wd = wg_ref[:, cols], wu_ref[:, cols], wd_ref[cols, :]
        return mm(b, wg), mm(b, wu), mm_t(dy, wd)

    def point(gate, up, dact):
        dact = dact.astype(BF).astype(F32)
        sig = 0.5 + 0.5 * jnp.tanh(0.5 * gate)
        silu = gate * sig
        return (silu * up).astype(BF), (dact * up * (sig + silu * (1 - sig))).astype(BF), (dact * silu).astype(BF)

    dbs = []

    def out(cols, act, dgate, dup):
        dbs.append(mm_t(dgate, wg_ref[:, cols]) + mm_t(dup, wu_ref[:, cols]))
        ag[:, cols] += mm(bt, dgate)
        au[:, cols] += mm(bt, dup)
        ad[cols, :] += mm(act.T, dy)

    strips = [slice(s, s + strip) for s in range(0, fj, strip)]
    ahead = into(strips[0])
    for n, c in enumerate(strips):
        now, ahead = ahead, into(strips[n + 1]) if n + 1 < len(strips) else None
        out(c, *point(*now))
    db = sum(dbs[1:], dbs[0])

    @pl.when(j == 0)
    def _():
        db_s[t] = db

    @pl.when(j > 0)
    def _():
        db_s[t] += db

    @pl.when(t == nt - 1)
    def _():
        dwg_ref[...] = ag[...].astype(BF)
        dwu_ref[...] = au[...].astype(BF)
        dwd_ref[...] = ad[...].astype(BF)

    @pl.when((j == nj - 1) & (t == 0))
    def _():
        ao[...] = jnp.zeros_like(ao)

    @pl.when(j == nj - 1)
    def _():
        @halves
        def _(at):
            dh = (dy_ref[at, :].astype(F32) + norm_back(h_s[t, at, :].astype(F32), db_s[t, at, :]).astype(BF).astype(F32)).astype(BF)
            dh_ref[at, :] = dh
            do = mm_t(dh, wo_ref[...]).astype(BF)
            o = jnp.concatenate([o_ref[h, at, :] for h in range(G)], axis=1)
            prod = do.astype(F32) * o.astype(F32)
            for h in range(G):
                do_ref[h, at, :] = do[:, HEAD * h : HEAD * h + HEAD]
            delta_ref[:, at] = jnp.concatenate([prod[:, HEAD * h : HEAD * h + HEAD].sum(-1, keepdims=True) for h in range(G)]
                                               + [jnp.zeros((TB, 8 - G), F32)], axis=1).T
            ao[...] += mm(o.T, dh)

        @pl.when(t == nt - 1)
        def _():
            dwo_ref[...] = ao[...].astype(BF)


def middle(x, dy, o, wo, wg, wu, wd, tb=1024, nj=4, strip=256):
    T, D = x.shape
    F = wg.shape[1]
    nt, fj = T // tb, F // nj
    early = lambda j, t: jnp.where(j == 0, t, nt - 1)
    late = lambda j, t: jnp.where(j == nj - 1, t, 0)
    ends = lambda j, t: jnp.where(j == 0, t, jnp.where(j == nj - 1, t, nt - 1))
    once = dict(pipeline_mode=pl.Buffered(1))
    return pl.pallas_call(
        functools.partial(_middle, tb=tb, nj=nj, nt=nt, strip=strip),
        grid=(nj, nt),
        in_specs=[pl.BlockSpec((tb, D), lambda j, t: (early(j, t), 0)), pl.BlockSpec((tb, D), lambda j, t: (t, 0)),
                  pl.BlockSpec((G, tb, HEAD), lambda j, t: (0, ends(j, t), 0)), pl.BlockSpec(wo.shape, lambda j, t: (0, 0), **once),
                  pl.BlockSpec((D, fj), lambda j, t: (0, j)), pl.BlockSpec((D, fj), lambda j, t: (0, j)), pl.BlockSpec((fj, D), lambda j, t: (j, 0))],
        out_specs=[pl.BlockSpec((tb, D), lambda j, t: (late(j, t), 0)), pl.BlockSpec((G, tb, HEAD), lambda j, t: (0, late(j, t), 0)),
                   pl.BlockSpec((8, tb), lambda j, t: (0, late(j, t))), pl.BlockSpec(wo.shape, lambda j, t: (0, 0), **once),
                   pl.BlockSpec((D, fj), lambda j, t: (0, j)), pl.BlockSpec((D, fj), lambda j, t: (0, j)), pl.BlockSpec((fj, D), lambda j, t: (j, 0))],
        out_shape=[jax.ShapeDtypeStruct((T, D), BF), jax.ShapeDtypeStruct((G, T, HEAD), BF), jax.ShapeDtypeStruct((8, T), F32),
                   *(jax.ShapeDtypeStruct(a.shape, BF) for a in (wo, wg, wu, wd))],
        scratch_shapes=[pltpu.VMEM((nt, tb, D), BF), pltpu.VMEM((nt, tb, D), BF), pltpu.VMEM((nt, D, tb), BF),
                        pltpu.VMEM((nt, tb, D), F32),
                        pltpu.VMEM(wo.shape, F32), pltpu.VMEM((D, fj), F32), pltpu.VMEM((D, fj), F32), pltpu.VMEM((fj, D), F32)],
        compiler_params=pltpu.CompilerParams(dimension_semantics=("arbitrary", "arbitrary"), vmem_limit_bytes=67043328), name="middle",
    )(x, dy, o, wo, wg, wu, wd)


def _hand_over(*refs):
    half = len(refs) // 2
    for src, dst in zip(refs[:half], refs[half:]):
        dst[...] = src[...]


def hand_over(dx, small):
    T, D = dx.shape[1:]
    specs = [pl.BlockSpec((1, TB, D), lambda n: (0, n, 0))] + [whole(a.shape) for a in small]
    return pl.pallas_call(
        _hand_over, grid=(NT,), in_specs=specs, out_specs=specs, out_shape=[jax.ShapeDtypeStruct(a.shape, BF) for a in (dx, *small)],
        compiler_params=pltpu.CompilerParams(dimension_semantics=("arbitrary",)), name="hand_over",
    )(dx, *small)


def solution(mesh):
    gq, gr, sq, sr = Gather(*QKV, in_vmem=True), Gather(*REST), Scatter(*QKV, in_vmem=True), Scatter(*REST)

    def step(x, dy, *weights):
        x, dy = x[0], dy[0]
        T, D = x.shape
        tables = turn_tables(T)
        lse, q, k, v, at, o, w, *rest = front(x, tables, weights, gq, gr)
        rest = [a.reshape(D, -1) for a in rest[:3]] + [rest[3].reshape(-1, D)]
        dh, do, delta, *grads = middle(x, dy, o, *rest)
        grads = [g.reshape(X, Y, -1, LINE, g.shape[1]) for g in grads]
        dx, *by_w = back(q, k, v, do, lse, delta, at, x, dh, w.reshape(D, -1), tables, grads, sq, sr)
        return hand_over(dx[None], by_w)

    states, cut = P(("rep", "dp"), None, None), P(None, "dp", None)
    return jax.shard_map(
        step,
        mesh=mesh,
        in_specs=(states, states) + (cut,) * 7,
        out_specs=(states,) + (P("rep", "dp", None),) * 7,
        check_vma=False,
    )
```

```python
import functools

import jax
import jax.numpy as jnp
import numpy as np
from jax import lax
from jax.experimental import pallas as pl
from jax.experimental.pallas import tpu as pltpu
from jax.sharding import PartitionSpec as P


F32, BF = jnp.float32, jnp.bfloat16
X, Y, Z, C = 4, 4, 8, 2
LINE = Z * C
DMA = pltpu.SemaphoreType.DMA
THIN = 3
TALL = THIN * LINE
WIDTH, HIDDEN_UNITS, HEAD = 768, 2048, 128
ALL = slice(None)
BOTH = ((0, 1), (1, 3))


def place():
    me = lax.axis_index("dp")
    return me // (LINE * Y), lax.rem(me // LINE, Y), lax.rem(me, LINE), lax.rem(me, C)


def device(x, y, slot):
    return {"dp": (x * Y + y) * LINE + slot}


def on(a, k, n=4):
    return lax.rem(a + k, n)


def remote(src, dst, sems, where):
    send, recv = sems
    return pltpu.make_async_remote_copy(src_ref=src, dst_ref=dst, send_sem=send, recv_sem=recv, device_id=where, device_id_type=pl.DeviceIdType.MESH)


def start(copies):
    for cp in copies:
        cp.start()


def landed(copies):
    for cp in copies:
        cp.wait_recv()


def left(copies):
    for cp in copies:
        cp.wait_send()


def peers():
    x, y, slot, _ = place()
    who = [device(x, y, on(slot, k, LINE)) for k in range(1, LINE)]
    for _, k in BOTH:
        who += [device(on(x, k), y, slot), device(x, on(y, k), slot)]
    return who


def hello():
    for d in peers():
        pl.semaphore_signal(pltpu.get_barrier_semaphore(), inc=1, device_id=d, device_id_type=pl.DeviceIdType.MESH)


def meet():
    pl.semaphore_wait(pltpu.get_barrier_semaphore(), len(peers()))


def cols(first, size):
    return pl.ds(pl.multiple_of(first, 128), size)


def pair(sems, *index):
    return sems[0].at[index], sems[1].at[index]


class Ring:
    def __init__(self, along_x):
        x, y, slot, c = place()
        self.at = x if along_x else y
        self.to = lambda k: device(on(x, k), y, slot) if along_x else device(x, on(y, k), slot)


class Gather:
    def __init__(self, arrays, pieces, in_vmem=False):
        self.arrays, self.pieces, self.in_vmem = arrays, pieces, in_vmem

    def scratch(self):
        A, P = len(self.arrays), len(self.pieces)
        both = lambda *s: [DMA(s), DMA(s)]
        wide = [n if parts else n // 2 for _, n, parts in self.arrays]
        inputs = sum(max(len(a[2]), 1) for a in self.arrays)
        return dict(
            blocks=[pltpu.VMEM((LINE, a[0], w), BF) for a, w in zip(self.arrays, wide)],
            rows=[pltpu.VMEM((TALL, w) if a[0] == THIN else (8, 128), BF) for a, w in zip(self.arrays, wide)],
            tall=pltpu.VMEM((TALL, max(wide)), F32),
            own=DMA((inputs,)), put=DMA((P,)), line=[DMA((LINE, inputs)), DMA((A,))],
            near=both(P, 2), far=both(P, 2), near2=both(P, 2), far2=both(P, 2), over=both(P, 4),
        )

    def outs(self):
        return [jax.ShapeDtypeStruct((X, Y, TALL, a[1]) if a[0] == THIN else (X, Y, LINE, a[0], a[1]), BF) for a in self.arrays]

    def bind(self, ins, outs, s):
        self.ins, self.res, self.s = ins, outs, s
        self.spot = place()
        return self

    def _parts(self, slot, core):
        out = []
        for i, (r, width, parts) in enumerate(self.arrays):
            half, dst = width // 2, self.s["blocks"][i].at[slot]
            for first, w in parts:
                out.append((len(out), i, self.ins[len(out)].at[0], dst.at[:, pl.ds(first, w)]))
            if not parts:
                out.append((len(out), i, self.ins[len(out)].at[0, :, cols(core * half, half)], dst))
        return out

    def _line(self, do):
        x, y, slot, _ = self.spot

        def each(k, _):
            to = on(slot, k, LINE)
            do([remote(src, dst, (self.s["line"][0].at[k, n], self.s["line"][1].at[i]), device(x, y, to))
                for n, i, src, dst in self._parts(slot, lax.rem(to, C))])

        lax.fori_loop(1, LINE, each, None)

    def _own(self):
        _, _, slot, c = self.spot
        return [pltpu.make_async_copy(src, dst, self.s["own"].at[n]) for n, i, src, dst in self._parts(slot, c)]

    def down(self):
        self._line(start)
        start(self._own())

    def lay(self):
        for cp in self._own():
            cp.wait()
        for i, b in enumerate(self.s["blocks"]):
            some = b.at[pl.ds(0, LINE - 1)]
            pltpu.make_async_copy(some, some, self.s["line"][1].at[i]).wait()
        tall = self.s["tall"]
        for i, b in enumerate(self.s["blocks"]):
            if self.arrays[i][0] == THIN:
                w = b.shape[2]
                for d in range(LINE):
                    tall[THIN * d : THIN * d + THIN, :w] = b[d].astype(F32)
                self.s["rows"][i][...] = tall[:, :w].astype(BF)

    def _view(self, i, lo, w, xs, ys, core, rows=ALL):
        at = cols(core * (self.arrays[i][1] // 2) + lo, w)
        if rows == slice(LINE, None) and self.arrays[i][0] == THIN:
            rows = pl.ds(LINE, 2 * LINE)
        return self.res[i].at[xs, ys, rows, at] if self.arrays[i][0] == THIN else self.res[i].at[xs, ys, rows, :, at]

    def _half(self, i, k):
        n = LINE if self.arrays[i][0] == THIN else LINE // 2
        return slice(n, None) if k else slice(n)

    def _put(self):
        x, y, _, c = self.spot
        out = []
        for p, (i, lo, w, colour) in enumerate(self.pieces):
            r, n, parts = self.arrays[i]
            at = cols(c * (n // 2) + lo, w) if parts else pl.ds(lo, w)
            src = self.s["rows"][i].at[:, at] if r == THIN else self.s["blocks"][i].at[:, :, at]
            out.append((p, i, lo, w, colour, src))
        return out

    def _near(self, relay):
        x, y, _, c = self.spot
        copies = []
        for p, i, lo, w, colour, src in self._put():
            ring = Ring(colour == 1)
            for n, k in BOTH:
                if relay:
                    back = (on(x, 4 - k), y) if colour == 1 else (x, on(y, 4 - k))
                    v = self._view(i, lo, w, *back, c, self._half(i, n))
                    copies.append(remote(v, v, pair(self.s["near2"], p, n), ring.to(k)))
                else:
                    copies.append(remote(src, self._view(i, lo, w, x, y, c), pair(self.s["near"], p, n), ring.to(k)))
        return copies

    def _own_rows(self):
        x, y, _, c = self.spot
        return [pltpu.make_async_copy(src, self._view(i, lo, w, x, y, c), self.s["put"].at[p]) for p, i, lo, w, colour, src in self._put()]

    def near(self):
        start(self._near(False))
        if self.in_vmem:
            x, y, _, c = self.spot
            for rows, res in zip(self.s["rows"], self.res):
                n = rows.shape[1] // 2
                res[x, y, :, cols(c * n, n)] = rows[:, cols(c * n, n)]
        else:
            start(self._own_rows())

    def near2(self):
        landed(self._near(False))
        start(self._near(True))

    def _strip(self, i, lo, w, colour, k, core, half=ALL):
        x, y, _, _ = self.spot
        return self._view(i, lo, w, on(x, k), half, core) if colour == 0 else self._view(i, lo, w, half, on(y, k), core)

    def _far(self, relay):
        c, copies = self.spot[3], []
        for p, (i, lo, w, colour) in enumerate(self.pieces):
            ring = Ring(colour == 0)
            for n, k in BOTH:
                v = self._strip(i, lo, w, colour, 4 - k if relay else 0, c, slice(2 * n, 2 * n + 2) if relay else ALL)
                copies.append(remote(v, v, pair(self.s["far2" if relay else "far"], p, n), ring.to(k)))
        return copies

    def _over(self, ks):
        x, y, slot, c = self.spot
        copies = []
        for k in ks:
            for p, (i, lo, w, colour) in enumerate(self.pieces):
                v = self._strip(i, lo, w, colour, k, c)
                copies.append(remote(v, v, pair(self.s["over"], p, k), device(x, y, slot + 1 - 2 * c)))
        return copies

    def far(self):
        if not self.in_vmem:
            for cp in self._own_rows():
                cp.wait()
        landed(self._near(True))
        start(self._far(False))
        start(self._over([0]))

    def far2(self):
        landed(self._far(False))
        start(self._far(True))
        start(self._over([1, 3]))

    def over(self):
        landed(self._far(True))
        start(self._over([2]))

    def finish(self):
        landed(self._over(range(4)))
        self._line(left)
        for copies in (self._near(False), self._near(True), self._far(False), self._far(True), self._over(range(4))):
            left(copies)

    def steps(self):
        return [self.down, self.lay, self.near, self.near2, self.far, self.far2, self.over, self.finish]


class Scatter:
    def __init__(self, arrays, pieces, in_vmem=False):
        self.arrays, self.pieces, self.in_vmem = arrays, pieces, in_vmem

    def scratch(self):
        P = len(self.pieces)
        both = lambda *s: [DMA(s), DMA(s)]
        per = lambda *lead: [pltpu.VMEM((*lead, self._m(i), LINE, w), BF) for i, lo, w, _ in self.pieces]
        half = [pltpu.VMEM((2, 2, self._m(i), LINE, w), BF) for i, lo, w, _ in self.pieces]
        return dict(
            own=per(X, Y), other=per(X, Y), h1=half, f1=per(2, 4), t=per(4),
            h2=per(), f2=per(2),
            zs=[pltpu.VMEM((LINE, a[0], a[1] // 2), BF) for a in self.arrays], zr=[pltpu.VMEM((LINE, a[0], a[1] // 2), BF) for a in self.arrays],
            get=DMA((P,)), over=both(P), a=both(P, 2), a2=both(P, 2), b=both(P, 2), b2=both(P, 2),
            line=[DMA((LINE, len(self.arrays))), DMA((len(self.arrays),))],
        )

    def _m(self, i):
        return 3 if self.arrays[i][0] == THIN else LINE // 2

    def _parts(self, i):
        h = self._m(i) // 2
        return pl.ds(0, h), pl.ds(h, self._m(i) - h)

    def outs(self):
        return [jax.ShapeDtypeStruct((1, a[0], w), BF) for a in self.arrays for _, w in a[2] or [(0, a[1])]]

    def bind(self, ins, outs, s):
        self.ins, self.res, self.s = ins, outs, s
        self.spot = place()
        return self

    def _each(self):
        return [(p, i, lo, w, colour) for p, (i, lo, w, colour) in enumerate(self.pieces)]

    def _view(self, i, lo, w, core):
        return self.ins[i].at[:, :, :, :, cols(core * (self.arrays[i][1] // 2) + lo, w)]

    def _over(self):
        x, y, slot, c = self.spot
        return [remote(self._view(i, lo, w, 1 - c), self.s["other"][p], pair(self.s["over"], p), device(x, y, slot + 1 - 2 * c))
                for p, i, lo, w, colour in self._each()]

    def _get(self):
        return [pltpu.make_async_copy(self._view(i, lo, w, self.spot[3]), self.s["own"][p], self.s["get"].at[p]) for p, i, lo, w, colour in self._each()]

    def down(self):
        start(self._over())
        if not self.in_vmem:
            start(self._get())

    def _target(self, p, colour, k):
        x, y, _, _ = self.spot
        own = self.s["own"][p]
        return own.at[on(x, k)] if colour == 0 else own.at[:, on(y, k)]

    def _a(self):
        copies = []
        for p, i, lo, w, colour in self._each():
            for n, k in BOTH:
                copies.append(remote(self._target(p, colour, 2).at[pl.ds(2 * n, 2)], self.s["h1"][p].at[n], pair(self.s["a"], p, n), Ring(colour == 0).to(k)))
        return copies

    def _a2(self):
        return [remote(self._target(p, colour, k), self.s["f1"][p].at[n], pair(self.s["a2"], p, n), Ring(colour == 0).to(k))
                for p, i, lo, w, colour in self._each() for n, k in BOTH]

    def _of(self, copies, p):
        return [copies[2 * p], copies[2 * p + 1]]

    def near(self):
        over, a = self._over(), self._a()
        get = None if self.in_vmem else self._get()
        for p, i, lo, w, colour in self._each():
            if get:
                get[p].wait()
            over[p].wait_recv()
            own, other = self.s["own"][p], self.s["other"][p]
            mine = self._view(i, lo, w, self.spot[3]) if self.in_vmem else own

            def add(n, _):
                at = n // Y, lax.rem(n, Y)
                own[at] = (mine[at].astype(F32) + other[at].astype(F32)).astype(BF)

            lax.fori_loop(0, X * Y, add, None)
            start(self._of(a, p))

    def near2(self):
        a, a2 = self._a(), self._a2()
        for p, i, lo, w, colour in self._each():
            landed(self._of(a, p))
            for n, k in BOTH:
                to, h = self._target(p, colour, k), self.s["h1"][p]
                for q in range(2):
                    to[2 * n + q] = (to[2 * n + q].astype(F32) + h[n, q].astype(F32)).astype(BF)
            start(self._of(a2, p))

    def _b(self):
        copies = []
        x, y, _, _ = self.spot
        for p, i, lo, w, colour in self._each():
            ring = Ring(colour == 1)
            for (n, k), part in zip(BOTH, self._parts(i)):
                copies.append(remote(self.s["t"][p].at[on(ring.at, 2), part], self.s["h2"][p].at[part], pair(self.s["b"], p, n), ring.to(k)))
        return copies

    def _b2(self):
        copies = []
        for p, i, lo, w, colour in self._each():
            ring = Ring(colour == 1)
            copies += [remote(self.s["t"][p].at[on(ring.at, k)], self.s["f2"][p].at[n], pair(self.s["b2"], p, n), ring.to(k)) for n, k in BOTH]
        return copies

    def far(self):
        a2, b = self._a2(), self._b()
        for p, i, lo, w, colour in self._each():
            landed(self._of(a2, p))
            own, f, t = self._target(p, colour, 0), self.s["f1"][p], self.s["t"][p]

            def add(n, _):
                t[n] = (own[n].astype(F32) + f[0, n].astype(F32) + f[1, n].astype(F32)).astype(BF)

            lax.fori_loop(0, 4, add, None)
            start(self._of(b, p))

    def far2(self):
        b, b2 = self._b(), self._b2()
        for p, i, lo, w, colour in self._each():
            landed(self._of(b, p))
            ring, t = Ring(colour == 1), self.s["t"][p]
            for (_, k), part in zip(BOTH, self._parts(i)):
                at = on(ring.at, k), part
                t[at] = (t[at].astype(F32) + self.s["h2"][p][part].astype(F32)).astype(BF)
            start(self._of(b2, p))

    def _line(self, do):
        x, y, slot, _ = self.spot

        def each(k, _):
            to = on(slot, k, LINE)
            do([remote(zs.at[to], zr.at[slot], (self.s["line"][0].at[k, i], self.s["line"][1].at[i]), device(x, y, to))
                for i, (zs, zr) in enumerate(zip(self.s["zs"], self.s["zr"]))])

        lax.fori_loop(1, LINE, each, None)

    def line(self):
        b2, slot = self._b2(), self.spot[2]
        for p, i, lo, w, colour in self._each():
            landed(self._of(b2, p))
            f = self.s["f2"][p]
            total = self.s["t"][p][Ring(colour == 1).at].astype(F32) + f[0].astype(F32) + f[1].astype(F32)
            zs = self.s["zs"][i]
            if self.arrays[i][0] == THIN:
                total = total.reshape(TALL, w)
                for d in range(LINE):
                    zs[d, :, lo : lo + w] = total[THIN * d : THIN * d + THIN].astype(BF)
            else:
                zs[:, :, lo : lo + w] = total.reshape(LINE, -1, w).astype(BF)
        self._line(start)
        for zs, zr in zip(self.s["zs"], self.s["zr"]):
            zr[slot] = zs[slot]

    def finish(self):
        n = 0
        for i, (r, width, parts) in enumerate(self.arrays):
            zr = self.s["zr"][i]
            some = zr.at[pl.ds(0, LINE - 1)]
            pltpu.make_async_copy(some, some, self.s["line"][1].at[i]).wait()
            sums = []
            for core in range(C):
                total = zr[core].astype(F32)
                for k in range(1, Z):
                    total += zr[C * k + core].astype(F32)
                sums.append(total.astype(BF))
            whole = jnp.concatenate(sums, axis=1)
            for first, w in parts or [(0, width)]:
                self.res[n][0] = whole[:, first : first + w]
                n += 1
        self._line(left)
        for copies in (self._over(), self._a(), self._a2(), self._b(), self._b2()):
            left(copies)

    def steps(self):
        return [self.down, self.near, self.near2, self.far, self.far2, self.line, self.finish]


QKV = ([(THIN, WIDTH + 2 * HEAD, [(0, WIDTH), (WIDTH, HEAD), (WIDTH + HEAD, HEAD)])], [(0, 0, 256, 0), (0, 256, 256, 1)])
REST = (
    [(THIN, WIDTH, ()), (THIN, HIDDEN_UNITS, ()), (THIN, HIDDEN_UNITS, ()), (8, WIDTH, ())],
    [(1, 0, 1024, 0), (2, 0, 1024, 1), (0, 0, 384, 0), (3, 0, 128, 0), (3, 128, 256, 1)],
)


THETA = 10000
NAMES = ("wq", "wk", "wv", "wo", "w_gate", "w_up", "w_down")
G = 6
TB = 512
NT = 4
MB, MT, FJ, MJ = 1024, 2, 512, 4
BLOCKS = NT * (NT + 1) // 2
NEG = -1e30
HIDDEN = 2 * NEG
LOG2E = 1.4426950408889634
VMEM = 56 * 2**20
EPS = 1e-6


def mm(a, b):
    return lax.dot_general(a, b, (((1,), (0,)), ((), ())), preferred_element_type=F32)


def mm_t(a, b):
    return lax.dot_general(a, b, (((1,), (1,)), ((), ())), preferred_element_type=F32)


def norm(h):
    scale = lax.rsqrt(jnp.mean(h * h, -1, keepdims=True) + EPS)
    return (h * scale).astype(BF), scale


def norm_back(h, g):
    scale = lax.rsqrt(jnp.mean(h * h, -1, keepdims=True) + EPS)
    return scale * (g - h * (scale * scale * jnp.mean(g * h, -1, keepdims=True)))


def turn_table(tokens):
    half = HEAD // 2
    freq = np.float64(THETA) ** (-np.arange(half) / half)
    place = np.concatenate([HEAD * np.arange(tokens // HEAD), np.arange(HEAD)]) * 1.0
    angle = place[:, None] * np.concatenate([freq, freq])
    return jnp.asarray(np.stack([np.cos(angle), np.sin(angle)]).astype(np.float32))


def turner(table, n):
    far, near = pl.ds(n, 1), slice(-HEAD, None)
    fc, fs, nc, ns = table[0, far, :], table[1, far, :], table[0, near, :], table[1, near, :]
    sin = fs * nc + fc * ns
    return fc * nc - fs * ns, jnp.where(lax.broadcasted_iota(jnp.int32, sin.shape, 1) < HEAD // 2, -sin, sin)


def swap(t):
    return pltpu.roll(t, HEAD // 2, 1)


def whole(shape):
    return pl.BlockSpec(shape, lambda *_: (0,) * len(shape))


def stage(n, plan):
    for at, todo in plan.items():

        @pl.when(n == at)
        def _():
            for do in todo:
                do()


def block_of(m):
    i = sum((m >= (r * (r + 1)) // 2).astype(jnp.int32) for r in range(1, NT))
    return i, m - (i * (i + 1)) // 2


def rows(b, size=TB, first=0):
    return pl.ds(pl.multiple_of(b * TB + first, HEAD), size)


def wait(copies):
    for cp in copies:
        cp.wait()


HALVES = ((0, 0), (TB // 2, TB // 2))


def masked(s, key, query):
    return lax.broadcasted_iota(jnp.int32, s.shape, 0) + key <= lax.broadcasted_iota(jnp.int32, s.shape, 1) + query


def _front(x_ref, table_ref, *rest, gq, gr):
    weights, rest = rest[: len(NAMES)], rest[len(NAMES) :]
    hbm, outs, (ours, lse_s, table_s, vt_s, top_s, mix_s, w_s, sems, o_sem, sq, sr) = rest[:6], rest[6:11], rest[11:]
    q_s, k_s, v_s, at_s, o_s, x_s = ours
    n = pl.program_id(0)
    gq.bind(weights[:3], (w_s,), sq)
    gr.bind(weights[3:], outs[1:], sr)
    fetch = [pltpu.make_async_copy(a, b, sems.at[len(ours) + m]) for m, (a, b) in enumerate([(x_ref, x_s), (table_ref, table_s)])]
    lse_out = pltpu.make_async_copy(lse_s, hbm[5], sems.at[5])
    keep = [pltpu.make_async_copy(a, b, sems.at[m]) for m, (a, b) in enumerate(zip((q_s, k_s, v_s, at_s, w_s), (*hbm[:4], outs[0])))]
    o_out = lambda b: pltpu.make_async_copy(o_s.at[:, rows(b)], hbm[4].at[:, rows(b)], o_sem.at[b])

    def normed(first, last):
        for b in range(first, last):
            at = slice(b * TB, b * TB + TB)
            a, _ = norm(x_s[at, :].astype(F32))
            x_s[at, :] = a
            at_s[:, at] = a.T

    def early():
        start(fetch)
        hello()
        wait(fetch)
        normed(0, NT // 2)

    def late():
        normed(NT // 2, NT)

    def keep_all():
        start(keep)

    stage(n, {
        0: [early, meet, gq.down, gr.down, late, gq.lay, gq.near, gq.near2, gq.far, gr.lay, gr.near, gq.far2, gq.over, gr.near2, gq.finish],
        2: [gr.far],
        NT: [keep_all],
        10: [gr.far2],
        13: [gr.over],
    })

    @pl.when(n < NT)
    def _():
        a = x_s[rows(n), :]
        y = mm(a, w_s[...].reshape(a.shape[1], -1)).astype(BF)
        for i in range(TB // HEAD):
            here, there = slice(HEAD * i, HEAD * i + HEAD), rows(n, HEAD, HEAD * i)
            cos, sin = turner(table_s, n * (TB // HEAD) + i)
            for h in range(G + 1):
                t = y[here, HEAD * h : HEAD * h + HEAD].astype(F32)
                t = (t * cos + swap(t) * sin).astype(BF)
                if h < G:
                    q_s[h, there, :] = t
                else:
                    k_s[there, :] = t
        v = y[:, (G + 1) * HEAD :]
        v_s[rows(n), :] = v
        vt_s[n] = jnp.concatenate([v.T, jnp.ones((8, TB), BF)], axis=0)

    i, j = block_of(n - NT)
    e = HEAD**-0.5 * LOG2E

    @pl.when((n >= NT) & (j == 0))
    def _():
        top_s[...] = jnp.full(top_s.shape, NEG, F32)
        mix_s[...] = jnp.zeros(mix_s.shape, F32)

    def block(key, keys, query, mask):
        k = k_s[rows(j, keys, key), :]
        scores = [mm_t(k, q_s[h, rows(i, TB - query, query), :]) for h in range(G)]
        weights, keeps = [], []
        for h, s in enumerate(scores):
            if mask:
                s = jnp.where(masked(s, key, query), s, HIDDEN)
            old = top_s[h : h + 1, query:]
            top = jnp.maximum(old, s.max(axis=0, keepdims=True))
            top_s[h : h + 1, query:] = top
            weights.append(jnp.exp2((s - top) * e).astype(BF))
            keeps.append(jnp.exp2((old - top) * e))
        for h in range(G):
            mix_s[h, :, query:] = mix_s[h, :, query:] * keeps[h] + mm(vt_s[j, :, key : key + keys], weights[h])

    @pl.when((n >= NT) & (j < i))
    def _():
        block(0, TB, 0, False)

    @pl.when((n >= NT) & (j == i))
    def _():
        for key, query in HALVES:
            block(key, TB // 2, query, True)
        for h in range(G):
            total = mix_s[h, HEAD : HEAD + 1, :]
            o_s[h, rows(i), :] = (mix_s[h, :HEAD, :] * (1 / total)).T.astype(BF)
            lse_s[h : h + 1, rows(i)] = top_s[h : h + 1, :] * HEAD**-0.5 + jnp.log(total)
        o_out(i).start()

    def finish():
        lse_out.start()
        gr.finish()
        lse_out.wait()
        wait(keep)
        wait([o_out(b) for b in range(NT)])

    stage(n, {NT + BLOCKS - 1: [finish]})


def front(x, table, weights, gq, gr):
    T, D = x.shape
    hbm = pl.BlockSpec(memory_space=pltpu.HBM)
    mine = [(G, T, HEAD), (T, HEAD), (T, HEAD), (D, T), (G, T, HEAD)]
    outs = [jax.ShapeDtypeStruct(s, BF) for s in mine] + [jax.ShapeDtypeStruct((8, T), F32)] + gq.outs() + gr.outs()
    return pl.pallas_call(
        functools.partial(_front, gq=gq, gr=gr),
        grid=(NT + BLOCKS,),
        in_specs=[hbm] * (2 + len(weights)),
        out_specs=[hbm] * len(outs),
        out_shape=outs,
        scratch_shapes=[[pltpu.VMEM(s, BF) for s in (*mine, (T, D))], pltpu.VMEM((8, T), F32), pltpu.VMEM(table.shape, F32),
                        pltpu.VMEM((NT, HEAD + 8, TB), BF), pltpu.VMEM((8, TB), F32), pltpu.VMEM((G, HEAD + 8, TB), F32),
                        pltpu.VMEM((X, Y, TALL, 1024), BF), DMA((8,)), DMA((NT,)), gq.scratch(), gr.scratch()],
        compiler_params=pltpu.CompilerParams(dimension_semantics=("arbitrary",), vmem_limit_bytes=VMEM, collective_id=1, has_side_effects=True),
        name="front",
    )(x, table, *weights)


def _back(*refs, sq, sr):
    hbm, then, grads, dx_ref, outs, rest = refs[:5], refs[5:11], refs[11:15], refs[15], refs[16:23], refs[23:]
    ours, more, sems, more_sem, dq_s, dk_s, dv_s, d_s, acc, dw_s, rq, rr = rest
    q_s, do_s, k_s, v_s, at_s = ours
    lse_ref, delta_ref, table_s, w_s, x_s, dh_s = more
    n = pl.program_id(0)
    sq.bind((dw_s,), outs[:3], rq)
    sr.bind(grads, outs[3:], rr)

    def fetch(b):
        at = [(ALL, rows(b)), (ALL, rows(b)), (rows(b),), (rows(b),), (ALL, rows(b))]
        return [pltpu.make_async_copy(src.at[a], dst.at[a], sems.at[m, b]) for m, (src, dst, a) in enumerate(zip(hbm, ours, at))]

    whole_ones = [pltpu.make_async_copy(src, dst, more_sem.at[m]) for m, (src, dst) in enumerate(zip(then, more))]

    def fetch_all():
        start(whole_ones[:3])
        for b in range(NT):
            start(fetch(b))
        start(whole_ones[3:])

    def rest_here():
        wait(whole_ones[3:])

    i, j = block_of(n)
    stage(n, {0: [fetch_all, hello]})

    @pl.when((n < BLOCKS) & (j == 0))
    def _():
        wait(fetch(i))

        @pl.when(n == 0)
        def _():
            wait(whole_ones[:3])

    stage(n, {1: [meet, sr.down], 3: [sr.near], 5: [sr.near2], 8: [sr.far], 9: [sr.far2]})
    scale = HEAD**-0.5
    e = scale * LOG2E

    @pl.when(n == 0)
    def _():
        dk_s[...] = jnp.zeros_like(dk_s)
        dv_s[...] = jnp.zeros_like(dv_s)
        acc[...] = jnp.zeros_like(acc)

    @pl.when((n < BLOCKS) & (j == 0))
    def _():
        dq_s[...] = jnp.zeros_like(dq_s)

    def block(key, keys, query, mask):
        here, there = rows(j, keys, key), rows(i, TB - query, query)
        k, v = k_s[here, :], v_s[here, :]
        kt = k.T
        qs = [q_s[h, there, :] for h in range(G)]
        dos = [do_s[h, there, :] for h in range(G)]
        scores = [mm_t(k, q) for q in qs]
        dps = [mm_t(v, do) for do in dos]
        for h in range(G):
            p = jnp.exp2(scores[h] * e - lse_ref[h : h + 1, there] * LOG2E)
            if mask:
                p = jnp.where(masked(p, key, query), p, 0.0)
            ds = (p * (dps[h] - delta_ref[h : h + 1, there])).astype(BF)
            dv_s[j, key : key + keys] += mm(p.astype(BF), dos[h])
            dk_s[j, key : key + keys] += mm(ds, qs[h])
            dq_s[h, :, query:] += mm(kt, ds)

    def turn_back(t, b, r):
        cos, sin = turner(table_s, b * (TB // HEAD) + r)
        t = t[HEAD * r : HEAD * r + HEAD].astype(F32)
        return (t * cos - swap(t) * sin).astype(BF)

    @pl.when((n < BLOCKS) & (j < i))
    def _():
        block(0, TB, 0, False)

    @pl.when((n < BLOCKS) & (j == i))
    def _():
        for key, query in HALVES:
            block(key, TB // 2, query, True)
        for h in range(G):
            dq = (dq_s[h] * scale).T.astype(BF)
            for r in range(TB // HEAD):
                d_s[i, HEAD * r : HEAD * r + HEAD, HEAD * h : HEAD * h + HEAD] = turn_back(dq, i, r)
        acc[:, : G * HEAD] += mm(at_s[:, rows(i)], d_s[i, :, : G * HEAD])

    def last():
        for b in range(NT):
            dk = (dk_s[b] * scale).astype(BF)
            for r in range(TB // HEAD):
                d_s[b, HEAD * r : HEAD * r + HEAD, G * HEAD : (G + 1) * HEAD] = turn_back(dk, b, r)
            d_s[b, :, (G + 1) * HEAD :] = dv_s[b].astype(BF)
            acc[:, G * HEAD :] += mm(at_s[:, rows(b)], d_s[b, :, G * HEAD :])
        dw_s[...] = acc[...].astype(BF).reshape(dw_s.shape)

    stage(n, {BLOCKS: [last, sq.down, sr.line, rest_here], BLOCKS + 1: [sq.near], BLOCKS + 2: [sq.near2], BLOCKS + 3: [sq.far]})

    @pl.when(n >= BLOCKS)
    def _():
        da = mm_t(d_s[n - BLOCKS], w_s[...])
        at = rows(n - BLOCKS)
        dx_ref[...] = (dh_s[at, :].astype(F32) + norm_back(x_s[at, :].astype(F32), da)).astype(BF)

    stage(n, {BLOCKS + NT - 1: [sq.far2, sq.line, sr.finish, sq.finish]})


def back(q, k, v, do, lse, delta, at, x, dh, w, table, grads, sq, sr):
    T, D = x.shape
    hbm = pl.BlockSpec(memory_space=pltpu.HBM)
    outs = sq.outs() + sr.outs()
    ins, then = (q, do, k, v, at), (lse, delta, table, w, x, dh)
    return pl.pallas_call(
        functools.partial(_back, sq=sq, sr=sr),
        grid=(BLOCKS + NT,),
        in_specs=[hbm] * (len(ins) + len(then) + len(grads)),
        out_specs=[pl.BlockSpec((TB, D), lambda n: (jnp.maximum(n - BLOCKS, 0), 0))] + [whole(o.shape) for o in outs],
        out_shape=[jax.ShapeDtypeStruct((T, D), BF)] + outs,
        scratch_shapes=[[pltpu.VMEM(a.shape, BF) for a in ins], [pltpu.VMEM(a.shape, a.dtype) for a in then], DMA((len(ins), NT)), DMA((len(then),)),
                        pltpu.VMEM((G, HEAD, TB), F32), pltpu.VMEM((NT, TB, HEAD), F32), pltpu.VMEM((NT, TB, HEAD), F32),
                        pltpu.VMEM((NT, TB, 1024), BF), pltpu.VMEM(w.shape, F32), pltpu.VMEM((X, Y, THIN, LINE, 1024), BF), sq.scratch(), sr.scratch()],
        compiler_params=pltpu.CompilerParams(dimension_semantics=("arbitrary",), vmem_limit_bytes=63 * 2**20, collective_id=2, has_side_effects=True),
        name="back",
    )(*ins, *then, *grads)


def _middle(x_ref, o_ref, wo_ref, dy_hbm, wg_hbm, wu_hbm, wd_hbm, dh_ref, do_ref, delta_ref, dwo_ref, dwg_hbm, dwu_hbm, dwd_hbm,
            h_s, b_s, bt_s, db_s, dy_s, wg_s, wu_s, wd_s, ao, ag, au, ad, tg, tu, td, dy_sem, in_sem, out_sem):
    n = pl.program_id(0)
    m = n - NT
    j, t = m // MT, lax.rem(m, MT)
    is_main = (m >= 0) & (m < MJ * MT)
    dy_in = pltpu.make_async_copy(dy_hbm, dy_s, dy_sem)

    def chunk(j):
        at, to = cols(j * FJ, FJ), lax.rem(j, 2)
        pairs = [(wg_hbm.at[:, at], wg_s), (wu_hbm.at[:, at], wu_s), (wd_hbm.at[at, :], wd_s)]
        return [pltpu.make_async_copy(src, dst.at[to], in_sem.at[i, to]) for i, (src, dst) in enumerate(pairs)]

    def grads(j):
        at = cols(j * FJ, FJ)
        pairs = [(tg, dwg_hbm.at[:, at]), (tu, dwu_hbm.at[:, at]), (td, dwd_hbm.at[at, :])]
        return [pltpu.make_async_copy(src, dst, out_sem.at[i]) for i, (src, dst) in enumerate(pairs)]

    @pl.when(n == 0)
    def _():
        start(chunk(0))
        dy_in.start()

    @pl.when(n < NT)
    def _():
        o = jnp.concatenate([o_ref[h] for h in range(G)], axis=1)
        h = (x_ref[...].astype(F32) + mm(o, wo_ref[...]).astype(BF).astype(F32)).astype(BF)
        h_s[rows(n), :] = h
        b, _ = norm(h.astype(F32))
        b_s[rows(n), :] = b
        bt_s[:, rows(n)] = b.T

    @pl.when(m == 0)
    def _():
        dy_in.wait()

    @pl.when(is_main & (t == 0))
    def _():
        wait(chunk(j))
        ag[...] = jnp.zeros_like(ag)
        au[...] = jnp.zeros_like(au)
        ad[...] = jnp.zeros_like(ad)

        @pl.when(j + 1 < MJ)
        def _():
            start(chunk(j + 1))

    @pl.when(is_main)
    def _():
        these, slot = pl.ds(pl.multiple_of(t * MB, MB), MB), lax.rem(j, 2)
        b, bt, dy = b_s[these, :], bt_s[:, these], dy_s[these, :]

        def into(c):
            return mm(b, wg_s[slot, :, c]), mm(b, wu_s[slot, :, c]), mm_t(dy, wd_s[slot, c, :])

        def point(gate, up, dact):
            dact = dact.astype(BF).astype(F32)
            sig = 0.5 + 0.5 * jnp.tanh(0.5 * gate)
            silu = gate * sig
            return (silu * up).astype(BF), (dact * up * (sig + silu * (1 - sig))).astype(BF), (dact * silu).astype(BF)

        strips = [slice(a, a + 256) for a in range(0, FJ, 256)]
        ahead, dbs = into(strips[0]), []
        for i, c in enumerate(strips):
            now, ahead = ahead, into(strips[i + 1]) if i + 1 < len(strips) else ()
            act, dgate, dup = point(*now)
            dbs.append(mm_t(dgate, wg_s[slot, :, c]) + mm_t(dup, wu_s[slot, :, c]))
            ag[:, c] += mm(bt, dgate)
            au[:, c] += mm(bt, dup)
            ad[c, :] += mm(act.T, dy)
        db = sum(dbs[1:], dbs[0])

        @pl.when(j == 0)
        def _():
            db_s[these, :] = db

        @pl.when(j > 0)
        def _():
            db_s[these, :] += db

        @pl.when(t == MT - 1)
        def _():
            @pl.when(j > 0)
            def _():
                wait(grads(j - 1))

            tg[...] = ag[...].astype(BF)
            tu[...] = au[...].astype(BF)
            td[...] = ad[...].astype(BF)
            start(grads(j))

    last = m - MJ * MT

    @pl.when(last == 0)
    def _():
        ao[...] = jnp.zeros_like(ao)

    @pl.when(last >= 0)
    def _():
        at = rows(jnp.maximum(last, 0))
        dh = (dy_s[at, :].astype(F32) + norm_back(h_s[at, :].astype(F32), db_s[at, :]).astype(BF).astype(F32)).astype(BF)
        dh_ref[...] = dh
        do = mm_t(dh, wo_ref[...]).astype(BF)
        o = jnp.concatenate([o_ref[h] for h in range(G)], axis=1)
        prod = do.astype(F32) * o.astype(F32)
        for h in range(G):
            do_ref[h] = do[:, HEAD * h : HEAD * h + HEAD]
        delta_ref[...] = jnp.concatenate([prod[:, HEAD * h : HEAD * h + HEAD].sum(-1, keepdims=True) for h in range(G)]
                                         + [jnp.zeros((TB, 8 - G), F32)], axis=1).T
        ao[...] += mm(o.T, dh)

    @pl.when(last == NT - 1)
    def _():
        dwo_ref[...] = ao[...].astype(BF)
        wait(grads(MJ - 1))


def middle(x, dy, o, wo, wg, wu, wd):
    T, D = x.shape
    end = NT + MJ * MT
    late = lambda n: jnp.maximum(n - end, 0)
    ends = lambda n: jnp.where(n < NT, n, jnp.where(n < end, NT - 1, n - end))
    once = pl.BlockSpec(wo.shape, lambda n: (0, 0), pipeline_mode=pl.Buffered(1))
    hbm = pl.BlockSpec(memory_space=pltpu.HBM)
    buf = lambda *s, dtype=BF: pltpu.VMEM(s, dtype)
    return pl.pallas_call(
        _middle,
        grid=(end + NT,),
        in_specs=[pl.BlockSpec((TB, D), lambda n: (jnp.minimum(n, NT - 1), 0)), pl.BlockSpec((G, TB, HEAD), lambda n: (0, ends(n), 0)), once,
                  hbm, hbm, hbm, hbm],
        out_specs=[pl.BlockSpec((TB, D), lambda n: (late(n), 0)), pl.BlockSpec((G, TB, HEAD), lambda n: (0, late(n), 0)),
                   pl.BlockSpec((8, TB), lambda n: (0, late(n))), once, hbm, hbm, hbm],
        out_shape=[jax.ShapeDtypeStruct((T, D), BF), jax.ShapeDtypeStruct((G, T, HEAD), BF), jax.ShapeDtypeStruct((8, T), F32),
                   *(jax.ShapeDtypeStruct(a.shape, BF) for a in (wo, wg, wu, wd))],
        scratch_shapes=[buf(T, D), buf(T, D), buf(D, T), buf(T, D, dtype=F32), buf(T, D), buf(2, D, FJ), buf(2, D, FJ), buf(2, FJ, D),
                        buf(D, D, dtype=F32), buf(D, FJ, dtype=F32), buf(D, FJ, dtype=F32), buf(FJ, D, dtype=F32), buf(D, FJ), buf(D, FJ), buf(FJ, D),
                        DMA(()), DMA((3, 2)), DMA((3,))],
        compiler_params=pltpu.CompilerParams(dimension_semantics=("arbitrary",), vmem_limit_bytes=67043328), name="middle",
    )(x, o, wo, dy, wg, wu, wd)


def _hand_over(*refs):
    half = len(refs) // 2
    for src, dst in zip(refs[:half], refs[half:]):
        dst[...] = src[...]


def hand_over(dx, small):
    T, D = dx.shape[1:]
    specs = [pl.BlockSpec((1, TB, D), lambda n: (0, n, 0))] + [whole(a.shape) for a in small]
    return pl.pallas_call(
        _hand_over, grid=(NT,), in_specs=specs, out_specs=specs, out_shape=[jax.ShapeDtypeStruct(a.shape, BF) for a in (dx, *small)],
        compiler_params=pltpu.CompilerParams(dimension_semantics=("arbitrary",)), name="hand_over",
    )(dx, *small)


def solution(mesh):
    gq, gr, sq, sr = Gather(*QKV, in_vmem=True), Gather(*REST), Scatter(*QKV, in_vmem=True), Scatter(*REST)

    def step(x, dy, *weights):
        x, dy = x[0], dy[0]
        T, D = x.shape
        table = turn_table(T)
        q, k, v, at, o, lse, w, *rest = front(x, table, weights, gq, gr)
        rest = [a.reshape(D, -1) for a in rest[:3]] + [rest[3].reshape(-1, D)]
        dh, do, delta, *grads = middle(x, dy, o, *rest)
        grads = [g.reshape(X, Y, -1, LINE, g.shape[1]) for g in grads]
        dx, *by_w = back(q, k, v, do, lse, delta, at, x, dh, w.reshape(D, -1), table, grads, sq, sr)
        return hand_over(dx[None], by_w)

    states, cut = P(("rep", "dp"), None, None), P(None, "dp", None)
    return jax.shard_map(
        step,
        mesh=mesh,
        in_specs=(states, states) + (cut,) * 7,
        out_specs=(states,) + (P("rep", "dp", None),) * 7,
        check_vma=False,
    )
```

```python
import functools

import jax
import jax.numpy as jnp
import numpy as np
from jax import lax
from jax.experimental import pallas as pl
from jax.experimental.pallas import tpu as pltpu
from jax.sharding import PartitionSpec as P


F32, BF = jnp.float32, jnp.bfloat16
X, Y, Z, C = 4, 4, 8, 2
LINE = Z * C
DMA = pltpu.SemaphoreType.DMA
THIN = 3
TALL = THIN * LINE
WIDTH, HIDDEN_UNITS, HEAD = 768, 2048, 128
ALL = slice(None)
DIRECT = ((2, 2),)
BOTH = ((0, 1), (1, 3))


def place():
    me = lax.axis_index("dp")
    return me // (LINE * Y), lax.rem(me // LINE, Y), lax.rem(me, LINE), lax.rem(me, C)


def device(x, y, slot):
    return {"dp": (x * Y + y) * LINE + slot}


def on(a, k, n=4):
    return lax.rem(a + k, n)


def remote(src, dst, sems, where):
    send, recv = sems
    return pltpu.make_async_remote_copy(src_ref=src, dst_ref=dst, send_sem=send, recv_sem=recv, device_id=where, device_id_type=pl.DeviceIdType.MESH)


def start(copies):
    for cp in copies:
        cp.start()


def landed(copies):
    for cp in copies:
        cp.wait_recv()


def left(copies):
    for cp in copies:
        cp.wait_send()


def peers():
    x, y, slot, _ = place()
    who = [device(x, y, on(slot, k, LINE)) for k in range(1, LINE)]
    for k in range(1, X):
        who += [device(on(x, k), y, slot), device(x, on(y, k), slot)]
    return who


def hello():
    for d in peers():
        pl.semaphore_signal(pltpu.get_barrier_semaphore(), inc=1, device_id=d, device_id_type=pl.DeviceIdType.MESH)


def meet():
    pl.semaphore_wait(pltpu.get_barrier_semaphore(), len(peers()))


def cols(first, size):
    return pl.ds(pl.multiple_of(first, 128), size)


def pair(sems, *index):
    return sems[0].at[index], sems[1].at[index]


class Ring:
    def __init__(self, along_x):
        x, y, slot, c = place()
        self.at = x if along_x else y
        self.to = lambda k: device(on(x, k), y, slot) if along_x else device(x, on(y, k), slot)


class Gather:
    def __init__(self, arrays, pieces, in_vmem=False):
        self.arrays, self.pieces, self.in_vmem, self.direct = arrays, pieces, in_vmem, in_vmem

    def scratch(self):
        A, P = len(self.arrays), len(self.pieces)
        both = lambda *s: [DMA(s), DMA(s)]
        wide = [n if parts else n // 2 for _, n, parts in self.arrays]
        inputs = sum(max(len(a[2]), 1) for a in self.arrays)
        return dict(
            blocks=[pltpu.VMEM((LINE, a[0], w), BF) for a, w in zip(self.arrays, wide)],
            rows=[pltpu.VMEM((TALL, w) if a[0] == THIN else (8, 128), BF) for a, w in zip(self.arrays, wide)],
            tall=pltpu.VMEM((TALL, max(wide)), F32),
            own=DMA((inputs,)), put=DMA((P,)), line=both(A),
            near=both(P, 3), far=both(P, 2), near2=both(P, 2), far2=both(P, 2), over=both(P, 4),
        )

    def outs(self):
        return [jax.ShapeDtypeStruct((X, Y, TALL, a[1]) if a[0] == THIN else (X, Y, LINE, a[0], a[1]), BF) for a in self.arrays]

    def bind(self, ins, outs, s, own=None):
        self.ins, self.own, self.res, self.s = ins, own or ins, outs, s
        self.spot = place()

    def _parts(self, slot, core, ins):
        out = []
        for i, (r, width, parts) in enumerate(self.arrays):
            half, dst = width // 2, self.s["blocks"][i].at[slot]
            for first, w in parts:
                out.append((len(out), i, ins[len(out)].at[0], dst.at[:, pl.ds(first, w)]))
            if not parts:
                out.append((len(out), i, ins[len(out)].at[0, :, cols(core * half, half)], dst))
        return out

    def _line(self):
        x, y, slot, _ = self.spot

        def each(k, _):
            to = on(slot, k, LINE)
            start([remote(src, dst, pair(self.s["line"], i), device(x, y, to)) for n, i, src, dst in self._parts(slot, lax.rem(to, C), self.ins)])

        lax.fori_loop(1, LINE, each, None)

    def _all_of(self, sems):
        for i, b in enumerate(self.s["blocks"]):
            some = b.at[pl.ds(0, LINE - 1)]
            pltpu.make_async_copy(some, some, sems.at[i]).wait()

    def _own(self):
        _, _, slot, c = self.spot
        return [pltpu.make_async_copy(src, dst, self.s["own"].at[n]) for n, i, src, dst in self._parts(slot, c, self.own)]

    def down(self):
        self._line()
        start(self._own())

    def lay(self):
        for cp in self._own():
            cp.wait()
        self._all_of(self.s["line"][1])
        tall = self.s["tall"]
        for i, b in enumerate(self.s["blocks"]):
            if self.arrays[i][0] == THIN:
                w = b.shape[2]
                for d in range(LINE):
                    tall[THIN * d : THIN * d + THIN, :w] = b[d].astype(F32)
                self.s["rows"][i][...] = tall[:, :w].astype(BF)

    def _view(self, i, lo, w, xs, ys, core, rows=ALL):
        at = cols(core * (self.arrays[i][1] // 2) + lo, w)
        if rows == slice(LINE, None) and self.arrays[i][0] == THIN:
            rows = pl.ds(LINE, 2 * LINE)
        return self.res[i].at[xs, ys, rows, at] if self.arrays[i][0] == THIN else self.res[i].at[xs, ys, rows, :, at]

    def _half(self, i, k):
        n = LINE if self.arrays[i][0] == THIN else LINE // 2
        return slice(n, None) if k else slice(n)

    def _put(self):
        x, y, _, c = self.spot
        out = []
        for p, (i, lo, w, colour) in enumerate(self.pieces):
            r, n, parts = self.arrays[i]
            at = cols(c * (n // 2) + lo, w) if parts else pl.ds(lo, w)
            src = self.s["rows"][i].at[:, at] if r == THIN else self.s["blocks"][i].at[:, :, at]
            out.append((p, i, lo, w, colour, src))
        return out

    def _near(self, relay):
        x, y, _, c = self.spot
        copies = []
        for p, i, lo, w, colour, src in self._put():
            ring = Ring(colour == 1)
            for n, k in () if relay and self.direct else BOTH + DIRECT if self.direct else BOTH:
                if relay:
                    back = (on(x, 4 - k), y) if colour == 1 else (x, on(y, 4 - k))
                    v = self._view(i, lo, w, *back, c, self._half(i, n))
                    copies.append(remote(v, v, pair(self.s["near2"], p, n), ring.to(k)))
                else:
                    copies.append(remote(src, self._view(i, lo, w, x, y, c), pair(self.s["near"], p, n), ring.to(k)))
        return copies

    def _own_rows(self):
        x, y, _, c = self.spot
        return [pltpu.make_async_copy(src, self._view(i, lo, w, x, y, c), self.s["put"].at[p]) for p, i, lo, w, colour, src in self._put()]

    def near(self):
        start(self._near(False))
        if self.in_vmem:
            x, y, _, c = self.spot
            for rows, res in zip(self.s["rows"], self.res):
                n = rows.shape[1] // 2
                res[x, y, :, cols(c * n, n)] = rows[:, cols(c * n, n)]
        else:
            start(self._own_rows())

    def near2(self):
        landed(self._near(False))
        start(self._near(True))

    def _strip(self, i, lo, w, colour, k, core, half=ALL):
        x, y, _, _ = self.spot
        return self._view(i, lo, w, on(x, k), half, core) if colour == 0 else self._view(i, lo, w, half, on(y, k), core)

    def _far(self, relay):
        c, copies = self.spot[3], []
        for p, (i, lo, w, colour) in enumerate(self.pieces):
            ring = Ring(colour == 0)
            for n, k in BOTH:
                v = self._strip(i, lo, w, colour, 4 - k if relay else 0, c, slice(2 * n, 2 * n + 2) if relay else ALL)
                copies.append(remote(v, v, pair(self.s["far2" if relay else "far"], p, n), ring.to(k)))
        return copies

    def _over(self, ks):
        x, y, slot, c = self.spot
        copies = []
        for k in ks:
            for p, (i, lo, w, colour) in enumerate(self.pieces):
                v = self._strip(i, lo, w, colour, k, c)
                copies.append(remote(v, v, pair(self.s["over"], p, k), device(x, y, slot + 1 - 2 * c)))
        return copies

    def far(self):
        if not self.in_vmem:
            for cp in self._own_rows():
                cp.wait()
        landed(self._near(not self.direct))
        start(self._far(False))
        start(self._over([0]))

    def far2(self):
        landed(self._far(False))
        start(self._far(True))
        start(self._over([1, 3]))

    def over(self):
        landed(self._far(True))
        start(self._over([2]))

    def finish(self):
        landed(self._over(range(4)))
        self._all_of(self.s["line"][0])
        for copies in (self._near(False), self._near(True), self._far(False), self._far(True), self._over(range(4))):
            left(copies)


class Scatter:
    def __init__(self, arrays, pieces, in_vmem=False):
        self.arrays, self.pieces, self.in_vmem = arrays, pieces, in_vmem

    def scratch(self):
        P = len(self.pieces)
        both = lambda *s: [DMA(s), DMA(s)]
        per = lambda *lead: [pltpu.VMEM((*lead, self._m(i), LINE, w), BF) for i, lo, w, _ in self.pieces]
        half = [pltpu.VMEM((2, 2, self._m(i), LINE, w), BF) for i, lo, w, _ in self.pieces]
        return dict(
            own=per(X, Y), other=per(X, Y), h1=half, f1=per(2, 4), t=per(4),
            h2=per(), f2=per(3),
            zs=[pltpu.VMEM((LINE, a[0], a[1] // 2), BF) for a in self.arrays], zr=[pltpu.VMEM((LINE, a[0], a[1] // 2), BF) for a in self.arrays],
            get=DMA((P,)), over=both(P), a=both(P, 2), a2=both(P, 2), b=both(P, 2), b2=both(P, 3),
            line=both(len(self.arrays)),
        )

    def _m(self, i):
        return 3 if self.arrays[i][0] == THIN else LINE // 2

    def _parts(self, i):
        h = self._m(i) // 2
        return pl.ds(0, h), pl.ds(h, self._m(i) - h)

    def outs(self):
        return [jax.ShapeDtypeStruct((1, a[0], w), BF) for a in self.arrays for _, w in a[2] or [(0, a[1])]]

    def bind(self, ins, outs, s):
        self.ins, self.res, self.s = ins, outs, s
        self.spot = place()

    def _each(self):
        return [(p, i, lo, w, colour) for p, (i, lo, w, colour) in enumerate(self.pieces)]

    def _view(self, i, lo, w, core):
        return self.ins[i].at[:, :, :, :, cols(core * (self.arrays[i][1] // 2) + lo, w)]

    def _over(self):
        x, y, slot, c = self.spot
        return [remote(self._view(i, lo, w, 1 - c), self.s["other"][p], pair(self.s["over"], p), device(x, y, slot + 1 - 2 * c))
                for p, i, lo, w, colour in self._each()]

    def _get(self):
        return [pltpu.make_async_copy(self._view(i, lo, w, self.spot[3]), self.s["own"][p], self.s["get"].at[p]) for p, i, lo, w, colour in self._each()]

    def down(self):
        start(self._over())
        if not self.in_vmem:
            start(self._get())

    def _target(self, p, colour, k):
        x, y, _, _ = self.spot
        own = self.s["own"][p]
        return own.at[on(x, k)] if colour == 0 else own.at[:, on(y, k)]

    def _a(self):
        copies = []
        for p, i, lo, w, colour in self._each():
            for n, k in BOTH:
                copies.append(remote(self._target(p, colour, 2).at[pl.ds(2 * n, 2)], self.s["h1"][p].at[n], pair(self.s["a"], p, n), Ring(colour == 0).to(k)))
        return copies

    def _a2(self):
        return [remote(self._target(p, colour, k), self.s["f1"][p].at[n], pair(self.s["a2"], p, n), Ring(colour == 0).to(k))
                for p, i, lo, w, colour in self._each() for n, k in BOTH]

    def _of(self, copies, p):
        n = len(copies) // len(self.pieces)
        return copies[n * p : n * p + n]

    def near(self):
        over, a = self._over(), self._a()
        get = None if self.in_vmem else self._get()
        for p, i, lo, w, colour in self._each():
            if get:
                get[p].wait()
            over[p].wait_recv()
            own, other = self.s["own"][p], self.s["other"][p]
            mine = self._view(i, lo, w, self.spot[3]) if self.in_vmem else own

            def add(n, _):
                at = n // Y, lax.rem(n, Y)
                own[at] = (mine[at].astype(F32) + other[at].astype(F32)).astype(BF)

            lax.fori_loop(0, X * Y, add, None)
            start(self._of(a, p))

    def near2(self):
        a, a2 = self._a(), self._a2()
        for p, i, lo, w, colour in self._each():
            landed(self._of(a, p))
            for n, k in BOTH:
                to, h = self._target(p, colour, k), self.s["h1"][p]
                for q in range(2):
                    to[2 * n + q] = (to[2 * n + q].astype(F32) + h[n, q].astype(F32)).astype(BF)
            start(self._of(a2, p))

    def _b(self):
        copies = []
        x, y, _, _ = self.spot
        for p, i, lo, w, colour in self._each():
            ring = Ring(colour == 1)
            for (n, k), part in zip(BOTH, self._parts(i)):
                copies.append(remote(self.s["t"][p].at[on(ring.at, 2), part], self.s["h2"][p].at[part], pair(self.s["b"], p, n), ring.to(k)))
        return copies

    def _b2(self):
        copies = []
        for p, i, lo, w, colour in self._each():
            ring = Ring(colour == 1)
            copies += [remote(self.s["t"][p].at[on(ring.at, k)], self.s["f2"][p].at[n], pair(self.s["b2"], p, n), ring.to(k)) for n, k in self._ways()]
        return copies

    def _ways(self):
        return BOTH + DIRECT if self.in_vmem else BOTH

    def far(self):
        a2, b = self._a2(), self._b2() if self.in_vmem else self._b()
        for p, i, lo, w, colour in self._each():
            landed(self._of(a2, p))
            own, f, t = self._target(p, colour, 0), self.s["f1"][p], self.s["t"][p]

            def add(n, _):
                t[n] = (own[n].astype(F32) + f[0, n].astype(F32) + f[1, n].astype(F32)).astype(BF)

            lax.fori_loop(0, 4, add, None)
            start(self._of(b, p))

    def far2(self):
        b, b2 = self._b(), self._b2()
        for p, i, lo, w, colour in self._each():
            landed(self._of(b, p))
            ring, t = Ring(colour == 1), self.s["t"][p]
            for (_, k), part in zip(BOTH, self._parts(i)):
                at = on(ring.at, k), part
                t[at] = (t[at].astype(F32) + self.s["h2"][p][part].astype(F32)).astype(BF)
            start(self._of(b2, p))

    def _line(self):
        x, y, slot, _ = self.spot

        def each(k, _):
            to = on(slot, k, LINE)
            start([remote(zs.at[to], zr.at[slot], pair(self.s["line"], i), device(x, y, to)) for i, (zs, zr) in enumerate(zip(self.s["zs"], self.s["zr"]))])

        lax.fori_loop(1, LINE, each, None)

    def _all_of(self, i, sems):
        some = self.s["zr"][i].at[pl.ds(0, LINE - 1)]
        pltpu.make_async_copy(some, some, sems.at[i]).wait()

    def line(self):
        b2, slot = self._b2(), self.spot[2]
        for p, i, lo, w, colour in self._each():
            landed(self._of(b2, p))
            f = self.s["f2"][p]
            total = self.s["t"][p][Ring(colour == 1).at].astype(F32)
            for n, _ in self._ways():
                total += f[n].astype(F32)
            zs = self.s["zs"][i]
            if self.arrays[i][0] == THIN:
                total = total.reshape(TALL, w)
                for d in range(LINE):
                    zs[d, :, lo : lo + w] = total[THIN * d : THIN * d + THIN].astype(BF)
            else:
                zs[:, :, lo : lo + w] = total.reshape(LINE, -1, w).astype(BF)
        self._line()
        for zs, zr in zip(self.s["zs"], self.s["zr"]):
            zr[slot] = zs[slot]

    def finish(self):
        n = 0
        for i, (r, width, parts) in enumerate(self.arrays):
            zr = self.s["zr"][i]
            self._all_of(i, self.s["line"][1])
            sums = []
            for core in range(C):
                total = zr[core].astype(F32)
                for k in range(1, Z):
                    total += zr[C * k + core].astype(F32)
                sums.append(total.astype(BF))
            whole = jnp.concatenate(sums, axis=1)
            for first, w in parts or [(0, width)]:
                self.res[n][0] = whole[:, first : first + w]
                n += 1
            self._all_of(i, self.s["line"][0])
        for copies in (self._over(), self._a(), self._a2(), [] if self.in_vmem else self._b(), self._b2()):
            left(copies)


QKV = ([(THIN, WIDTH + 2 * HEAD, [(0, WIDTH), (WIDTH, HEAD), (WIDTH + HEAD, HEAD)])], [(0, 0, 256, 0), (0, 256, 256, 1)])
REST = (
    [(THIN, WIDTH, ()), (THIN, HIDDEN_UNITS, ()), (THIN, HIDDEN_UNITS, ()), (8, WIDTH, ())],
    [(1, 0, 1024, 0), (2, 0, 1024, 1), (0, 0, 384, 0), (3, 0, 128, 0), (3, 128, 256, 1)],
)


THETA = 10000
NAMES = ("wq", "wk", "wv", "wo", "w_gate", "w_up", "w_down")
G = 6
TB = 512
NT = 4
MB, MT, FJ, MJ = 1024, 2, 512, 4
BLOCKS = NT * (NT + 1) // 2
NEG = -1e30
HIDDEN = 2 * NEG
LOG2E = 1.4426950408889634
VMEM = 56 * 2**20
EPS = 1e-6


def mm(a, b):
    return lax.dot_general(a, b, (((1,), (0,)), ((), ())), preferred_element_type=F32)


def mm_t(a, b):
    return lax.dot_general(a, b, (((1,), (1,)), ((), ())), preferred_element_type=F32)


def norm(h):
    scale = lax.rsqrt(jnp.mean(h * h, -1, keepdims=True) + EPS)
    return (h * scale).astype(BF), scale


def norm_back(h, g):
    scale = lax.rsqrt(jnp.mean(h * h, -1, keepdims=True) + EPS)
    return scale * (g - h * (scale * scale * jnp.mean(g * h, -1, keepdims=True)))


def turn_table(tokens):
    half = HEAD // 2
    freq = np.float64(THETA) ** (-np.arange(half) / half)
    place = np.concatenate([HEAD * np.arange(tokens // HEAD), np.arange(HEAD)]) * 1.0
    angle = place[:, None] * np.concatenate([freq, freq])
    return jnp.asarray(np.stack([np.cos(angle), np.sin(angle)]).astype(np.float32))


def turner(table, n):
    far, near = pl.ds(n, 1), slice(-HEAD, None)
    fc, fs, nc, ns = table[0, far, :], table[1, far, :], table[0, near, :], table[1, near, :]
    sin = fs * nc + fc * ns
    return fc * nc - fs * ns, jnp.where(lax.broadcasted_iota(jnp.int32, sin.shape, 1) < HEAD // 2, -sin, sin)


def swap(t):
    return pltpu.roll(t, HEAD // 2, 1)


def whole(shape):
    return pl.BlockSpec(shape, lambda *_: (0,) * len(shape))


def stage(n, plan):
    for at, todo in plan.items():

        @pl.when(n == at)
        def _():
            for do in todo:
                do()


def block_of(m):
    i = sum((m >= (r * (r + 1)) // 2).astype(jnp.int32) for r in range(1, NT))
    return i, m - (i * (i + 1)) // 2


def rows(b, size=TB, first=0):
    return pl.ds(pl.multiple_of(b * TB + first, HEAD), size)


def wait(copies):
    for cp in copies:
        cp.wait()


HALVES = ((0, 0), (TB // 2, TB // 2))


def masked(s, key, query):
    return lax.broadcasted_iota(jnp.int32, s.shape, 0) + key <= lax.broadcasted_iota(jnp.int32, s.shape, 1) + query


def _front(x_ref, table_ref, *rest, gq, gr):
    weights, rest = rest[: len(NAMES)], rest[len(NAMES) :]
    hbm, outs, (ours, qkv_s, lse_s, table_s, vt_s, top_s, mix_s, w_s, sems, o_sem, sq, sr) = rest[:6], rest[6:11], rest[11:]
    q_s, k_s, v_s, at_s, o_s, x_s = ours
    n = pl.program_id(0)
    gq.bind(qkv_s, (w_s,), sq, own=weights[:3])
    gr.bind(weights[3:], outs[1:], sr)
    fetch = [pltpu.make_async_copy(a, b, sems.at[len(ours) + m]) for m, (a, b) in enumerate([*zip(weights, qkv_s), (x_ref, x_s), (table_ref, table_s)])]
    lse_out = pltpu.make_async_copy(lse_s, hbm[5], sems.at[5])
    keep = [pltpu.make_async_copy(a, b, sems.at[m]) for m, (a, b) in enumerate(zip((q_s, k_s, v_s, at_s, w_s), (*hbm[:4], outs[0])))]
    o_out = lambda b: pltpu.make_async_copy(o_s.at[:, rows(b)], hbm[4].at[:, rows(b)], o_sem.at[b])

    def normed(first, last):
        for b in range(first, last):
            at = slice(b * TB, b * TB + TB)
            a, _ = norm(x_s[at, :].astype(F32))
            x_s[at, :] = a
            at_s[:, at] = a.T

    def early():
        start(fetch)
        hello()
        wait(fetch)
        normed(0, NT // 2)

    def late():
        normed(NT // 2, NT)

    def keep_all():
        start(keep)

    stage(n, {
        0: [early, meet, gq.down, gr.down, late, gq.lay, gq.near, gq.far, gr.lay, gr.near, gq.far2, gq.over, gr.near2, gq.finish],
        2: [gr.far],
        NT: [keep_all],
        10: [gr.far2],
        13: [gr.over],
    })

    @pl.when(n < NT)
    def _():
        a = x_s[rows(n), :]
        y = mm(a, w_s[...].reshape(a.shape[1], -1)).astype(BF)
        for i in range(TB // HEAD):
            here, there = slice(HEAD * i, HEAD * i + HEAD), rows(n, HEAD, HEAD * i)
            cos, sin = turner(table_s, n * (TB // HEAD) + i)
            for h in range(G + 1):
                t = y[here, HEAD * h : HEAD * h + HEAD].astype(F32)
                t = (t * cos + swap(t) * sin).astype(BF)
                if h < G:
                    q_s[h, there, :] = t
                else:
                    k_s[there, :] = t
        v = y[:, (G + 1) * HEAD :]
        v_s[rows(n), :] = v
        vt_s[n] = jnp.concatenate([v.T, jnp.ones((8, TB), BF)], axis=0)

    i, j = block_of(n - NT)
    e = HEAD**-0.5 * LOG2E

    @pl.when((n >= NT) & (j == 0))
    def _():
        top_s[...] = jnp.full(top_s.shape, NEG, F32)
        mix_s[...] = jnp.zeros(mix_s.shape, F32)

    def block(key, keys, query, mask):
        k = k_s[rows(j, keys, key), :]
        scores = [mm_t(k, q_s[h, rows(i, TB - query, query), :]) for h in range(G)]
        weights, keeps = [], []
        for h, s in enumerate(scores):
            if mask:
                s = jnp.where(masked(s, key, query), s, HIDDEN)
            old = top_s[h : h + 1, query:]
            top = jnp.maximum(old, s.max(axis=0, keepdims=True))
            top_s[h : h + 1, query:] = top
            weights.append(jnp.exp2((s - top) * e).astype(BF))
            keeps.append(jnp.exp2((old - top) * e))
        for h in range(G):
            mix_s[h, :, query:] = mix_s[h, :, query:] * keeps[h] + mm(vt_s[j, :, key : key + keys], weights[h])

    @pl.when((n >= NT) & (j < i))
    def _():
        block(0, TB, 0, False)

    @pl.when((n >= NT) & (j == i))
    def _():
        for key, query in HALVES:
            block(key, TB // 2, query, True)
        for h in range(G):
            total = mix_s[h, HEAD : HEAD + 1, :]
            o_s[h, rows(i), :] = (mix_s[h, :HEAD, :] * (1 / total)).T.astype(BF)
            lse_s[h : h + 1, rows(i)] = top_s[h : h + 1, :] * HEAD**-0.5 + jnp.log(total)
        o_out(i).start()

    def finish():
        lse_out.start()
        gr.finish()
        lse_out.wait()
        wait(keep)
        wait([o_out(b) for b in range(NT)])

    stage(n, {NT + BLOCKS - 1: [finish]})


def front(x, table, weights, gq, gr):
    T, D = x.shape
    hbm = pl.BlockSpec(memory_space=pltpu.HBM)
    mine = [(G, T, HEAD), (T, HEAD), (T, HEAD), (D, T), (G, T, HEAD)]
    outs = [jax.ShapeDtypeStruct(s, BF) for s in mine] + [jax.ShapeDtypeStruct((8, T), F32)] + gq.outs() + gr.outs()
    return pl.pallas_call(
        functools.partial(_front, gq=gq, gr=gr),
        grid=(NT + BLOCKS,),
        in_specs=[hbm] * (2 + len(weights)),
        out_specs=[hbm] * len(outs),
        out_shape=outs,
        scratch_shapes=[[pltpu.VMEM(s, BF) for s in (*mine, (T, D))], [pltpu.VMEM(a.shape, BF) for a in weights[:3]], pltpu.VMEM((8, T), F32), pltpu.VMEM(table.shape, F32),
                        pltpu.VMEM((NT, HEAD + 8, TB), BF), pltpu.VMEM((8, TB), F32), pltpu.VMEM((G, HEAD + 8, TB), F32),
                        pltpu.VMEM((X, Y, TALL, 1024), BF), DMA((11,)), DMA((NT,)), gq.scratch(), gr.scratch()],
        compiler_params=pltpu.CompilerParams(dimension_semantics=("arbitrary",), vmem_limit_bytes=VMEM, collective_id=1, has_side_effects=True),
        name="front",
    )(x, table, *weights)


def _back(*refs, sq, sr):
    hbm, then, grads, dx_ref, outs, rest = refs[:5], refs[5:11], refs[11:15], refs[15], refs[16:23], refs[23:]
    ours, more, sems, more_sem, dq_s, dk_s, dv_s, d_s, acc, dw_s, rq, rr = rest
    q_s, do_s, k_s, v_s, at_s = ours
    lse_ref, delta_ref, table_s, w_s, x_s, dh_s = more
    n = pl.program_id(0)
    sq.bind((dw_s,), outs[:3], rq)
    sr.bind(grads, outs[3:], rr)

    def fetch(b):
        at = [(ALL, rows(b)), (ALL, rows(b)), (rows(b),), (rows(b),), (ALL, rows(b))]
        return [pltpu.make_async_copy(src.at[a], dst.at[a], sems.at[m, b]) for m, (src, dst, a) in enumerate(zip(hbm, ours, at))]

    whole_ones = [pltpu.make_async_copy(src, dst, more_sem.at[m]) for m, (src, dst) in enumerate(zip(then, more))]

    def fetch_all():
        start(whole_ones[:3])
        for b in range(NT):
            start(fetch(b))
        start(whole_ones[3:])

    def rest_here():
        wait(whole_ones[3:])

    i, j = block_of(n)
    stage(n, {0: [fetch_all, hello]})

    @pl.when((n < BLOCKS) & (j == 0))
    def _():
        wait(fetch(i))

        @pl.when(n == 0)
        def _():
            wait(whole_ones[:3])

    stage(n, {1: [meet, sr.down], 3: [sr.near], 5: [sr.near2], 9: [sr.far]})
    scale = HEAD**-0.5
    e = scale * LOG2E

    @pl.when(n == 0)
    def _():
        dk_s[...] = jnp.zeros_like(dk_s)
        dv_s[...] = jnp.zeros_like(dv_s)
        acc[...] = jnp.zeros_like(acc)

    @pl.when((n < BLOCKS) & (j == 0))
    def _():
        dq_s[...] = jnp.zeros_like(dq_s)

    def block(key, keys, query, mask):
        here, there = rows(j, keys, key), rows(i, TB - query, query)
        k, v = k_s[here, :], v_s[here, :]
        kt = k.T
        qs = [q_s[h, there, :] for h in range(G)]
        dos = [do_s[h, there, :] for h in range(G)]
        scores = [mm_t(k, q) for q in qs]
        dps = [mm_t(v, do) for do in dos]
        for h in range(G):
            p = jnp.exp2(scores[h] * e - lse_ref[h : h + 1, there] * LOG2E)
            if mask:
                p = jnp.where(masked(p, key, query), p, 0.0)
            ds = (p * (dps[h] - delta_ref[h : h + 1, there])).astype(BF)
            dv_s[j, key : key + keys] += mm(p.astype(BF), dos[h])
            dk_s[j, key : key + keys] += mm(ds, qs[h])
            dq_s[h, :, query:] += mm(kt, ds)

    def turn_back(t, b, r):
        cos, sin = turner(table_s, b * (TB // HEAD) + r)
        t = t[HEAD * r : HEAD * r + HEAD].astype(F32)
        return (t * cos - swap(t) * sin).astype(BF)

    @pl.when((n < BLOCKS) & (j < i))
    def _():
        block(0, TB, 0, False)

    @pl.when((n < BLOCKS) & (j == i))
    def _():
        for key, query in HALVES:
            block(key, TB // 2, query, True)
        for h in range(G):
            dq = (dq_s[h] * scale).T.astype(BF)
            for r in range(TB // HEAD):
                d_s[i, HEAD * r : HEAD * r + HEAD, HEAD * h : HEAD * h + HEAD] = turn_back(dq, i, r)
        acc[:, : G * HEAD] += mm(at_s[:, rows(i)], d_s[i, :, : G * HEAD])

    def last():
        for b in range(NT):
            dk = (dk_s[b] * scale).astype(BF)
            for r in range(TB // HEAD):
                d_s[b, HEAD * r : HEAD * r + HEAD, G * HEAD : (G + 1) * HEAD] = turn_back(dk, b, r)
            d_s[b, :, (G + 1) * HEAD :] = dv_s[b].astype(BF)
            acc[:, G * HEAD :] += mm(at_s[:, rows(b)], d_s[b, :, G * HEAD :])
        dw_s[...] = acc[...].astype(BF).reshape(dw_s.shape)

    stage(n, {BLOCKS: [sr.far2, last, sq.down, rest_here], BLOCKS + 1: [sq.near, sr.line], BLOCKS + 2: [sq.near2], BLOCKS + 3: [sq.far]})

    @pl.when(n >= BLOCKS)
    def _():
        da = mm_t(d_s[n - BLOCKS], w_s[...])
        at = rows(n - BLOCKS)
        dx_ref[...] = (dh_s[at, :].astype(F32) + norm_back(x_s[at, :].astype(F32), da)).astype(BF)

    stage(n, {BLOCKS + NT - 1: [sq.line, sr.finish, sq.finish]})


def back(q, k, v, do, lse, delta, at, x, dh, w, table, grads, sq, sr):
    T, D = x.shape
    hbm = pl.BlockSpec(memory_space=pltpu.HBM)
    outs = sq.outs() + sr.outs()
    ins, then = (q, do, k, v, at), (lse, delta, table, w, x, dh)
    return pl.pallas_call(
        functools.partial(_back, sq=sq, sr=sr),
        grid=(BLOCKS + NT,),
        in_specs=[hbm] * (len(ins) + len(then) + len(grads)),
        out_specs=[pl.BlockSpec((TB, D), lambda n: (jnp.maximum(n - BLOCKS, 0), 0))] + [whole(o.shape) for o in outs],
        out_shape=[jax.ShapeDtypeStruct((T, D), BF)] + outs,
        scratch_shapes=[[pltpu.VMEM(a.shape, BF) for a in ins], [pltpu.VMEM(a.shape, a.dtype) for a in then], DMA((len(ins), NT)), DMA((len(then),)),
                        pltpu.VMEM((G, HEAD, TB), F32), pltpu.VMEM((NT, TB, HEAD), F32), pltpu.VMEM((NT, TB, HEAD), F32),
                        pltpu.VMEM((NT, TB, 1024), BF), pltpu.VMEM(w.shape, F32), pltpu.VMEM((X, Y, THIN, LINE, 1024), BF), sq.scratch(), sr.scratch()],
        compiler_params=pltpu.CompilerParams(dimension_semantics=("arbitrary",), vmem_limit_bytes=63 * 2**20, collective_id=2, has_side_effects=True),
        name="back",
    )(*ins, *then, *grads)


def _middle(x_ref, o_ref, wo_ref, dy_hbm, wg_hbm, wu_hbm, wd_hbm, dh_ref, do_ref, delta_ref, dwo_ref, dwg_hbm, dwu_hbm, dwd_hbm,
            h_s, b_s, bt_s, db_s, dy_s, wg_s, wu_s, wd_s, ao, ag, au, ad, tg, tu, td, dy_sem, in_sem, out_sem):
    n = pl.program_id(0)
    m = n - NT
    j, t = m // MT, lax.rem(m, MT)
    is_main = (m >= 0) & (m < MJ * MT)
    dy_in = pltpu.make_async_copy(dy_hbm, dy_s, dy_sem)

    def chunk(j):
        at, to = cols(j * FJ, FJ), lax.rem(j, 2)
        pairs = [(wg_hbm.at[:, at], wg_s), (wu_hbm.at[:, at], wu_s), (wd_hbm.at[at, :], wd_s)]
        return [pltpu.make_async_copy(src, dst.at[to], in_sem.at[i, to]) for i, (src, dst) in enumerate(pairs)]

    def grads(j):
        at = cols(j * FJ, FJ)
        pairs = [(tg, dwg_hbm.at[:, at]), (tu, dwu_hbm.at[:, at]), (td, dwd_hbm.at[at, :])]
        return [pltpu.make_async_copy(src, dst, out_sem.at[i]) for i, (src, dst) in enumerate(pairs)]

    @pl.when(n == 0)
    def _():
        start(chunk(0))
        dy_in.start()

    @pl.when(n < NT)
    def _():
        o = jnp.concatenate([o_ref[h] for h in range(G)], axis=1)
        h = (x_ref[...].astype(F32) + mm(o, wo_ref[...]).astype(BF).astype(F32)).astype(BF)
        h_s[rows(n), :] = h
        b, _ = norm(h.astype(F32))
        b_s[rows(n), :] = b
        bt_s[:, rows(n)] = b.T
        db_s[rows(n), :] = jnp.zeros((TB, db_s.shape[1]), F32)

    @pl.when(m == 0)
    def _():
        dy_in.wait()

    @pl.when(is_main & (t == 0))
    def _():
        wait(chunk(j))
        ag[...] = jnp.zeros_like(ag)
        au[...] = jnp.zeros_like(au)
        ad[...] = jnp.zeros_like(ad)

        @pl.when(j + 1 < MJ)
        def _():
            start(chunk(j + 1))

    @pl.when(is_main)
    def _():
        these, slot = pl.ds(pl.multiple_of(t * MB, MB), MB), lax.rem(j, 2)
        b, bt, dy = b_s[these, :], bt_s[:, these], dy_s[these, :]

        def into(c):
            return mm(b, wg_s[slot, :, c]), mm(b, wu_s[slot, :, c]), mm_t(dy, wd_s[slot, c, :])

        def point(gate, up, dact):
            dact = dact.astype(BF).astype(F32)
            sig = 0.5 + 0.5 * jnp.tanh(0.5 * gate)
            silu = gate * sig
            return (silu * up).astype(BF), (dact * up * (sig + silu * (1 - sig))).astype(BF), (dact * silu).astype(BF)

        strips = [slice(a, a + 256) for a in range(0, FJ, 256)]
        ahead, dbs = into(strips[0]), []
        for i, c in enumerate(strips):
            now, ahead = ahead, into(strips[i + 1]) if i + 1 < len(strips) else ()
            act, dgate, dup = point(*now)
            dbs.append(mm_t(dgate, wg_s[slot, :, c]) + mm_t(dup, wu_s[slot, :, c]))
            ag[:, c] += mm(bt, dgate)
            au[:, c] += mm(bt, dup)
            ad[c, :] += mm(act.T, dy)
        db_s[these, :] += sum(dbs[1:], dbs[0])

        @pl.when(t == MT - 1)
        def _():
            @pl.when(j > 0)
            def _():
                wait(grads(j - 1))

            tg[...] = ag[...].astype(BF)
            tu[...] = au[...].astype(BF)
            td[...] = ad[...].astype(BF)
            start(grads(j))

    last = m - MJ * MT

    @pl.when(last == 0)
    def _():
        ao[...] = jnp.zeros_like(ao)

    @pl.when(last >= 0)
    def _():
        at = rows(jnp.maximum(last, 0))
        dh = (dy_s[at, :].astype(F32) + norm_back(h_s[at, :].astype(F32), db_s[at, :]).astype(BF).astype(F32)).astype(BF)
        dh_ref[...] = dh
        do = mm_t(dh, wo_ref[...]).astype(BF)
        o = jnp.concatenate([o_ref[h] for h in range(G)], axis=1)
        prod = do.astype(F32) * o.astype(F32)
        for h in range(G):
            do_ref[h] = do[:, HEAD * h : HEAD * h + HEAD]
        delta_ref[...] = jnp.concatenate([prod[:, HEAD * h : HEAD * h + HEAD].sum(-1, keepdims=True) for h in range(G)]
                                         + [jnp.zeros((TB, 8 - G), F32)], axis=1).T
        ao[...] += mm(o.T, dh)

    @pl.when(last == NT - 1)
    def _():
        dwo_ref[...] = ao[...].astype(BF)
        wait(grads(MJ - 1))


def middle(x, dy, o, wo, wg, wu, wd):
    T, D = x.shape
    end = NT + MJ * MT
    late = lambda n: jnp.maximum(n - end, 0)
    ends = lambda n: jnp.where(n < NT, n, jnp.where(n < end, NT - 1, n - end))
    once = pl.BlockSpec(wo.shape, lambda n: (0, 0), pipeline_mode=pl.Buffered(1))
    hbm = pl.BlockSpec(memory_space=pltpu.HBM)
    buf = lambda *s, dtype=BF: pltpu.VMEM(s, dtype)
    return pl.pallas_call(
        _middle,
        grid=(end + NT,),
        in_specs=[pl.BlockSpec((TB, D), lambda n: (jnp.minimum(n, NT - 1), 0)), pl.BlockSpec((G, TB, HEAD), lambda n: (0, ends(n), 0)), once,
                  hbm, hbm, hbm, hbm],
        out_specs=[pl.BlockSpec((TB, D), lambda n: (late(n), 0)), pl.BlockSpec((G, TB, HEAD), lambda n: (0, late(n), 0)),
                   pl.BlockSpec((8, TB), lambda n: (0, late(n))), once, hbm, hbm, hbm],
        out_shape=[jax.ShapeDtypeStruct((T, D), BF), jax.ShapeDtypeStruct((G, T, HEAD), BF), jax.ShapeDtypeStruct((8, T), F32),
                   *(jax.ShapeDtypeStruct(a.shape, BF) for a in (wo, wg, wu, wd))],
        scratch_shapes=[buf(T, D), buf(T, D), buf(D, T), buf(T, D, dtype=F32), buf(T, D), buf(2, D, FJ), buf(2, D, FJ), buf(2, FJ, D),
                        buf(D, D, dtype=F32), buf(D, FJ, dtype=F32), buf(D, FJ, dtype=F32), buf(FJ, D, dtype=F32), buf(D, FJ), buf(D, FJ), buf(FJ, D),
                        DMA(()), DMA((3, 2)), DMA((3,))],
        compiler_params=pltpu.CompilerParams(dimension_semantics=("arbitrary",), vmem_limit_bytes=67043328), name="middle",
    )(x, o, wo, dy, wg, wu, wd)


def _hand_over(*refs):
    *ends, bufs, big, sems = refs
    srcs, dsts = ends[: len(bufs)], ends[len(bufs) :]

    def pairs(src, dst, buf, sem):
        return pltpu.make_async_copy(src, buf, sem.at[0]), pltpu.make_async_copy(buf, dst, sem.at[1])

    copies = [pairs(s, d, b, sems.at[m]) for m, (s, d, b) in enumerate(zip(srcs, dsts, bufs))]
    some = [pl.ds(i * MB // NT, MB // NT) for i in range(srcs[0].shape[1] * NT // MB)]
    copies = [pairs(srcs[0].at[:, at], dsts[0].at[:, at], bufs[0].at[:, at], big.at[m]) for m, at in enumerate(some)] + copies[1:]
    start([get for get, _ in copies])
    for get, put in copies:
        get.wait()
        put.start()
    wait([put for _, put in copies])


def hand_over(results):
    hbm, n = pl.BlockSpec(memory_space=pltpu.HBM), len(results)
    return pl.pallas_call(
        _hand_over, in_specs=[hbm] * n, out_specs=[hbm] * n, out_shape=[jax.ShapeDtypeStruct(a.shape, BF) for a in results],
        scratch_shapes=[[pltpu.VMEM(a.shape, BF) for a in results], DMA((NT * NT, 2)), DMA((n, 2))],
        compiler_params=pltpu.CompilerParams(vmem_limit_bytes=2**24), name="hand_over",
    )(*results)


def solution(mesh):
    gq, gr, sq, sr = Gather(*QKV, in_vmem=True), Gather(*REST), Scatter(*QKV, in_vmem=True), Scatter(*REST)

    def step(x, dy, *weights):
        x, dy = x[0], dy[0]
        T, D = x.shape
        table = turn_table(T)
        q, k, v, at, o, lse, w, *rest = front(x, table, weights, gq, gr)
        rest = [a.reshape(D, -1) for a in rest[:3]] + [rest[3].reshape(-1, D)]
        dh, do, delta, *grads = middle(x, dy, o, *rest)
        grads = [g.reshape(X, Y, -1, LINE, g.shape[1]) for g in grads]
        dx, *by_w = back(q, k, v, do, lse, delta, at, x, dh, w.reshape(D, -1), table, grads, sq, sr)
        return hand_over([dx[None], *by_w])

    states, cut = P(("rep", "dp"), None, None), P(None, "dp", None)
    return jax.shard_map(
        step,
        mesh=mesh,
        in_specs=(states, states) + (cut,) * 7,
        out_specs=(states,) + (P("rep", "dp", None),) * 7,
        check_vma=False,
    )
```

```python
import functools

import jax
import jax.numpy as jnp
import numpy as np
from jax import lax
from jax.experimental import pallas as pl
from jax.experimental.pallas import tpu as pltpu
from jax.sharding import PartitionSpec as P


F32, BF = jnp.float32, jnp.bfloat16
X, Y, Z, C = 4, 4, 8, 2
LINE = Z * C
DMA = pltpu.SemaphoreType.DMA
THIN = 3
TALL = THIN * LINE
WIDTH, HIDDEN_UNITS, HEAD = 768, 2048, 128
ALL = slice(None)
DIRECT = ((2, 2),)
BOTH = ((0, 1), (1, 3))


def place():
    me = lax.axis_index("dp")
    return me // (LINE * Y), lax.rem(me // LINE, Y), lax.rem(me, LINE), lax.rem(me, C)


def device(x, y, slot):
    return {"dp": (x * Y + y) * LINE + slot}


def on(a, k, n=4):
    return lax.rem(a + k, n)


def remote(src, dst, sems, where):
    send, recv = sems
    return pltpu.make_async_remote_copy(src_ref=src, dst_ref=dst, send_sem=send, recv_sem=recv, device_id=where, device_id_type=pl.DeviceIdType.MESH)


def start(copies):
    for cp in copies:
        cp.start()


def landed(copies):
    for cp in copies:
        cp.wait_recv()


def left(copies):
    for cp in copies:
        cp.wait_send()


def peers():
    x, y, slot, _ = place()
    who = [device(x, y, on(slot, k, LINE)) for k in range(1, LINE)]
    for k in range(1, X):
        who += [device(on(x, k), y, slot), device(x, on(y, k), slot)]
    return who


def hello():
    for d in peers():
        pl.semaphore_signal(pltpu.get_barrier_semaphore(), inc=1, device_id=d, device_id_type=pl.DeviceIdType.MESH)


def meet():
    pl.semaphore_wait(pltpu.get_barrier_semaphore(), len(peers()))


def cols(first, size):
    return pl.ds(pl.multiple_of(first, 128), size)


def pair(sems, *index):
    return sems[0].at[index], sems[1].at[index]


class Ring:
    def __init__(self, along_x):
        x, y, slot, c = place()
        self.at = x if along_x else y
        self.to = lambda k: device(on(x, k), y, slot) if along_x else device(x, on(y, k), slot)


class Gather:
    def __init__(self, arrays, pieces, in_vmem=False):
        self.arrays, self.pieces, self.in_vmem, self.direct = arrays, pieces, in_vmem, in_vmem

    def scratch(self):
        A, P = len(self.arrays), len(self.pieces)
        both = lambda *s: [DMA(s), DMA(s)]
        wide = [n if parts else n // 2 for _, n, parts in self.arrays]
        inputs = sum(max(len(a[2]), 1) for a in self.arrays)
        return dict(
            blocks=[pltpu.VMEM((LINE, a[0], w), BF) for a, w in zip(self.arrays, wide)],
            rows=[pltpu.VMEM((TALL, w) if a[0] == THIN else (8, 128), BF) for a, w in zip(self.arrays, wide)],
            tall=pltpu.VMEM((TALL, max(wide)), F32),
            own=DMA((inputs,)), put=DMA((P,)), line=both(A),
            near=both(P, 3), far=both(P, 2), near2=both(P, 2), far2=both(P, 2), over=both(P, 4),
        )

    def outs(self):
        return [jax.ShapeDtypeStruct((X, Y, TALL, a[1]) if a[0] == THIN else (X, Y, LINE, a[0], a[1]), BF) for a in self.arrays]

    def bind(self, ins, outs, s, own=None):
        self.ins, self.own, self.res, self.s = ins, own or ins, outs, s
        self.spot = place()

    def _parts(self, slot, core, ins):
        out = []
        for i, (r, width, parts) in enumerate(self.arrays):
            half, dst = width // 2, self.s["blocks"][i].at[slot]
            for first, w in parts:
                out.append((len(out), i, ins[len(out)].at[0], dst.at[:, pl.ds(first, w)]))
            if not parts:
                out.append((len(out), i, ins[len(out)].at[0, :, cols(core * half, half)], dst))
        return out

    def _line(self):
        x, y, slot, _ = self.spot

        def each(k, _):
            to = on(slot, k, LINE)
            start([remote(src, dst, pair(self.s["line"], i), device(x, y, to)) for n, i, src, dst in self._parts(slot, lax.rem(to, C), self.ins)])

        lax.fori_loop(1, LINE, each, None)

    def _all_of(self, sems):
        for i, b in enumerate(self.s["blocks"]):
            some = b.at[pl.ds(0, LINE - 1)]
            pltpu.make_async_copy(some, some, sems.at[i]).wait()

    def _own(self):
        _, _, slot, c = self.spot
        return [pltpu.make_async_copy(src, dst, self.s["own"].at[n]) for n, i, src, dst in self._parts(slot, c, self.own)]

    def down(self):
        self._line()
        start(self._own())

    def lay(self):
        for cp in self._own():
            cp.wait()
        self._all_of(self.s["line"][1])
        tall = self.s["tall"]
        for i, b in enumerate(self.s["blocks"]):
            if self.arrays[i][0] == THIN:
                w = b.shape[2]
                for d in range(LINE):
                    tall[THIN * d : THIN * d + THIN, :w] = b[d].astype(F32)
                self.s["rows"][i][...] = tall[:, :w].astype(BF)

    def _view(self, i, lo, w, xs, ys, core, rows=ALL):
        at = cols(core * (self.arrays[i][1] // 2) + lo, w)
        if rows == slice(LINE, None) and self.arrays[i][0] == THIN:
            rows = pl.ds(LINE, 2 * LINE)
        return self.res[i].at[xs, ys, rows, at] if self.arrays[i][0] == THIN else self.res[i].at[xs, ys, rows, :, at]

    def _half(self, i, k):
        n = LINE if self.arrays[i][0] == THIN else LINE // 2
        return slice(n, None) if k else slice(n)

    def _put(self):
        x, y, _, c = self.spot
        out = []
        for p, (i, lo, w, colour) in enumerate(self.pieces):
            r, n, parts = self.arrays[i]
            at = cols(c * (n // 2) + lo, w) if parts else pl.ds(lo, w)
            src = self.s["rows"][i].at[:, at] if r == THIN else self.s["blocks"][i].at[:, :, at]
            out.append((p, i, lo, w, colour, src))
        return out

    def _near(self, relay):
        x, y, _, c = self.spot
        copies = []
        for p, i, lo, w, colour, src in self._put():
            ring = Ring(colour == 1)
            for n, k in () if relay and self.direct else BOTH + DIRECT if self.direct else BOTH:
                if relay:
                    back = (on(x, 4 - k), y) if colour == 1 else (x, on(y, 4 - k))
                    v = self._view(i, lo, w, *back, c, self._half(i, n))
                    copies.append(remote(v, v, pair(self.s["near2"], p, n), ring.to(k)))
                else:
                    copies.append(remote(src, self._view(i, lo, w, x, y, c), pair(self.s["near"], p, n), ring.to(k)))
        return copies

    def _own_rows(self):
        x, y, _, c = self.spot
        return [pltpu.make_async_copy(src, self._view(i, lo, w, x, y, c), self.s["put"].at[p]) for p, i, lo, w, colour, src in self._put()]

    def near(self):
        start(self._near(False))
        if self.in_vmem:
            x, y, _, c = self.spot
            for rows, res in zip(self.s["rows"], self.res):
                n = rows.shape[1] // 2
                res[x, y, :, cols(c * n, n)] = rows[:, cols(c * n, n)]
        else:
            start(self._own_rows())

    def near2(self):
        landed(self._near(False))
        start(self._near(True))

    def _strip(self, i, lo, w, colour, k, core, half=ALL):
        x, y, _, _ = self.spot
        return self._view(i, lo, w, on(x, k), half, core) if colour == 0 else self._view(i, lo, w, half, on(y, k), core)

    def _some(self, ps):
        return [(p, piece) for p, piece in enumerate(self.pieces) if not ps or p in ps]

    def _far(self, relay, ps=()):
        c, copies = self.spot[3], []
        for p, (i, lo, w, colour) in self._some(ps):
            ring = Ring(colour == 0)
            for n, k in BOTH:
                v = self._strip(i, lo, w, colour, 4 - k if relay else 0, c, slice(2 * n, 2 * n + 2) if relay else ALL)
                copies.append(remote(v, v, pair(self.s["far2" if relay else "far"], p, n), ring.to(k)))
        return copies

    def _over(self, ks, ps=()):
        x, y, slot, c = self.spot
        copies = []
        for k in ks:
            for p, (i, lo, w, colour) in self._some(ps):
                v = self._strip(i, lo, w, colour, k, c)
                copies.append(remote(v, v, pair(self.s["over"], p, k), device(x, y, slot + 1 - 2 * c)))
        return copies

    def far(self):
        if not self.in_vmem:
            for cp in self._own_rows():
                cp.wait()
        landed(self._near(not self.direct))
        start(self._far(False))
        start(self._over([0]))

    def far2(self, *ps):
        landed(self._far(False, ps))
        start(self._far(True, ps))
        start(self._over([1, 3], ps))

    def over(self, *ps):
        landed(self._far(True, ps))
        start(self._over([2], ps))

    def finish(self):
        landed(self._over(range(4)))
        self._all_of(self.s["line"][0])
        for copies in (self._near(False), self._near(True), self._far(False), self._far(True), self._over(range(4))):
            left(copies)


class Scatter:
    def __init__(self, arrays, pieces, in_vmem=False):
        self.arrays, self.pieces, self.in_vmem = arrays, pieces, in_vmem

    def scratch(self):
        P = len(self.pieces)
        both = lambda *s: [DMA(s), DMA(s)]
        per = lambda *lead: [pltpu.VMEM((*lead, self._m(i), LINE, w), BF) for i, lo, w, _ in self.pieces]
        half = [pltpu.VMEM((2, 2, self._m(i), LINE, w), BF) for i, lo, w, _ in self.pieces]
        return dict(
            own=per(X, Y), other=per(X, Y), h1=half, f1=per(2, 4), t=per(4),
            h2=per(), f2=per(3),
            zs=[pltpu.VMEM((LINE, a[0], a[1] // 2), BF) for a in self.arrays], zr=[pltpu.VMEM((LINE, a[0], a[1] // 2), BF) for a in self.arrays],
            get=DMA((P,)), over=both(P), a=both(P, 2), a2=both(P, 2), b=both(P, 2), b2=both(P, 3),
            line=both(len(self.arrays)),
        )

    def _m(self, i):
        return 3 if self.arrays[i][0] == THIN else LINE // 2

    def _parts(self, i):
        h = self._m(i) // 2
        return pl.ds(0, h), pl.ds(h, self._m(i) - h)

    def outs(self):
        return [jax.ShapeDtypeStruct((1, a[0], w), BF) for a in self.arrays for _, w in a[2] or [(0, a[1])]]

    def bind(self, ins, outs, s):
        self.ins, self.res, self.s = ins, outs, s
        self.spot = place()

    def _each(self):
        return [(p, i, lo, w, colour) for p, (i, lo, w, colour) in enumerate(self.pieces)]

    def _view(self, i, lo, w, core):
        return self.ins[i].at[:, :, :, :, cols(core * (self.arrays[i][1] // 2) + lo, w)]

    def _over(self):
        x, y, slot, c = self.spot
        return [remote(self._view(i, lo, w, 1 - c), self.s["other"][p], pair(self.s["over"], p), device(x, y, slot + 1 - 2 * c))
                for p, i, lo, w, colour in self._each()]

    def _get(self):
        return [pltpu.make_async_copy(self._view(i, lo, w, self.spot[3]), self.s["own"][p], self.s["get"].at[p]) for p, i, lo, w, colour in self._each()]

    def down(self):
        start(self._over())
        if not self.in_vmem:
            start(self._get())

    def _target(self, p, colour, k):
        x, y, _, _ = self.spot
        own = self.s["own"][p]
        return own.at[on(x, k)] if colour == 0 else own.at[:, on(y, k)]

    def _a(self):
        copies = []
        for p, i, lo, w, colour in self._each():
            for n, k in BOTH:
                copies.append(remote(self._target(p, colour, 2).at[pl.ds(2 * n, 2)], self.s["h1"][p].at[n], pair(self.s["a"], p, n), Ring(colour == 0).to(k)))
        return copies

    def _a2(self):
        return [remote(self._target(p, colour, k), self.s["f1"][p].at[n], pair(self.s["a2"], p, n), Ring(colour == 0).to(k))
                for p, i, lo, w, colour in self._each() for n, k in BOTH]

    def _of(self, copies, p):
        n = len(copies) // len(self.pieces)
        return copies[n * p : n * p + n]

    def near(self):
        over, a = self._over(), self._a()
        get = None if self.in_vmem else self._get()
        for p, i, lo, w, colour in self._each():
            if get:
                get[p].wait()
            over[p].wait_recv()
            own, other = self.s["own"][p], self.s["other"][p]
            mine = self._view(i, lo, w, self.spot[3]) if self.in_vmem else own

            def add(n, _):
                at = n // Y, lax.rem(n, Y)
                own[at] = (mine[at].astype(F32) + other[at].astype(F32)).astype(BF)

            lax.fori_loop(0, X * Y, add, None)
            start(self._of(a, p))

    def near2(self):
        a, a2 = self._a(), self._a2()
        for p, i, lo, w, colour in self._each():
            landed(self._of(a, p))
            for n, k in BOTH:
                to, h = self._target(p, colour, k), self.s["h1"][p]
                for q in range(2):
                    to[2 * n + q] = (to[2 * n + q].astype(F32) + h[n, q].astype(F32)).astype(BF)
            start(self._of(a2, p))

    def _b(self):
        copies = []
        x, y, _, _ = self.spot
        for p, i, lo, w, colour in self._each():
            ring = Ring(colour == 1)
            for (n, k), part in zip(BOTH, self._parts(i)):
                copies.append(remote(self.s["t"][p].at[on(ring.at, 2), part], self.s["h2"][p].at[part], pair(self.s["b"], p, n), ring.to(k)))
        return copies

    def _b2(self):
        copies = []
        for p, i, lo, w, colour in self._each():
            ring = Ring(colour == 1)
            copies += [remote(self.s["t"][p].at[on(ring.at, k)], self.s["f2"][p].at[n], pair(self.s["b2"], p, n), ring.to(k)) for n, k in self._ways()]
        return copies

    def _ways(self):
        return BOTH + DIRECT if self.in_vmem else BOTH

    def far(self):
        a2, b = self._a2(), self._b2() if self.in_vmem else self._b()
        for p, i, lo, w, colour in self._each():
            landed(self._of(a2, p))
            own, f, t = self._target(p, colour, 0), self.s["f1"][p], self.s["t"][p]

            def add(n, _):
                t[n] = (own[n].astype(F32) + f[0, n].astype(F32) + f[1, n].astype(F32)).astype(BF)

            lax.fori_loop(0, 4, add, None)
            start(self._of(b, p))

    def far2(self):
        b, b2 = self._b(), self._b2()
        for p, i, lo, w, colour in self._each():
            landed(self._of(b, p))
            ring, t = Ring(colour == 1), self.s["t"][p]
            for (_, k), part in zip(BOTH, self._parts(i)):
                at = on(ring.at, k), part
                t[at] = (t[at].astype(F32) + self.s["h2"][p][part].astype(F32)).astype(BF)
            start(self._of(b2, p))

    def _line(self):
        x, y, slot, _ = self.spot

        def each(k, _):
            to = on(slot, k, LINE)
            start([remote(zs.at[to], zr.at[slot], pair(self.s["line"], i), device(x, y, to)) for i, (zs, zr) in enumerate(zip(self.s["zs"], self.s["zr"]))])

        lax.fori_loop(1, LINE, each, None)

    def _all_of(self, i, sems):
        some = self.s["zr"][i].at[pl.ds(0, LINE - 1)]
        pltpu.make_async_copy(some, some, sems.at[i]).wait()

    def line(self):
        b2, slot = self._b2(), self.spot[2]
        for p, i, lo, w, colour in self._each():
            landed(self._of(b2, p))
            f = self.s["f2"][p]
            total = self.s["t"][p][Ring(colour == 1).at].astype(F32)
            for n, _ in self._ways():
                total += f[n].astype(F32)
            zs = self.s["zs"][i]
            if self.arrays[i][0] == THIN:
                total = total.reshape(TALL, w)
                for d in range(LINE):
                    zs[d, :, lo : lo + w] = total[THIN * d : THIN * d + THIN].astype(BF)
            else:
                zs[:, :, lo : lo + w] = total.reshape(LINE, -1, w).astype(BF)
        self._line()
        for zs, zr in zip(self.s["zs"], self.s["zr"]):
            zr[slot] = zs[slot]

    def finish(self):
        n = 0
        for i, (r, width, parts) in enumerate(self.arrays):
            zr = self.s["zr"][i]
            self._all_of(i, self.s["line"][1])
            sums = []
            for core in range(C):
                total = zr[core].astype(F32)
                for k in range(1, Z):
                    total += zr[C * k + core].astype(F32)
                sums.append(total.astype(BF))
            whole = jnp.concatenate(sums, axis=1)
            for first, w in parts or [(0, width)]:
                self.res[n][0] = whole[:, first : first + w]
                n += 1
            self._all_of(i, self.s["line"][0])
        for copies in (self._over(), self._a(), self._a2(), [] if self.in_vmem else self._b(), self._b2()):
            left(copies)


QKV = ([(THIN, WIDTH + 2 * HEAD, [(0, WIDTH), (WIDTH, HEAD), (WIDTH + HEAD, HEAD)])], [(0, 0, 256, 0), (0, 256, 256, 1)])
REST = (
    [(THIN, WIDTH, ()), (THIN, HIDDEN_UNITS, ()), (THIN, HIDDEN_UNITS, ()), (8, WIDTH, ())],
    [(1, 0, 1024, 0), (2, 0, 1024, 1), (0, 0, 384, 0), (3, 0, 128, 0), (3, 128, 256, 1)],
)


THETA = 10000
NAMES = ("wq", "wk", "wv", "wo", "w_gate", "w_up", "w_down")
G = 6
TB = 512
NT = 4
MB, MT, FJ, MJ = 1024, 2, 512, 4
BLOCKS = NT * (NT + 1) // 2
NEG = -1e30
HIDDEN = 2 * NEG
LOG2E = 1.4426950408889634
VMEM = 56 * 2**20
EPS = 1e-6


def mm(a, b):
    return lax.dot_general(a, b, (((1,), (0,)), ((), ())), preferred_element_type=F32)


def mm_t(a, b):
    return lax.dot_general(a, b, (((1,), (1,)), ((), ())), preferred_element_type=F32)


def norm(h):
    scale = lax.rsqrt(jnp.mean(h * h, -1, keepdims=True) + EPS)
    return (h * scale).astype(BF), scale


def norm_back(h, g):
    scale = lax.rsqrt(jnp.mean(h * h, -1, keepdims=True) + EPS)
    return scale * (g - h * (scale * scale * jnp.mean(g * h, -1, keepdims=True)))


def turn_table(tokens):
    half = HEAD // 2
    freq = np.float64(THETA) ** (-np.arange(half) / half)
    place = np.concatenate([HEAD * np.arange(tokens // HEAD), np.arange(HEAD)]) * 1.0
    angle = place[:, None] * np.concatenate([freq, freq])
    return jnp.asarray(np.stack([np.cos(angle), np.sin(angle)]).astype(np.float32))


def turner(table, n):
    far, near = pl.ds(n, 1), slice(-HEAD, None)
    fc, fs, nc, ns = table[0, far, :], table[1, far, :], table[0, near, :], table[1, near, :]
    sin = fs * nc + fc * ns
    return fc * nc - fs * ns, jnp.where(lax.broadcasted_iota(jnp.int32, sin.shape, 1) < HEAD // 2, -sin, sin)


def swap(t):
    return pltpu.roll(t, HEAD // 2, 1)


def whole(shape):
    return pl.BlockSpec(shape, lambda *_: (0,) * len(shape))


def stage(n, plan):
    for at, todo in plan.items():

        @pl.when(n == at)
        def _():
            for do in todo:
                do()


def block_of(m):
    i = sum((m >= (r * (r + 1)) // 2).astype(jnp.int32) for r in range(1, NT))
    return i, m - (i * (i + 1)) // 2


def rows(b, size=TB, first=0):
    return pl.ds(pl.multiple_of(b * TB + first, HEAD), size)


def wait(copies):
    for cp in copies:
        cp.wait()


HALVES = ((0, 0), (TB // 2, TB // 2))


def masked(s, key, query):
    return lax.broadcasted_iota(jnp.int32, s.shape, 0) + key <= lax.broadcasted_iota(jnp.int32, s.shape, 1) + query


def _front(x_ref, table_ref, *rest, gq, gr):
    weights, rest = rest[: len(NAMES)], rest[len(NAMES) :]
    hbm, outs, (ours, qkv_s, lse_s, table_s, vt_s, top_s, mix_s, w_s, sems, o_sem, sq, sr) = rest[:6], rest[6:11], rest[11:]
    q_s, k_s, v_s, at_s, o_s, x_s = ours
    n = pl.program_id(0)
    gq.bind(qkv_s, (w_s,), sq, own=weights[:3])
    gr.bind(weights[3:], outs[1:], sr)
    fetch = [pltpu.make_async_copy(a, b, sems.at[len(ours) + m]) for m, (a, b) in enumerate([*zip(weights, qkv_s), (x_ref, x_s), (table_ref, table_s)])]
    lse_out = pltpu.make_async_copy(lse_s, hbm[5], sems.at[5])
    keep = [pltpu.make_async_copy(a, b, sems.at[m]) for m, (a, b) in enumerate(zip((q_s, k_s, v_s, at_s, w_s), (*hbm[:4], outs[0])))]
    o_out = lambda b: pltpu.make_async_copy(o_s.at[:, rows(b)], hbm[4].at[:, rows(b)], o_sem.at[b])

    def normed(first, last):
        for b in range(first, last):
            at = slice(b * TB, b * TB + TB)
            a, _ = norm(x_s[at, :].astype(F32))
            x_s[at, :] = a
            at_s[:, at] = a.T

    def early():
        start(fetch)
        hello()
        wait(fetch)
        normed(0, NT // 2)

    def late():
        normed(NT // 2, NT)

    def keep_all():
        start(keep)

    stage(n, {
        0: [early, meet, gq.down, gr.down, late, gq.lay, gq.near, gq.far, gr.lay, gr.near, gq.far2, gq.over, gr.near2, gq.finish],
        1: [gr.far],
        NT: [keep_all],
        8: [functools.partial(gr.far2, 0, 1)],
        10: [functools.partial(gr.far2, 2, 3, 4)],
        12: [functools.partial(gr.over, 0, 1)],
        13: [functools.partial(gr.over, 2, 3, 4)],
    })

    @pl.when(n < NT)
    def _():
        a = x_s[rows(n), :]
        y = mm(a, w_s[...].reshape(a.shape[1], -1)).astype(BF)
        for i in range(TB // HEAD):
            here, there = slice(HEAD * i, HEAD * i + HEAD), rows(n, HEAD, HEAD * i)
            cos, sin = turner(table_s, n * (TB // HEAD) + i)
            for h in range(G + 1):
                t = y[here, HEAD * h : HEAD * h + HEAD].astype(F32)
                t = (t * cos + swap(t) * sin).astype(BF)
                if h < G:
                    q_s[h, there, :] = t
                else:
                    k_s[there, :] = t
        v = y[:, (G + 1) * HEAD :]
        v_s[rows(n), :] = v
        vt_s[n] = jnp.concatenate([v.T, jnp.ones((8, TB), BF)], axis=0)

    i, j = block_of(n - NT)
    e = HEAD**-0.5 * LOG2E

    @pl.when((n >= NT) & (j == 0))
    def _():
        top_s[...] = jnp.full(top_s.shape, NEG, F32)
        mix_s[...] = jnp.zeros(mix_s.shape, F32)

    def block(key, keys, query, mask):
        k = k_s[rows(j, keys, key), :]
        scores = [mm_t(k, q_s[h, rows(i, TB - query, query), :]) for h in range(G)]
        weights, keeps = [], []
        for h, s in enumerate(scores):
            if mask:
                s = jnp.where(masked(s, key, query), s, HIDDEN)
            old = top_s[h : h + 1, query:]
            top = jnp.maximum(old, s.max(axis=0, keepdims=True))
            top_s[h : h + 1, query:] = top
            weights.append(jnp.exp2((s - top) * e).astype(BF))
            keeps.append(jnp.exp2((old - top) * e))
        for h in range(G):
            mix_s[h, :, query:] = mix_s[h, :, query:] * keeps[h] + mm(vt_s[j, :, key : key + keys], weights[h])

    @pl.when((n >= NT) & (j < i))
    def _():
        block(0, TB, 0, False)

    @pl.when((n >= NT) & (j == i))
    def _():
        for key, query in HALVES:
            block(key, TB // 2, query, True)
        for h in range(G):
            total = mix_s[h, HEAD : HEAD + 1, :]
            o_s[h, rows(i), :] = (mix_s[h, :HEAD, :] * (1 / total)).T.astype(BF)
            lse_s[h : h + 1, rows(i)] = top_s[h : h + 1, :] * HEAD**-0.5 + jnp.log(total)
        o_out(i).start()

    def finish():
        lse_out.start()
        gr.finish()
        lse_out.wait()
        wait(keep)
        wait([o_out(b) for b in range(NT)])

    stage(n, {NT + BLOCKS - 1: [finish]})


def front(x, table, weights, gq, gr):
    T, D = x.shape
    hbm = pl.BlockSpec(memory_space=pltpu.HBM)
    mine = [(G, T, HEAD), (T, HEAD), (T, HEAD), (D, T), (G, T, HEAD)]
    outs = [jax.ShapeDtypeStruct(s, BF) for s in mine] + [jax.ShapeDtypeStruct((8, T), F32)] + gq.outs() + gr.outs()
    return pl.pallas_call(
        functools.partial(_front, gq=gq, gr=gr),
        grid=(NT + BLOCKS,),
        in_specs=[hbm] * (2 + len(weights)),
        out_specs=[hbm] * len(outs),
        out_shape=outs,
        scratch_shapes=[[pltpu.VMEM(s, BF) for s in (*mine, (T, D))], [pltpu.VMEM(a.shape, BF) for a in weights[:3]], pltpu.VMEM((8, T), F32), pltpu.VMEM(table.shape, F32),
                        pltpu.VMEM((NT, HEAD + 8, TB), BF), pltpu.VMEM((8, TB), F32), pltpu.VMEM((G, HEAD + 8, TB), F32),
                        pltpu.VMEM((X, Y, TALL, 1024), BF), DMA((11,)), DMA((NT,)), gq.scratch(), gr.scratch()],
        compiler_params=pltpu.CompilerParams(dimension_semantics=("arbitrary",), vmem_limit_bytes=VMEM, collective_id=1, has_side_effects=True),
        name="front",
    )(x, table, *weights)


def _back(*refs, sq, sr):
    hbm, then, grads, dx_ref, outs, rest = refs[:5], refs[5:11], refs[11:15], refs[15], refs[16:23], refs[23:]
    ours, more, sems, more_sem, dq_s, dk_s, dv_s, d_s, acc, dw_s, rq, rr = rest
    q_s, do_s, k_s, v_s, at_s = ours
    lse_ref, delta_ref, table_s, w_s, x_s, dh_s = more
    n = pl.program_id(0)
    sq.bind((dw_s,), outs[:3], rq)
    sr.bind(grads, outs[3:], rr)

    def fetch(b):
        at = [(ALL, rows(b)), (ALL, rows(b)), (rows(b),), (rows(b),), (ALL, rows(b))]
        return [pltpu.make_async_copy(src.at[a], dst.at[a], sems.at[m, b]) for m, (src, dst, a) in enumerate(zip(hbm, ours, at))]

    whole_ones = [pltpu.make_async_copy(src, dst, more_sem.at[m]) for m, (src, dst) in enumerate(zip(then, more))]

    def fetch_first():
        start(whole_ones[:3] + fetch(0))

    def fetch_more():
        for b in range(1, NT):
            start(fetch(b))

    def fetch_last():
        start(whole_ones[3:])

    def rest_here():
        wait(whole_ones[3:])

    i, j = block_of(n)
    stage(n, {0: [fetch_first, hello]})

    @pl.when((n < BLOCKS) & (j == 0))
    def _():
        wait(fetch(i))

        @pl.when(n == 0)
        def _():
            wait(whole_ones[:3])
            fetch_more()

    stage(n, {1: [meet, sr.down], 3: [fetch_last, sr.near], 5: [sr.near2], 9: [sr.far]})
    scale = HEAD**-0.5
    e = scale * LOG2E

    @pl.when(n == 0)
    def _():
        dk_s[...] = jnp.zeros_like(dk_s)
        dv_s[...] = jnp.zeros_like(dv_s)
        acc[...] = jnp.zeros_like(acc)

    @pl.when((n < BLOCKS) & (j == 0))
    def _():
        dq_s[...] = jnp.zeros_like(dq_s)

    def block(key, keys, query, mask):
        here, there = rows(j, keys, key), rows(i, TB - query, query)
        k, v = k_s[here, :], v_s[here, :]
        kt = k.T
        qs = [q_s[h, there, :] for h in range(G)]
        dos = [do_s[h, there, :] for h in range(G)]
        scores = [mm_t(k, q) for q in qs]
        dps = [mm_t(v, do) for do in dos]
        for h in range(G):
            p = jnp.exp2(scores[h] * e - lse_ref[h : h + 1, there] * LOG2E)
            if mask:
                p = jnp.where(masked(p, key, query), p, 0.0)
            ds = (p * (dps[h] - delta_ref[h : h + 1, there])).astype(BF)
            dv_s[j, key : key + keys] += mm(p.astype(BF), dos[h])
            dk_s[j, key : key + keys] += mm(ds, qs[h])
            dq_s[h, :, query:] += mm(kt, ds)

    def turn_back(t, b, r):
        cos, sin = turner(table_s, b * (TB // HEAD) + r)
        t = t[HEAD * r : HEAD * r + HEAD].astype(F32)
        return (t * cos - swap(t) * sin).astype(BF)

    @pl.when((n < BLOCKS) & (j < i))
    def _():
        block(0, TB, 0, False)

    @pl.when((n < BLOCKS) & (j == i))
    def _():
        for key, query in HALVES:
            block(key, TB // 2, query, True)

    stage(n, {BLOCKS - 1: [sr.far2]})

    @pl.when((n < BLOCKS) & (j == i))
    def _():
        for h in range(G):
            dq = (dq_s[h] * scale).T.astype(BF)
            for r in range(TB // HEAD):
                d_s[i, HEAD * r : HEAD * r + HEAD, HEAD * h : HEAD * h + HEAD] = turn_back(dq, i, r)
        acc[:, : G * HEAD] += mm(at_s[:, rows(i)], d_s[i, :, : G * HEAD])

    def last():
        for b in range(NT):
            dk = (dk_s[b] * scale).astype(BF)
            for r in range(TB // HEAD):
                d_s[b, HEAD * r : HEAD * r + HEAD, G * HEAD : (G + 1) * HEAD] = turn_back(dk, b, r)
            d_s[b, :, (G + 1) * HEAD :] = dv_s[b].astype(BF)
            acc[:, G * HEAD :] += mm(at_s[:, rows(b)], d_s[b, :, G * HEAD :])
        dw_s[...] = acc[...].astype(BF).reshape(dw_s.shape)

    stage(n, {BLOCKS: [last, sq.down, rest_here, sr.line], BLOCKS + 1: [sq.near], BLOCKS + 2: [sq.near2], BLOCKS + 3: [sq.far]})

    @pl.when(n >= BLOCKS)
    def _():
        da = mm_t(d_s[n - BLOCKS], w_s[...])
        at = rows(n - BLOCKS)
        dx_ref[...] = (dh_s[at, :].astype(F32) + norm_back(x_s[at, :].astype(F32), da)).astype(BF)

    stage(n, {BLOCKS + NT - 1: [sq.line, sr.finish, sq.finish]})


def back(q, k, v, do, lse, delta, at, x, dh, w, table, grads, sq, sr):
    T, D = x.shape
    hbm = pl.BlockSpec(memory_space=pltpu.HBM)
    outs = sq.outs() + sr.outs()
    ins, then = (q, do, k, v, at), (lse, delta, table, w, x, dh)
    return pl.pallas_call(
        functools.partial(_back, sq=sq, sr=sr),
        grid=(BLOCKS + NT,),
        in_specs=[hbm] * (len(ins) + len(then) + len(grads)),
        out_specs=[pl.BlockSpec((TB, D), lambda n: (jnp.maximum(n - BLOCKS, 0), 0))] + [whole(o.shape) for o in outs],
        out_shape=[jax.ShapeDtypeStruct((T, D), BF)] + outs,
        scratch_shapes=[[pltpu.VMEM(a.shape, BF) for a in ins], [pltpu.VMEM(a.shape, a.dtype) for a in then], DMA((len(ins), NT)), DMA((len(then),)),
                        pltpu.VMEM((G, HEAD, TB), F32), pltpu.VMEM((NT, TB, HEAD), F32), pltpu.VMEM((NT, TB, HEAD), F32),
                        pltpu.VMEM((NT, TB, 1024), BF), pltpu.VMEM(w.shape, F32), pltpu.VMEM((X, Y, THIN, LINE, 1024), BF), sq.scratch(), sr.scratch()],
        compiler_params=pltpu.CompilerParams(dimension_semantics=("arbitrary",), vmem_limit_bytes=63 * 2**20, collective_id=2, has_side_effects=True),
        name="back",
    )(*ins, *then, *grads)


def _middle(x_ref, o_ref, wo_ref, dy_hbm, wg_hbm, wu_hbm, wd_hbm, dh_ref, do_ref, delta_ref, dwo_ref, dwg_hbm, dwu_hbm, dwd_hbm,
            h_s, b_s, bt_s, db_s, dy_s, wg_s, wu_s, wd_s, ao, ag, au, ad, tg, tu, td, dy_sem, in_sem, out_sem):
    n = pl.program_id(0)
    m = n - NT
    j, t = m // MT, lax.rem(m, MT)
    is_main = (m >= 0) & (m < MJ * MT)
    dy_in = pltpu.make_async_copy(dy_hbm, dy_s, dy_sem)

    def chunk(j):
        at, to = cols(j * FJ, FJ), lax.rem(j, 2)
        pairs = [(wg_hbm.at[:, at], wg_s), (wu_hbm.at[:, at], wu_s), (wd_hbm.at[at, :], wd_s)]
        return [pltpu.make_async_copy(src, dst.at[to], in_sem.at[i, to]) for i, (src, dst) in enumerate(pairs)]

    def grads(j):
        at = cols(j * FJ, FJ)
        pairs = [(tg, dwg_hbm.at[:, at]), (tu, dwu_hbm.at[:, at]), (td, dwd_hbm.at[at, :])]
        return [pltpu.make_async_copy(src, dst, out_sem.at[i]) for i, (src, dst) in enumerate(pairs)]

    @pl.when(n == 0)
    def _():
        start(chunk(0))
        dy_in.start()

    @pl.when(n < NT)
    def _():
        o = jnp.concatenate([o_ref[h] for h in range(G)], axis=1)
        h = (x_ref[...].astype(F32) + mm(o, wo_ref[...]).astype(BF).astype(F32)).astype(BF)
        h_s[rows(n), :] = h
        b, _ = norm(h.astype(F32))
        b_s[rows(n), :] = b
        bt_s[:, rows(n)] = b.T
        db_s[rows(n), :] = jnp.zeros((TB, db_s.shape[1]), F32)

    @pl.when(m == 0)
    def _():
        dy_in.wait()

    @pl.when(is_main & (t == 0))
    def _():
        wait(chunk(j))
        ag[...] = jnp.zeros_like(ag)
        au[...] = jnp.zeros_like(au)
        ad[...] = jnp.zeros_like(ad)

        @pl.when(j + 1 < MJ)
        def _():
            start(chunk(j + 1))

    @pl.when(is_main)
    def _():
        these, slot = pl.ds(pl.multiple_of(t * MB, MB), MB), lax.rem(j, 2)
        b, bt, dy = b_s[these, :], bt_s[:, these], dy_s[these, :]

        def into(c):
            return mm(b, wg_s[slot, :, c]), mm(b, wu_s[slot, :, c]), mm_t(dy, wd_s[slot, c, :])

        def point(gate, up, dact):
            dact = dact.astype(BF).astype(F32)
            sig = 0.5 + 0.5 * jnp.tanh(0.5 * gate)
            silu = gate * sig
            return (silu * up).astype(BF), (dact * up * (sig + silu * (1 - sig))).astype(BF), (dact * silu).astype(BF)

        strips = [slice(a, a + 256) for a in range(0, FJ, 256)]
        ahead, dbs = into(strips[0]), []
        for i, c in enumerate(strips):
            now, ahead = ahead, into(strips[i + 1]) if i + 1 < len(strips) else ()
            act, dgate, dup = point(*now)
            dbs.append(mm_t(dgate, wg_s[slot, :, c]) + mm_t(dup, wu_s[slot, :, c]))
            ag[:, c] += mm(bt, dgate)
            au[:, c] += mm(bt, dup)
            ad[c, :] += mm(act.T, dy)
        db_s[these, :] += sum(dbs[1:], dbs[0])

        @pl.when(t == MT - 1)
        def _():
            @pl.when(j > 0)
            def _():
                wait(grads(j - 1))

            tg[...] = ag[...].astype(BF)
            tu[...] = au[...].astype(BF)
            td[...] = ad[...].astype(BF)
            start(grads(j))

    last = m - MJ * MT

    @pl.when(last == 0)
    def _():
        ao[...] = jnp.zeros_like(ao)

    @pl.when(last >= 0)
    def _():
        at = rows(jnp.maximum(last, 0))
        dh = (dy_s[at, :].astype(F32) + norm_back(h_s[at, :].astype(F32), db_s[at, :]).astype(BF).astype(F32)).astype(BF)
        dh_ref[...] = dh
        do = mm_t(dh, wo_ref[...]).astype(BF)
        o = jnp.concatenate([o_ref[h] for h in range(G)], axis=1)
        prod = do.astype(F32) * o.astype(F32)
        for h in range(G):
            do_ref[h] = do[:, HEAD * h : HEAD * h + HEAD]
        delta_ref[...] = jnp.concatenate([prod[:, HEAD * h : HEAD * h + HEAD].sum(-1, keepdims=True) for h in range(G)]
                                         + [jnp.zeros((TB, 8 - G), F32)], axis=1).T
        ao[...] += mm(o.T, dh)

    @pl.when(last == NT - 1)
    def _():
        dwo_ref[...] = ao[...].astype(BF)
        wait(grads(MJ - 1))


def middle(x, dy, o, wo, wg, wu, wd):
    T, D = x.shape
    end = NT + MJ * MT
    late = lambda n: jnp.maximum(n - end, 0)
    ends = lambda n: jnp.where(n < NT, n, jnp.where(n < end, NT - 1, n - end))
    once = pl.BlockSpec(wo.shape, lambda n: (0, 0), pipeline_mode=pl.Buffered(1))
    hbm = pl.BlockSpec(memory_space=pltpu.HBM)
    buf = lambda *s, dtype=BF: pltpu.VMEM(s, dtype)
    return pl.pallas_call(
        _middle,
        grid=(end + NT,),
        in_specs=[pl.BlockSpec((TB, D), lambda n: (jnp.minimum(n, NT - 1), 0)), pl.BlockSpec((G, TB, HEAD), lambda n: (0, ends(n), 0)), once,
                  hbm, hbm, hbm, hbm],
        out_specs=[pl.BlockSpec((TB, D), lambda n: (late(n), 0)), pl.BlockSpec((G, TB, HEAD), lambda n: (0, late(n), 0)),
                   pl.BlockSpec((8, TB), lambda n: (0, late(n))), once, hbm, hbm, hbm],
        out_shape=[jax.ShapeDtypeStruct((T, D), BF), jax.ShapeDtypeStruct((G, T, HEAD), BF), jax.ShapeDtypeStruct((8, T), F32),
                   *(jax.ShapeDtypeStruct(a.shape, BF) for a in (wo, wg, wu, wd))],
        scratch_shapes=[buf(T, D), buf(T, D), buf(D, T), buf(T, D, dtype=F32), buf(T, D), buf(2, D, FJ), buf(2, D, FJ), buf(2, FJ, D),
                        buf(D, D, dtype=F32), buf(D, FJ, dtype=F32), buf(D, FJ, dtype=F32), buf(FJ, D, dtype=F32), buf(D, FJ), buf(D, FJ), buf(FJ, D),
                        DMA(()), DMA((3, 2)), DMA((3,))],
        compiler_params=pltpu.CompilerParams(dimension_semantics=("arbitrary",), vmem_limit_bytes=67043328), name="middle",
    )(x, o, wo, dy, wg, wu, wd)


def _hand_over(*refs):
    *ends, bufs, big, sems = refs
    srcs, dsts = ends[: len(bufs)], ends[len(bufs) :]

    def pairs(src, dst, buf, sem):
        return pltpu.make_async_copy(src, buf, sem.at[0]), pltpu.make_async_copy(buf, dst, sem.at[1])

    copies = [pairs(s, d, b, sems.at[m]) for m, (s, d, b) in enumerate(zip(srcs, dsts, bufs))]
    some = [pl.ds(i * MB // NT, MB // NT) for i in range(srcs[0].shape[1] * NT // MB)]
    copies = [pairs(srcs[0].at[:, at], dsts[0].at[:, at], bufs[0].at[:, at], big.at[m]) for m, at in enumerate(some)] + copies[1:]
    start([get for get, _ in copies])
    for get, put in copies:
        get.wait()
        put.start()
    wait([put for _, put in copies])


def hand_over(results):
    hbm, n = pl.BlockSpec(memory_space=pltpu.HBM), len(results)
    return pl.pallas_call(
        _hand_over, in_specs=[hbm] * n, out_specs=[hbm] * n, out_shape=[jax.ShapeDtypeStruct(a.shape, BF) for a in results],
        scratch_shapes=[[pltpu.VMEM(a.shape, BF) for a in results], DMA((NT * NT, 2)), DMA((n, 2))],
        compiler_params=pltpu.CompilerParams(vmem_limit_bytes=VMEM), name="hand_over",
    )(*results)


def solution(mesh):
    gq, gr, sq, sr = Gather(*QKV, in_vmem=True), Gather(*REST), Scatter(*QKV, in_vmem=True), Scatter(*REST)

    def step(x, dy, *weights):
        x, dy = x[0], dy[0]
        T, D = x.shape
        table = turn_table(T)
        q, k, v, at, o, lse, w, *rest = front(x, table, weights, gq, gr)
        rest = [a.reshape(D, -1) for a in rest[:3]] + [rest[3].reshape(-1, D)]
        dh, do, delta, *grads = middle(x, dy, o, *rest)
        grads = [g.reshape(X, Y, -1, LINE, g.shape[1]) for g in grads]
        dx, *by_w = back(q, k, v, do, lse, delta, at, x, dh, w.reshape(D, -1), table, grads, sq, sr)
        return hand_over([dx[None], *by_w])

    states, cut = P(("rep", "dp"), None, None), P(None, "dp", None)
    return jax.shard_map(
        step,
        mesh=mesh,
        in_specs=(states, states) + (cut,) * 7,
        out_specs=(states,) + (P("rep", "dp", None),) * 7,
        check_vma=False,
    )
```

```python
import functools

import jax
import jax.numpy as jnp
import numpy as np
from jax import lax
from jax.experimental import pallas as pl
from jax.experimental.pallas import tpu as pltpu
from jax.sharding import PartitionSpec as P


F32, BF = jnp.float32, jnp.bfloat16
X, Y, Z, C = 4, 4, 8, 2
LINE = Z * C
DMA = pltpu.SemaphoreType.DMA
THIN = 3
TALL = THIN * LINE
WIDTH, HIDDEN_UNITS, HEAD = 768, 2048, 128
ALL = slice(None)
DIRECT = ((2, 2),)
BOTH = ((0, 1), (1, 3))


def place():
    me = lax.axis_index("dp")
    return me // (LINE * Y), lax.rem(me // LINE, Y), lax.rem(me, LINE), lax.rem(me, C)


def device(x, y, slot):
    return {"dp": (x * Y + y) * LINE + slot}


def on(a, k, n=4):
    return lax.rem(a + k, n)


def remote(src, dst, sems, where):
    send, recv = sems
    return pltpu.make_async_remote_copy(src_ref=src, dst_ref=dst, send_sem=send, recv_sem=recv, device_id=where, device_id_type=pl.DeviceIdType.MESH)


def start(copies):
    for cp in copies:
        cp.start()


def settle(ref, sem):
    pltpu.make_async_copy(ref, ref, sem).wait()


def peers():
    x, y, slot, _ = place()
    who = [device(x, y, on(slot, k, LINE)) for k in range(1, LINE)]
    for k in range(1, X):
        who += [device(on(x, k), y, slot), device(x, on(y, k), slot)]
    return who


def hello():
    for d in peers():
        pl.semaphore_signal(pltpu.get_barrier_semaphore(), inc=1, device_id=d, device_id_type=pl.DeviceIdType.MESH)


def meet():
    pl.semaphore_wait(pltpu.get_barrier_semaphore(), len(peers()))


def cols(first, size):
    return pl.ds(pl.multiple_of(first, 128), size)


def pair(sems, n):
    return sems[0].at[n], sems[1].at[n]


SENT, CAME = 0, 1


class Ring:
    def __init__(self, along_x):
        x, y, slot, c = place()
        self.at = x if along_x else y
        self.to = lambda k: device(on(x, k), y, slot) if along_x else device(x, on(y, k), slot)


class Gather:
    STAGES = ("near", "near2", "far", "far2", "over")

    def __init__(self, arrays, pieces, in_vmem=False):
        self.arrays, self.pieces, self.in_vmem, self.direct = arrays, pieces, in_vmem, in_vmem

    def scratch(self):
        A, P = len(self.arrays), len(self.pieces)
        both = lambda *s: [DMA(s), DMA(s)]
        wide = [n if parts else n // 2 for _, n, parts in self.arrays]
        inputs = sum(max(len(a[2]), 1) for a in self.arrays)
        return dict(
            blocks=[pltpu.VMEM((LINE, a[0], w), BF) for a, w in zip(self.arrays, wide)],
            rows=[pltpu.VMEM((TALL, w) if a[0] == THIN else (8, 128), BF) for a, w in zip(self.arrays, wide)],
            tall=pltpu.VMEM((TALL, max(wide)), F32),
            own=DMA((inputs,)), put=DMA((P,)), line=both(A),
            **{name: both(P) for name in self.STAGES},
        )

    def outs(self):
        return [jax.ShapeDtypeStruct((X, Y, TALL, a[1]) if a[0] == THIN else (X, Y, LINE, a[0], a[1]), BF) for a in self.arrays]

    def bind(self, ins, outs, s, own=None):
        self.ins, self.own, self.res, self.s = ins, own or ins, outs, s
        self.spot = place()

    def _parts(self, slot, core, ins):
        out = []
        for i, (r, width, parts) in enumerate(self.arrays):
            half, dst = width // 2, self.s["blocks"][i].at[slot]
            for first, w in parts:
                out.append((len(out), i, ins[len(out)].at[0], dst.at[:, pl.ds(first, w)]))
            if not parts:
                out.append((len(out), i, ins[len(out)].at[0, :, cols(core * half, half)], dst))
        return out

    def _line(self):
        x, y, slot, _ = self.spot

        def each(k, _):
            to = on(slot, k, LINE)
            start([remote(src, dst, pair(self.s["line"], i), device(x, y, to)) for n, i, src, dst in self._parts(slot, lax.rem(to, C), self.ins)])

        lax.fori_loop(1, LINE, each, None)

    def _all_of(self, which):
        for i, b in enumerate(self.s["blocks"]):
            settle(b.at[pl.ds(0, LINE - 1)], self.s["line"][which].at[i])

    def _done(self, stage, which, ps=()):
        x, y, _, c = self.spot
        for p, (i, lo, w, colour) in self._some(ps):
            two, units = pl.ds(0, 2), pl.ds(0, X - 1 if self.direct else 2)
            at = {"near": (x, units) if colour == 0 else (units, y), "near2": (x, y), "far": (two, ALL) if colour == 0 else (ALL, two),
                  "far2": (x, ALL) if colour == 0 else (ALL, y), "over": (ALL, ALL)}[stage]
            settle(self._view(i, lo, w, *at, c), self.s[stage][which].at[p])

    def _own(self):
        _, _, slot, c = self.spot
        return [pltpu.make_async_copy(src, dst, self.s["own"].at[n]) for n, i, src, dst in self._parts(slot, c, self.own)]

    def down(self):
        self._line()
        start(self._own())

    def lay(self):
        for cp in self._own():
            cp.wait()
        self._all_of(CAME)
        tall = self.s["tall"]
        for i, b in enumerate(self.s["blocks"]):
            if self.arrays[i][0] == THIN:
                w = b.shape[2]
                for d in range(LINE):
                    tall[THIN * d : THIN * d + THIN, :w] = b[d].astype(F32)
                self.s["rows"][i][...] = tall[:, :w].astype(BF)

    def _view(self, i, lo, w, xs, ys, core, rows=ALL):
        at = cols(core * (self.arrays[i][1] // 2) + lo, w)
        if rows == slice(LINE, None) and self.arrays[i][0] == THIN:
            rows = pl.ds(LINE, 2 * LINE)
        return self.res[i].at[xs, ys, rows, at] if self.arrays[i][0] == THIN else self.res[i].at[xs, ys, rows, :, at]

    def _half(self, i, k):
        n = LINE if self.arrays[i][0] == THIN else LINE // 2
        return slice(n, None) if k else slice(n)

    def _put(self):
        x, y, _, c = self.spot
        out = []
        for p, (i, lo, w, colour) in enumerate(self.pieces):
            r, n, parts = self.arrays[i]
            at = cols(c * (n // 2) + lo, w) if parts else pl.ds(lo, w)
            src = self.s["rows"][i].at[:, at] if r == THIN else self.s["blocks"][i].at[:, :, at]
            out.append((p, i, lo, w, colour, src))
        return out

    def _near(self, relay):
        x, y, _, c = self.spot
        copies = []
        for p, i, lo, w, colour, src in self._put():
            ring = Ring(colour == 1)
            for n, k in BOTH + DIRECT if self.direct else BOTH:
                if relay:
                    back = (on(x, 4 - k), y) if colour == 1 else (x, on(y, 4 - k))
                    v = self._view(i, lo, w, *back, c, self._half(i, n))
                    copies.append(remote(v, v, pair(self.s["near2"], p), ring.to(k)))
                else:
                    copies.append(remote(src, self._view(i, lo, w, x, y, c), pair(self.s["near"], p), ring.to(k)))
        return copies

    def _own_rows(self):
        x, y, _, c = self.spot
        return [pltpu.make_async_copy(src, self._view(i, lo, w, x, y, c), self.s["put"].at[p]) for p, i, lo, w, colour, src in self._put()]

    def near(self):
        start(self._near(False))
        if self.in_vmem:
            x, y, _, c = self.spot
            for rows, res in zip(self.s["rows"], self.res):
                n = rows.shape[1] // 2
                res[x, y, :, cols(c * n, n)] = rows[:, cols(c * n, n)]
        else:
            start(self._own_rows())

    def near2(self):
        self._done("near", CAME)
        start(self._near(True))

    def _strip(self, i, lo, w, colour, k, core, half=ALL):
        x, y, _, _ = self.spot
        return self._view(i, lo, w, on(x, k), half, core) if colour == 0 else self._view(i, lo, w, half, on(y, k), core)

    def _some(self, ps):
        return [(p, piece) for p, piece in enumerate(self.pieces) if not ps or p in ps]

    def _far(self, relay, ps=()):
        c, copies = self.spot[3], []
        for p, (i, lo, w, colour) in self._some(ps):
            ring = Ring(colour == 0)
            for n, k in BOTH:
                v = self._strip(i, lo, w, colour, 4 - k if relay else 0, c, slice(2 * n, 2 * n + 2) if relay else ALL)
                copies.append(remote(v, v, pair(self.s["far2" if relay else "far"], p), ring.to(k)))
        return copies

    def _over(self, ks, ps=()):
        x, y, slot, c = self.spot
        copies = []
        for k in ks:
            for p, (i, lo, w, colour) in self._some(ps):
                v = self._strip(i, lo, w, colour, k, c)
                copies.append(remote(v, v, pair(self.s["over"], p), device(x, y, slot + 1 - 2 * c)))
        return copies

    def far(self):
        if not self.in_vmem:
            for cp in self._own_rows():
                cp.wait()
        self._done("near" if self.direct else "near2", CAME)
        start(self._far(False))
        start(self._over([0]))

    def far2(self, *ps):
        self._done("far", CAME, ps)
        start(self._far(True, ps))
        start(self._over([1, 3], ps))

    def over(self, *ps):
        self._done("far2", CAME, ps)
        start(self._over([2], ps))

    def finish(self):
        self._done("over", CAME)
        self._all_of(SENT)
        for stage in self.STAGES:
            if not (self.direct and stage == "near2"):
                self._done(stage, SENT)


class Scatter:
    def __init__(self, arrays, pieces, in_vmem=False):
        self.arrays, self.pieces, self.in_vmem = arrays, pieces, in_vmem

    def scratch(self):
        P = len(self.pieces)
        both = lambda *s: [DMA(s), DMA(s)]
        per = lambda *lead: [pltpu.VMEM((*lead, self._m(i), LINE, w), BF) for i, lo, w, _ in self.pieces]
        half = [pltpu.VMEM((2, 2, self._m(i), LINE, w), BF) for i, lo, w, _ in self.pieces]
        return dict(
            own=per(X, Y), other=per(X, Y), h1=half, f1=per(2, 4), t=per(4),
            h2=per(), f2=per(3),
            zs=[pltpu.VMEM((LINE, a[0], a[1] // 2), BF) for a in self.arrays], zr=[pltpu.VMEM((LINE, a[0], a[1] // 2), BF) for a in self.arrays],
            get=DMA((P,)), **{name: both(P) for name in ("over", "a", "a2", "b", "b2")}, line=both(len(self.arrays)),
        )

    def _m(self, i):
        return 3 if self.arrays[i][0] == THIN else LINE // 2

    def _parts(self, i):
        h = self._m(i) // 2
        return pl.ds(0, h), pl.ds(h, self._m(i) - h)

    def outs(self):
        return [jax.ShapeDtypeStruct((1, a[0], w), BF) for a in self.arrays for _, w in a[2] or [(0, a[1])]]

    def bind(self, ins, outs, s):
        self.ins, self.res, self.s = ins, outs, s
        self.spot = place()

    def _each(self):
        return [(p, i, lo, w, colour) for p, (i, lo, w, colour) in enumerate(self.pieces)]

    def _view(self, i, lo, w, core):
        return self.ins[i].at[:, :, :, :, cols(core * (self.arrays[i][1] // 2) + lo, w)]

    def _over(self):
        x, y, slot, c = self.spot
        return [remote(self._view(i, lo, w, 1 - c), self.s["other"][p], pair(self.s["over"], p), device(x, y, slot + 1 - 2 * c))
                for p, i, lo, w, colour in self._each()]

    def _get(self):
        return [pltpu.make_async_copy(self._view(i, lo, w, self.spot[3]), self.s["own"][p], self.s["get"].at[p]) for p, i, lo, w, colour in self._each()]

    def down(self):
        start(self._over())
        if not self.in_vmem:
            start(self._get())

    def _target(self, p, colour, k):
        x, y, _, _ = self.spot
        own = self.s["own"][p]
        return own.at[on(x, k)] if colour == 0 else own.at[:, on(y, k)]

    def _a(self):
        copies = []
        for p, i, lo, w, colour in self._each():
            for n, k in BOTH:
                copies.append(remote(self._target(p, colour, 2).at[pl.ds(2 * n, 2)], self.s["h1"][p].at[n], pair(self.s["a"], p), Ring(colour == 0).to(k)))
        return copies

    def _a2(self):
        return [remote(self._target(p, colour, k), self.s["f1"][p].at[n], pair(self.s["a2"], p), Ring(colour == 0).to(k))
                for p, i, lo, w, colour in self._each() for n, k in BOTH]

    def _of(self, copies, p):
        n = len(copies) // len(self.pieces)
        return copies[n * p : n * p + n]

    def _done(self, stage, which, p):
        ref = self.s[{"over": "other", "a": "h1", "a2": "f1", "b": "h2", "b2": "f2"}[stage]][p]
        settle(ref.at[pl.ds(0, len(self._ways()))] if stage == "b2" else ref, self.s[stage][which].at[p])

    def near(self):
        a = self._a()
        get = None if self.in_vmem else self._get()
        for p, i, lo, w, colour in self._each():
            if get:
                get[p].wait()
            self._done("over", CAME, p)
            own, other = self.s["own"][p], self.s["other"][p]
            mine = self._view(i, lo, w, self.spot[3]) if self.in_vmem else own

            def add(n, _):
                at = n // Y, lax.rem(n, Y)
                own[at] = (mine[at].astype(F32) + other[at].astype(F32)).astype(BF)

            lax.fori_loop(0, X * Y, add, None)
            start(self._of(a, p))

    def near2(self):
        a2 = self._a2()
        for p, i, lo, w, colour in self._each():
            self._done("a", CAME, p)
            for n, k in BOTH:
                to, h = self._target(p, colour, k), self.s["h1"][p]
                for q in range(2):
                    to[2 * n + q] = (to[2 * n + q].astype(F32) + h[n, q].astype(F32)).astype(BF)
            start(self._of(a2, p))

    def _b(self):
        copies = []
        x, y, _, _ = self.spot
        for p, i, lo, w, colour in self._each():
            ring = Ring(colour == 1)
            for (n, k), part in zip(BOTH, self._parts(i)):
                copies.append(remote(self.s["t"][p].at[on(ring.at, 2), part], self.s["h2"][p].at[part], pair(self.s["b"], p), ring.to(k)))
        return copies

    def _b2(self):
        copies = []
        for p, i, lo, w, colour in self._each():
            ring = Ring(colour == 1)
            copies += [remote(self.s["t"][p].at[on(ring.at, k)], self.s["f2"][p].at[n], pair(self.s["b2"], p), ring.to(k)) for n, k in self._ways()]
        return copies

    def _ways(self):
        return BOTH + DIRECT if self.in_vmem else BOTH

    def far(self):
        b = self._b2() if self.in_vmem else self._b()
        for p, i, lo, w, colour in self._each():
            self._done("a2", CAME, p)
            own, f, t = self._target(p, colour, 0), self.s["f1"][p], self.s["t"][p]

            def add(n, _):
                t[n] = (own[n].astype(F32) + f[0, n].astype(F32) + f[1, n].astype(F32)).astype(BF)

            lax.fori_loop(0, 4, add, None)
            start(self._of(b, p))

    def far2(self):
        b2 = self._b2()
        for p, i, lo, w, colour in self._each():
            self._done("b", CAME, p)
            ring, t = Ring(colour == 1), self.s["t"][p]
            for (_, k), part in zip(BOTH, self._parts(i)):
                at = on(ring.at, k), part
                t[at] = (t[at].astype(F32) + self.s["h2"][p][part].astype(F32)).astype(BF)
            start(self._of(b2, p))

    def _line(self):
        x, y, slot, _ = self.spot

        def each(k, _):
            to = on(slot, k, LINE)
            start([remote(zs.at[to], zr.at[slot], pair(self.s["line"], i), device(x, y, to)) for i, (zs, zr) in enumerate(zip(self.s["zs"], self.s["zr"]))])

        lax.fori_loop(1, LINE, each, None)

    def _all_of(self, i, which):
        settle(self.s["zr"][i].at[pl.ds(0, LINE - 1)], self.s["line"][which].at[i])

    def line(self):
        slot = self.spot[2]
        for p, i, lo, w, colour in self._each():
            self._done("b2", CAME, p)
            f = self.s["f2"][p]
            total = self.s["t"][p][Ring(colour == 1).at].astype(F32)
            for n, _ in self._ways():
                total += f[n].astype(F32)
            zs = self.s["zs"][i]
            if self.arrays[i][0] == THIN:
                total = total.reshape(TALL, w)
                for d in range(LINE):
                    zs[d, :, lo : lo + w] = total[THIN * d : THIN * d + THIN].astype(BF)
            else:
                zs[:, :, lo : lo + w] = total.reshape(LINE, -1, w).astype(BF)
        self._line()
        for zs, zr in zip(self.s["zs"], self.s["zr"]):
            zr[slot] = zs[slot]

    def finish(self):
        n = 0
        for i, (r, width, parts) in enumerate(self.arrays):
            zr = self.s["zr"][i]
            self._all_of(i, CAME)
            sums = []
            for core in range(C):
                total = zr[core].astype(F32)
                for k in range(1, Z):
                    total += zr[C * k + core].astype(F32)
                sums.append(total.astype(BF))
            whole = jnp.concatenate(sums, axis=1)
            for first, w in parts or [(0, width)]:
                self.res[n][0] = whole[:, first : first + w]
                n += 1
            self._all_of(i, SENT)
        for stage in ("over", "a", "a2", "b2") if self.in_vmem else ("over", "a", "a2", "b", "b2"):
            for p in range(len(self.pieces)):
                self._done(stage, SENT, p)


QKV = ([(THIN, WIDTH + 2 * HEAD, [(0, WIDTH), (WIDTH, HEAD), (WIDTH + HEAD, HEAD)])], [(0, 0, 256, 0), (0, 256, 256, 1)])
REST = (
    [(THIN, WIDTH, ()), (THIN, HIDDEN_UNITS, ()), (THIN, HIDDEN_UNITS, ()), (8, WIDTH, ())],
    [(1, 0, 1024, 0), (2, 0, 1024, 1), (0, 0, 384, 0), (3, 0, 128, 0), (3, 128, 256, 1)],
)


THETA = 10000
NAMES = ("wq", "wk", "wv", "wo", "w_gate", "w_up", "w_down")
G = 6
TB = 512
NT = 4
MB, MT, FJ, MJ = 1024, 2, 512, 4
BLOCKS = NT * (NT + 1) // 2
NEG = -1e30
HIDDEN = 2 * NEG
LOG2E = 1.4426950408889634
VMEM = 56 * 2**20
EPS = 1e-6


def mm(a, b):
    return lax.dot_general(a, b, (((1,), (0,)), ((), ())), preferred_element_type=F32)


def mm_t(a, b):
    return lax.dot_general(a, b, (((1,), (1,)), ((), ())), preferred_element_type=F32)


def norm(h):
    scale = lax.rsqrt(jnp.mean(h * h, -1, keepdims=True) + EPS)
    return (h * scale).astype(BF), scale


def norm_back(h, g):
    scale = lax.rsqrt(jnp.mean(h * h, -1, keepdims=True) + EPS)
    return scale * (g - h * (scale * scale * jnp.mean(g * h, -1, keepdims=True)))


def turn_table(tokens):
    half = HEAD // 2
    freq = np.float64(THETA) ** (-np.arange(half) / half)
    place = np.concatenate([HEAD * np.arange(tokens // HEAD), np.arange(HEAD)]) * 1.0
    angle = place[:, None] * np.concatenate([freq, freq])
    return jnp.asarray(np.stack([np.cos(angle), np.sin(angle)]).astype(np.float32))


def turner(table, n):
    far, near = pl.ds(n, 1), slice(-HEAD, None)
    fc, fs, nc, ns = table[0, far, :], table[1, far, :], table[0, near, :], table[1, near, :]
    sin = fs * nc + fc * ns
    return fc * nc - fs * ns, jnp.where(lax.broadcasted_iota(jnp.int32, sin.shape, 1) < HEAD // 2, -sin, sin)


def swap(t):
    return pltpu.roll(t, HEAD // 2, 1)


def whole(shape):
    return pl.BlockSpec(shape, lambda *_: (0,) * len(shape))


def stage(n, plan):
    for at, todo in plan.items():

        @pl.when(n == at)
        def _():
            for do in todo:
                do()


def block_of(m):
    i = sum((m >= (r * (r + 1)) // 2).astype(jnp.int32) for r in range(1, NT))
    return i, m - (i * (i + 1)) // 2


def rows(b, size=TB, first=0):
    return pl.ds(pl.multiple_of(b * TB + first, HEAD), size)


def wait(copies):
    for cp in copies:
        cp.wait()


HALVES = ((0, 0), (TB // 2, TB // 2))


def masked(s, key, query):
    return lax.broadcasted_iota(jnp.int32, s.shape, 0) + key <= lax.broadcasted_iota(jnp.int32, s.shape, 1) + query


def _front(x_ref, table_ref, *rest, gq, gr):
    weights, rest = rest[: len(NAMES)], rest[len(NAMES) :]
    hbm, outs, (ours, qkv_s, lse_s, table_s, vt_s, top_s, mix_s, w_s, sems, o_sem, sq, sr) = rest[:6], rest[6:11], rest[11:]
    q_s, k_s, v_s, at_s, o_s, x_s = ours
    n = pl.program_id(0)
    gq.bind(qkv_s, (w_s,), sq, own=weights[:3])
    gr.bind(weights[3:], outs[1:], sr)
    fetch = [pltpu.make_async_copy(a, b, sems.at[len(ours) + m]) for m, (a, b) in enumerate([*zip(weights, qkv_s), (x_ref, x_s), (table_ref, table_s)])]
    lse_out = pltpu.make_async_copy(lse_s, hbm[5], sems.at[5])
    keep = [pltpu.make_async_copy(a, b, sems.at[m]) for m, (a, b) in enumerate(zip((q_s, k_s, v_s, at_s, w_s), (*hbm[:4], outs[0])))]
    o_out = lambda b: pltpu.make_async_copy(o_s.at[:, rows(b)], hbm[4].at[:, rows(b)], o_sem.at[b])

    def normed(first, last):
        for b in range(first, last):
            at = slice(b * TB, b * TB + TB)
            a, _ = norm(x_s[at, :].astype(F32))
            x_s[at, :] = a
            at_s[:, at] = a.T

    def early():
        start(fetch)
        hello()
        wait(fetch)
        normed(0, NT // 2)

    def late():
        normed(NT // 2, NT)

    def keep_all():
        start(keep)

    stage(n, {
        0: [early, meet, gq.down, gr.down, late, gq.lay, gq.near, gq.far, gr.lay, gq.far2, gr.near, gq.over, gq.finish],
        1: [gr.near2],
        NT: [gr.far, keep_all],
        10: [functools.partial(gr.far2, 0, 1)],
        11: [functools.partial(gr.far2, 2, 3, 4)],
        13: [functools.partial(gr.over, 0, 1)],
    })

    @pl.when(n < NT)
    def _():
        a = x_s[rows(n), :]
        y = mm(a, w_s[...].reshape(a.shape[1], -1)).astype(BF)
        for i in range(TB // HEAD):
            here, there = slice(HEAD * i, HEAD * i + HEAD), rows(n, HEAD, HEAD * i)
            cos, sin = turner(table_s, n * (TB // HEAD) + i)
            for h in range(G + 1):
                t = y[here, HEAD * h : HEAD * h + HEAD].astype(F32)
                t = (t * cos + swap(t) * sin).astype(BF)
                if h < G:
                    q_s[h, there, :] = t
                else:
                    k_s[there, :] = t
        v = y[:, (G + 1) * HEAD :]
        v_s[rows(n), :] = v
        vt_s[n] = jnp.concatenate([v.T, jnp.ones((8, TB), BF)], axis=0)

    i, j = block_of(n - NT)
    e = HEAD**-0.5 * LOG2E

    @pl.when((n >= NT) & (j == 0))
    def _():
        top_s[...] = jnp.full(top_s.shape, NEG, F32)
        mix_s[...] = jnp.zeros(mix_s.shape, F32)

    def block(key, keys, query, mask):
        k = k_s[rows(j, keys, key), :]
        scores = [mm_t(k, q_s[h, rows(i, TB - query, query), :]) for h in range(G)]
        weights, keeps = [], []
        for h, s in enumerate(scores):
            if mask:
                s = jnp.where(masked(s, key, query), s, HIDDEN)
            old = top_s[h : h + 1, query:]
            top = jnp.maximum(old, s.max(axis=0, keepdims=True))
            top_s[h : h + 1, query:] = top
            weights.append(jnp.exp2((s - top) * e).astype(BF))
            keeps.append(jnp.exp2((old - top) * e))
        for h in range(G):
            mix_s[h, :, query:] = mix_s[h, :, query:] * keeps[h] + mm(vt_s[j, :, key : key + keys], weights[h])

    @pl.when((n >= NT) & (j < i))
    def _():
        block(0, TB, 0, False)

    @pl.when((n >= NT) & (j == i))
    def _():
        for key, query in HALVES:
            block(key, TB // 2, query, True)
        for h in range(G):
            total = mix_s[h, HEAD : HEAD + 1, :]
            o_s[h, rows(i), :] = (mix_s[h, :HEAD, :] * (1 / total)).T.astype(BF)
            lse_s[h : h + 1, rows(i)] = top_s[h : h + 1, :] * HEAD**-0.5 + jnp.log(total)
        o_out(i).start()

    def finish():
        lse_out.start()
        gr.over(2, 3, 4)
        gr.finish()
        lse_out.wait()
        wait(keep)
        wait([o_out(b) for b in range(NT)])

    stage(n, {NT + BLOCKS - 1: [finish]})


def front(x, table, weights, gq, gr):
    T, D = x.shape
    hbm = pl.BlockSpec(memory_space=pltpu.HBM)
    mine = [(G, T, HEAD), (T, HEAD), (T, HEAD), (D, T), (G, T, HEAD)]
    outs = [jax.ShapeDtypeStruct(s, BF) for s in mine] + [jax.ShapeDtypeStruct((8, T), F32)] + gq.outs() + gr.outs()
    return pl.pallas_call(
        functools.partial(_front, gq=gq, gr=gr),
        grid=(NT + BLOCKS,),
        in_specs=[hbm] * (2 + len(weights)),
        out_specs=[hbm] * len(outs),
        out_shape=outs,
        scratch_shapes=[[pltpu.VMEM(s, BF) for s in (*mine, (T, D))], [pltpu.VMEM(a.shape, BF) for a in weights[:3]], pltpu.VMEM((8, T), F32), pltpu.VMEM(table.shape, F32),
                        pltpu.VMEM((NT, HEAD + 8, TB), BF), pltpu.VMEM((8, TB), F32), pltpu.VMEM((G, HEAD + 8, TB), F32),
                        pltpu.VMEM((X, Y, TALL, 1024), BF), DMA((11,)), DMA((NT,)), gq.scratch(), gr.scratch()],
        compiler_params=pltpu.CompilerParams(dimension_semantics=("arbitrary",), vmem_limit_bytes=VMEM, collective_id=1, has_side_effects=True),
        name="front",
    )(x, table, *weights)


def _back(*refs, sq, sr):
    hbm, then, grads, dx_ref, outs, rest = refs[:5], refs[5:11], refs[11:15], refs[15], refs[16:23], refs[23:]
    ours, more, sems, more_sem, dq_s, dk_s, dv_s, d_s, acc, dw_s, rq, rr = rest
    q_s, do_s, k_s, v_s, at_s = ours
    lse_ref, delta_ref, table_s, w_s, x_s, dh_s = more
    n = pl.program_id(0)
    sq.bind((dw_s,), outs[:3], rq)
    sr.bind(grads, outs[3:], rr)

    def fetch(b):
        at = [(ALL, rows(b)), (ALL, rows(b)), (rows(b),), (rows(b),), (ALL, rows(b))]
        return [pltpu.make_async_copy(src.at[a], dst.at[a], sems.at[m, b]) for m, (src, dst, a) in enumerate(zip(hbm, ours, at))]

    whole_ones = [pltpu.make_async_copy(src, dst, more_sem.at[m]) for m, (src, dst) in enumerate(zip(then, more))]

    def fetch_first():
        start(whole_ones[:3] + fetch(0))

    def fetch_more():
        for b in range(1, NT):
            start(fetch(b))

    def fetch_last():
        start(whole_ones[3:])

    def rest_here():
        wait(whole_ones[3:])

    i, j = block_of(n)
    stage(n, {0: [fetch_first, hello]})

    @pl.when((n < BLOCKS) & (j == 0))
    def _():
        wait(fetch(i))

        @pl.when(n == 0)
        def _():
            wait(whole_ones[:3])
            fetch_more()

    stage(n, {1: [meet, sr.down], 3: [fetch_last, sr.near], 5: [sr.near2], 9: [sr.far]})
    scale = HEAD**-0.5
    e = scale * LOG2E

    @pl.when(n == 0)
    def _():
        dk_s[...] = jnp.zeros_like(dk_s)
        dv_s[...] = jnp.zeros_like(dv_s)
        acc[...] = jnp.zeros_like(acc)

    @pl.when((n < BLOCKS) & (j == 0))
    def _():
        dq_s[...] = jnp.zeros_like(dq_s)

    def block(key, keys, query, mask):
        here, there = rows(j, keys, key), rows(i, TB - query, query)
        k, v = k_s[here, :], v_s[here, :]
        kt = k.T
        qs = [q_s[h, there, :] for h in range(G)]
        dos = [do_s[h, there, :] for h in range(G)]
        scores = [mm_t(k, q) for q in qs]
        dps = [mm_t(v, do) for do in dos]
        for h in range(G):
            p = jnp.exp2(scores[h] * e - lse_ref[h : h + 1, there] * LOG2E)
            if mask:
                p = jnp.where(masked(p, key, query), p, 0.0)
            ds = (p * (dps[h] - delta_ref[h : h + 1, there])).astype(BF)
            dv_s[j, key : key + keys] += mm(p.astype(BF), dos[h])
            dk_s[j, key : key + keys] += mm(ds, qs[h])
            dq_s[h, :, query:] += mm(kt, ds)

    def turn_back(t, b, r):
        cos, sin = turner(table_s, b * (TB // HEAD) + r)
        t = t[HEAD * r : HEAD * r + HEAD].astype(F32)
        return (t * cos - swap(t) * sin).astype(BF)

    @pl.when((n < BLOCKS) & (j < i))
    def _():
        block(0, TB, 0, False)

    @pl.when((n < BLOCKS) & (j == i))
    def _():
        for key, query in HALVES:
            block(key, TB // 2, query, True)

    stage(n, {BLOCKS - 1: [sr.far2]})

    @pl.when((n < BLOCKS) & (j == i))
    def _():
        for h in range(G):
            dq = (dq_s[h] * scale).T.astype(BF)
            for r in range(TB // HEAD):
                d_s[i, HEAD * r : HEAD * r + HEAD, HEAD * h : HEAD * h + HEAD] = turn_back(dq, i, r)
        acc[:, : G * HEAD] += mm(at_s[:, rows(i)], d_s[i, :, : G * HEAD])

    def last():
        for b in range(NT):
            dk = (dk_s[b] * scale).astype(BF)
            for r in range(TB // HEAD):
                d_s[b, HEAD * r : HEAD * r + HEAD, G * HEAD : (G + 1) * HEAD] = turn_back(dk, b, r)
            d_s[b, :, (G + 1) * HEAD :] = dv_s[b].astype(BF)
            acc[:, G * HEAD :] += mm(at_s[:, rows(b)], d_s[b, :, G * HEAD :])
        dw_s[...] = acc[...].astype(BF).reshape(dw_s.shape)

    stage(n, {BLOCKS: [last, sq.down, rest_here, sr.line], BLOCKS + 1: [sq.near], BLOCKS + 2: [sq.near2], BLOCKS + 3: [sq.far]})

    @pl.when(n >= BLOCKS)
    def _():
        da = mm_t(d_s[n - BLOCKS], w_s[...])
        at = rows(n - BLOCKS)
        dx_ref[...] = (dh_s[at, :].astype(F32) + norm_back(x_s[at, :].astype(F32), da)).astype(BF)

    stage(n, {BLOCKS + NT - 1: [sq.line, sr.finish, sq.finish]})


def back(q, k, v, do, lse, delta, at, x, dh, w, table, grads, sq, sr):
    T, D = x.shape
    hbm = pl.BlockSpec(memory_space=pltpu.HBM)
    outs = sq.outs() + sr.outs()
    ins, then = (q, do, k, v, at), (lse, delta, table, w, x, dh)
    return pl.pallas_call(
        functools.partial(_back, sq=sq, sr=sr),
        grid=(BLOCKS + NT,),
        in_specs=[hbm] * (len(ins) + len(then) + len(grads)),
        out_specs=[pl.BlockSpec((TB, D), lambda n: (jnp.maximum(n - BLOCKS, 0), 0))] + [whole(o.shape) for o in outs],
        out_shape=[jax.ShapeDtypeStruct((T, D), BF)] + outs,
        scratch_shapes=[[pltpu.VMEM(a.shape, BF) for a in ins], [pltpu.VMEM(a.shape, a.dtype) for a in then], DMA((len(ins), NT)), DMA((len(then),)),
                        pltpu.VMEM((G, HEAD, TB), F32), pltpu.VMEM((NT, TB, HEAD), F32), pltpu.VMEM((NT, TB, HEAD), F32),
                        pltpu.VMEM((NT, TB, 1024), BF), pltpu.VMEM(w.shape, F32), pltpu.VMEM((X, Y, THIN, LINE, 1024), BF), sq.scratch(), sr.scratch()],
        compiler_params=pltpu.CompilerParams(dimension_semantics=("arbitrary",), vmem_limit_bytes=63 * 2**20, collective_id=2, has_side_effects=True),
        name="back",
    )(*ins, *then, *grads)


def _middle(x_ref, o_ref, wo_ref, dy_hbm, wg_hbm, wu_hbm, wd_hbm, dh_ref, do_ref, delta_ref, dwo_ref, dwg_hbm, dwu_hbm, dwd_hbm,
            h_s, b_s, bt_s, db_s, dy_s, wg_s, wu_s, wd_s, ao, ag, au, ad, tg, tu, td, dy_sem, in_sem, out_sem):
    n = pl.program_id(0)
    m = n - NT
    j, t = m // MT, lax.rem(m, MT)
    is_main = (m >= 0) & (m < MJ * MT)
    dy_in = pltpu.make_async_copy(dy_hbm, dy_s, dy_sem)

    def chunk(j):
        at, to = cols(j * FJ, FJ), lax.rem(j, 2)
        pairs = [(wg_hbm.at[:, at], wg_s), (wu_hbm.at[:, at], wu_s), (wd_hbm.at[at, :], wd_s)]
        return [pltpu.make_async_copy(src, dst.at[to], in_sem.at[i, to]) for i, (src, dst) in enumerate(pairs)]

    def grads(j):
        at = cols(j * FJ, FJ)
        pairs = [(tg, dwg_hbm.at[:, at]), (tu, dwu_hbm.at[:, at]), (td, dwd_hbm.at[at, :])]
        return [pltpu.make_async_copy(src, dst, out_sem.at[i]) for i, (src, dst) in enumerate(pairs)]

    @pl.when(n == 0)
    def _():
        start(chunk(0))
        dy_in.start()

    @pl.when(n < NT)
    def _():
        o = jnp.concatenate([o_ref[h] for h in range(G)], axis=1)
        h = (x_ref[...].astype(F32) + mm(o, wo_ref[...]).astype(BF).astype(F32)).astype(BF)
        h_s[rows(n), :] = h
        b, _ = norm(h.astype(F32))
        b_s[rows(n), :] = b
        bt_s[:, rows(n)] = b.T
        db_s[rows(n), :] = jnp.zeros((TB, db_s.shape[1]), F32)

    @pl.when(m == 0)
    def _():
        dy_in.wait()

    @pl.when(is_main & (t == 0))
    def _():
        wait(chunk(j))
        ag[...] = jnp.zeros_like(ag)
        au[...] = jnp.zeros_like(au)
        ad[...] = jnp.zeros_like(ad)

        @pl.when(j + 1 < MJ)
        def _():
            start(chunk(j + 1))

    @pl.when(is_main)
    def _():
        these, slot = pl.ds(pl.multiple_of(t * MB, MB), MB), lax.rem(j, 2)
        b, bt, dy = b_s[these, :], bt_s[:, these], dy_s[these, :]

        def into(c):
            return mm(b, wg_s[slot, :, c]), mm(b, wu_s[slot, :, c]), mm_t(dy, wd_s[slot, c, :])

        def point(gate, up, dact):
            dact = dact.astype(BF).astype(F32)
            sig = 0.5 + 0.5 * jnp.tanh(0.5 * gate)
            silu = gate * sig
            return (silu * up).astype(BF), (dact * up * (sig + silu * (1 - sig))).astype(BF), (dact * silu).astype(BF)

        strips = [slice(a, a + 256) for a in range(0, FJ, 256)]
        ahead, dbs = into(strips[0]), []
        for i, c in enumerate(strips):
            now, ahead = ahead, into(strips[i + 1]) if i + 1 < len(strips) else ()
            act, dgate, dup = point(*now)
            dbs.append(mm_t(dgate, wg_s[slot, :, c]) + mm_t(dup, wu_s[slot, :, c]))
            ag[:, c] += mm(bt, dgate)
            au[:, c] += mm(bt, dup)
            ad[c, :] += mm(act.T, dy)
        db_s[these, :] += sum(dbs[1:], dbs[0])

        @pl.when(t == MT - 1)
        def _():
            @pl.when(j > 0)
            def _():
                wait(grads(j - 1))

            tg[...] = ag[...].astype(BF)
            tu[...] = au[...].astype(BF)
            td[...] = ad[...].astype(BF)
            start(grads(j))

    last = m - MJ * MT

    @pl.when(last == 0)
    def _():
        ao[...] = jnp.zeros_like(ao)

    @pl.when(last >= 0)
    def _():
        at = rows(jnp.maximum(last, 0))
        dh = (dy_s[at, :].astype(F32) + norm_back(h_s[at, :].astype(F32), db_s[at, :]).astype(BF).astype(F32)).astype(BF)
        dh_ref[...] = dh
        do = mm_t(dh, wo_ref[...]).astype(BF)
        o = jnp.concatenate([o_ref[h] for h in range(G)], axis=1)
        prod = do.astype(F32) * o.astype(F32)
        for h in range(G):
            do_ref[h] = do[:, HEAD * h : HEAD * h + HEAD]
        delta_ref[...] = jnp.concatenate([prod[:, HEAD * h : HEAD * h + HEAD].sum(-1, keepdims=True) for h in range(G)]
                                         + [jnp.zeros((TB, 8 - G), F32)], axis=1).T
        ao[...] += mm(o.T, dh)

    @pl.when(last == NT - 1)
    def _():
        dwo_ref[...] = ao[...].astype(BF)
        wait(grads(MJ - 1))


def middle(x, dy, o, wo, wg, wu, wd):
    T, D = x.shape
    end = NT + MJ * MT
    late = lambda n: jnp.maximum(n - end, 0)
    ends = lambda n: jnp.where(n < NT, n, jnp.where(n < end, NT - 1, n - end))
    once = pl.BlockSpec(wo.shape, lambda n: (0, 0), pipeline_mode=pl.Buffered(1))
    hbm = pl.BlockSpec(memory_space=pltpu.HBM)
    buf = lambda *s, dtype=BF: pltpu.VMEM(s, dtype)
    return pl.pallas_call(
        _middle,
        grid=(end + NT,),
        in_specs=[pl.BlockSpec((TB, D), lambda n: (jnp.minimum(n, NT - 1), 0)), pl.BlockSpec((G, TB, HEAD), lambda n: (0, ends(n), 0)), once,
                  hbm, hbm, hbm, hbm],
        out_specs=[pl.BlockSpec((TB, D), lambda n: (late(n), 0)), pl.BlockSpec((G, TB, HEAD), lambda n: (0, late(n), 0)),
                   pl.BlockSpec((8, TB), lambda n: (0, late(n))), once, hbm, hbm, hbm],
        out_shape=[jax.ShapeDtypeStruct((T, D), BF), jax.ShapeDtypeStruct((G, T, HEAD), BF), jax.ShapeDtypeStruct((8, T), F32),
                   *(jax.ShapeDtypeStruct(a.shape, BF) for a in (wo, wg, wu, wd))],
        scratch_shapes=[buf(T, D), buf(T, D), buf(D, T), buf(T, D, dtype=F32), buf(T, D), buf(2, D, FJ), buf(2, D, FJ), buf(2, FJ, D),
                        buf(D, D, dtype=F32), buf(D, FJ, dtype=F32), buf(D, FJ, dtype=F32), buf(FJ, D, dtype=F32), buf(D, FJ), buf(D, FJ), buf(FJ, D),
                        DMA(()), DMA((3, 2)), DMA((3,))],
        compiler_params=pltpu.CompilerParams(dimension_semantics=("arbitrary",), vmem_limit_bytes=67043328), name="middle",
    )(x, o, wo, dy, wg, wu, wd)


def _hand_over(*refs):
    *ends, bufs, big, sems = refs
    srcs, dsts = ends[: len(bufs)], ends[len(bufs) :]

    def pairs(src, dst, buf, sem):
        return pltpu.make_async_copy(src, buf, sem.at[0]), pltpu.make_async_copy(buf, dst, sem.at[1])

    copies = [pairs(s, d, b, sems.at[m]) for m, (s, d, b) in enumerate(zip(srcs, dsts, bufs))]
    some = [pl.ds(i * MB // NT, MB // NT) for i in range(srcs[0].shape[1] * NT // MB)]
    copies = [pairs(srcs[0].at[:, at], dsts[0].at[:, at], bufs[0].at[:, at], big.at[m]) for m, at in enumerate(some)] + copies[1:]
    start([get for get, _ in copies])
    for get, put in copies:
        get.wait()
        put.start()
    wait([put for _, put in copies])


def hand_over(results):
    hbm, n = pl.BlockSpec(memory_space=pltpu.HBM), len(results)
    return pl.pallas_call(
        _hand_over, in_specs=[hbm] * n, out_specs=[hbm] * n, out_shape=[jax.ShapeDtypeStruct(a.shape, BF) for a in results],
        scratch_shapes=[[pltpu.VMEM(a.shape, BF) for a in results], DMA((NT * NT, 2)), DMA((n, 2))],
        compiler_params=pltpu.CompilerParams(vmem_limit_bytes=VMEM), name="hand_over",
    )(*results)


def solution(mesh):
    gq, gr, sq, sr = Gather(*QKV, in_vmem=True), Gather(*REST), Scatter(*QKV, in_vmem=True), Scatter(*REST)

    def step(x, dy, *weights):
        x, dy = x[0], dy[0]
        T, D = x.shape
        table = turn_table(T)
        q, k, v, at, o, lse, w, *rest = front(x, table, weights, gq, gr)
        rest = [a.reshape(D, -1) for a in rest[:3]] + [rest[3].reshape(-1, D)]
        dh, do, delta, *grads = middle(x, dy, o, *rest)
        grads = [g.reshape(X, Y, -1, LINE, g.shape[1]) for g in grads]
        dx, *by_w = back(q, k, v, do, lse, delta, at, x, dh, w.reshape(D, -1), table, grads, sq, sr)
        return hand_over([dx[None], *by_w])

    states, cut = P(("rep", "dp"), None, None), P(None, "dp", None)
    return jax.shard_map(
        step,
        mesh=mesh,
        in_specs=(states, states) + (cut,) * 7,
        out_specs=(states,) + (P("rep", "dp", None),) * 7,
        check_vma=False,
    )
```

```python
import functools

import jax
import jax.numpy as jnp
import numpy as np
from jax import lax
from jax.experimental import pallas as pl
from jax.experimental.pallas import tpu as pltpu
from jax.sharding import PartitionSpec as P


F32, BF = jnp.float32, jnp.bfloat16
X, Y, Z, C = 4, 4, 8, 2
LINE = Z * C
DMA = pltpu.SemaphoreType.DMA
THIN = 3
TALL = THIN * LINE
WIDTH, HIDDEN_UNITS, HEAD = 768, 2048, 128
ALL = slice(None)
DIRECT = ((2, 2),)
BOTH = ((0, 1), (1, 3))


def place():
    me = lax.axis_index("dp")
    return me // (LINE * Y), lax.rem(me // LINE, Y), lax.rem(me, LINE), lax.rem(me, C)


def device(x, y, slot):
    return {"dp": (x * Y + y) * LINE + slot}


def on(a, k, n=4):
    return lax.rem(a + k, n)


def remote(src, dst, sems, where):
    send, recv = sems
    return pltpu.make_async_remote_copy(src_ref=src, dst_ref=dst, send_sem=send, recv_sem=recv, device_id=where, device_id_type=pl.DeviceIdType.MESH)


def start(copies):
    for cp in copies:
        cp.start()


def settle(ref, sem):
    pltpu.make_async_copy(ref, ref, sem).wait()


def peers():
    x, y, slot, _ = place()
    who = [device(x, y, on(slot, k, LINE)) for k in range(1, LINE)]
    for k in range(1, X):
        who += [device(on(x, k), y, slot), device(x, on(y, k), slot)]
    return who


def hello():
    for d in peers():
        pl.semaphore_signal(pltpu.get_barrier_semaphore(), inc=1, device_id=d, device_id_type=pl.DeviceIdType.MESH)


def meet():
    pl.semaphore_wait(pltpu.get_barrier_semaphore(), len(peers()))


def cols(first, size):
    return pl.ds(pl.multiple_of(first, 128), size)


def pair(sems, n):
    return sems[0].at[n], sems[1].at[n]


SENT, CAME = 0, 1


class Ring:
    def __init__(self, along_x):
        x, y, slot, c = place()
        self.at = x if along_x else y
        self.to = lambda k: device(on(x, k), y, slot) if along_x else device(x, on(y, k), slot)


class Gather:
    STAGES = ("near", "near2", "far", "far2", "over")

    def __init__(self, arrays, pieces, in_vmem=False):
        self.arrays, self.pieces, self.in_vmem, self.direct = arrays, pieces, in_vmem, in_vmem

    def scratch(self):
        A, P = len(self.arrays), len(self.pieces)
        both = lambda *s: [DMA(s), DMA(s)]
        wide = [n if parts else n // 2 for _, n, parts in self.arrays]
        inputs = sum(max(len(a[2]), 1) for a in self.arrays)
        return dict(
            blocks=[pltpu.VMEM((LINE, a[0], w), BF) for a, w in zip(self.arrays, wide)],
            rows=[pltpu.VMEM((TALL, w) if a[0] == THIN else (8, 128), BF) for a, w in zip(self.arrays, wide)],
            tall=pltpu.VMEM((TALL, max(wide)), F32),
            own=DMA((inputs,)), put=DMA((P,)), line=both(A),
            **{name: both(P) for name in self.STAGES},
        )

    def outs(self):
        return [jax.ShapeDtypeStruct((X, Y, TALL, a[1]) if a[0] == THIN else (X, Y, LINE, a[0], a[1]), BF) for a in self.arrays]

    def bind(self, ins, outs, s, own=None):
        self.ins, self.own, self.res, self.s = ins, own or ins, outs, s
        self.spot = place()

    def _parts(self, slot, core, ins):
        out = []
        for i, (r, width, parts) in enumerate(self.arrays):
            half, dst = width // 2, self.s["blocks"][i].at[slot]
            for first, w in parts:
                out.append((len(out), i, ins[len(out)].at[0], dst.at[:, pl.ds(first, w)]))
            if not parts:
                out.append((len(out), i, ins[len(out)].at[0, :, cols(core * half, half)], dst))
        return out

    def _line(self):
        x, y, slot, _ = self.spot

        def each(k, _):
            to = on(slot, k, LINE)
            start([remote(src, dst, pair(self.s["line"], i), device(x, y, to)) for n, i, src, dst in self._parts(slot, lax.rem(to, C), self.ins)])

        lax.fori_loop(1, LINE, each, None)

    def _all_of(self, which):
        for i, b in enumerate(self.s["blocks"]):
            settle(b.at[pl.ds(0, LINE - 1)], self.s["line"][which].at[i])

    def _done(self, stage, which, ps=()):
        x, y, _, c = self.spot
        for p, (i, lo, w, colour) in self._some(ps):
            two, units = pl.ds(0, 2), pl.ds(0, X - 1 if self.direct else 2)
            at = {"near": (x, units) if colour == 0 else (units, y), "near2": (x, y), "far": (two, ALL) if colour == 0 else (ALL, two),
                  "far2": (x, ALL) if colour == 0 else (ALL, y), "over": (ALL, ALL)}[stage]
            settle(self._view(i, lo, w, *at, c), self.s[stage][which].at[p])

    def _own(self):
        _, _, slot, c = self.spot
        return [pltpu.make_async_copy(src, dst, self.s["own"].at[n]) for n, i, src, dst in self._parts(slot, c, self.own)]

    def down(self):
        self._line()
        start(self._own())

    def lay(self):
        for cp in self._own():
            cp.wait()
        self._all_of(CAME)
        tall = self.s["tall"]
        for i, b in enumerate(self.s["blocks"]):
            if self.arrays[i][0] == THIN:
                w = b.shape[2]
                for d in range(LINE):
                    tall[THIN * d : THIN * d + THIN, :w] = b[d].astype(F32)
                self.s["rows"][i][...] = tall[:, :w].astype(BF)

    def _view(self, i, lo, w, xs, ys, core, rows=ALL):
        at = cols(core * (self.arrays[i][1] // 2) + lo, w)
        if rows == slice(LINE, None) and self.arrays[i][0] == THIN:
            rows = pl.ds(LINE, 2 * LINE)
        return self.res[i].at[xs, ys, rows, at] if self.arrays[i][0] == THIN else self.res[i].at[xs, ys, rows, :, at]

    def _half(self, i, k):
        n = LINE if self.arrays[i][0] == THIN else LINE // 2
        return slice(n, None) if k else slice(n)

    def _put(self):
        x, y, _, c = self.spot
        out = []
        for p, (i, lo, w, colour) in enumerate(self.pieces):
            r, n, parts = self.arrays[i]
            at = cols(c * (n // 2) + lo, w) if parts else pl.ds(lo, w)
            src = self.s["rows"][i].at[:, at] if r == THIN else self.s["blocks"][i].at[:, :, at]
            out.append((p, i, lo, w, colour, src))
        return out

    def _near(self, relay):
        x, y, _, c = self.spot
        copies = []
        for p, i, lo, w, colour, src in self._put():
            ring = Ring(colour == 1)
            for n, k in BOTH + DIRECT if self.direct else BOTH:
                if relay:
                    back = (on(x, 4 - k), y) if colour == 1 else (x, on(y, 4 - k))
                    v = self._view(i, lo, w, *back, c, self._half(i, n))
                    copies.append(remote(v, v, pair(self.s["near2"], p), ring.to(k)))
                else:
                    copies.append(remote(src, self._view(i, lo, w, x, y, c), pair(self.s["near"], p), ring.to(k)))
        return copies

    def _own_rows(self):
        x, y, _, c = self.spot
        return [pltpu.make_async_copy(src, self._view(i, lo, w, x, y, c), self.s["put"].at[p]) for p, i, lo, w, colour, src in self._put()]

    def near(self):
        start(self._near(False))
        if self.in_vmem:
            x, y, _, c = self.spot
            for rows, res in zip(self.s["rows"], self.res):
                n = rows.shape[1] // 2
                res[x, y, :, cols(c * n, n)] = rows[:, cols(c * n, n)]
        else:
            start(self._own_rows())

    def near2(self):
        self._done("near", CAME)
        start(self._near(True))

    def _strip(self, i, lo, w, colour, k, core, half=ALL):
        x, y, _, _ = self.spot
        return self._view(i, lo, w, on(x, k), half, core) if colour == 0 else self._view(i, lo, w, half, on(y, k), core)

    def _some(self, ps):
        return [(p, piece) for p, piece in enumerate(self.pieces) if not ps or p in ps]

    def _far(self, relay, ps=()):
        c, copies = self.spot[3], []
        for p, (i, lo, w, colour) in self._some(ps):
            ring = Ring(colour == 0)
            for n, k in BOTH:
                v = self._strip(i, lo, w, colour, 4 - k if relay else 0, c, slice(2 * n, 2 * n + 2) if relay else ALL)
                copies.append(remote(v, v, pair(self.s["far2" if relay else "far"], p), ring.to(k)))
        return copies

    def _over(self, ks, ps=()):
        x, y, slot, c = self.spot
        copies = []
        for k in ks:
            for p, (i, lo, w, colour) in self._some(ps):
                v = self._strip(i, lo, w, colour, k, c)
                copies.append(remote(v, v, pair(self.s["over"], p), device(x, y, slot + 1 - 2 * c)))
        return copies

    def far(self):
        if not self.in_vmem:
            for cp in self._own_rows():
                cp.wait()
        self._done("near" if self.direct else "near2", CAME)
        start(self._far(False))
        start(self._over([0]))

    def far2(self, *ps):
        self._done("far", CAME, ps)
        start(self._far(True, ps))
        start(self._over([1, 3], ps))

    def over(self, *ps):
        self._done("far2", CAME, ps)
        start(self._over([2], ps))

    def finish(self):
        self._done("over", CAME)
        self._all_of(SENT)
        for stage in self.STAGES:
            if not (self.direct and stage == "near2"):
                self._done(stage, SENT)


class Scatter:
    def __init__(self, arrays, pieces, in_vmem=False):
        self.arrays, self.pieces, self.in_vmem = arrays, pieces, in_vmem

    def scratch(self):
        P = len(self.pieces)
        both = lambda *s: [DMA(s), DMA(s)]
        per = lambda *lead: [pltpu.VMEM((*lead, self._m(i), LINE, w), BF) for i, lo, w, _ in self.pieces]
        half = [pltpu.VMEM((2, 2, self._m(i), LINE, w), BF) for i, lo, w, _ in self.pieces]
        return dict(
            own=per(X, Y), other=per(X, Y), h1=half, f1=per(2, 4), t=per(4),
            h2=per(), f2=per(3),
            zs=[pltpu.VMEM((LINE, a[0], a[1] // 2), BF) for a in self.arrays], zr=[pltpu.VMEM((LINE, a[0], a[1] // 2), BF) for a in self.arrays],
            get=DMA((P,)), **{name: both(P) for name in ("over", "a", "a2", "b", "b2")}, line=both(len(self.arrays)),
        )

    def _m(self, i):
        return 3 if self.arrays[i][0] == THIN else LINE // 2

    def _parts(self, i):
        h = self._m(i) // 2
        return pl.ds(0, h), pl.ds(h, self._m(i) - h)

    def outs(self):
        return [jax.ShapeDtypeStruct((1, a[0], w), BF) for a in self.arrays for _, w in a[2] or [(0, a[1])]]

    def bind(self, ins, outs, s):
        self.ins, self.res, self.s = ins, outs, s
        self.spot = place()

    def _each(self, ps=()):
        return [(p, i, lo, w, colour) for p, (i, lo, w, colour) in enumerate(self.pieces) if not ps or p in ps]

    def _view(self, i, lo, w, core):
        return self.ins[i].at[:, :, :, :, cols(core * (self.arrays[i][1] // 2) + lo, w)]

    def _over(self):
        x, y, slot, c = self.spot
        return [remote(self._view(i, lo, w, 1 - c), self.s["other"][p], pair(self.s["over"], p), device(x, y, slot + 1 - 2 * c))
                for p, i, lo, w, colour in self._each()]

    def _get(self):
        return [pltpu.make_async_copy(self._view(i, lo, w, self.spot[3]), self.s["own"][p], self.s["get"].at[p]) for p, i, lo, w, colour in self._each()]

    def down(self):
        start(self._over())
        if not self.in_vmem:
            start(self._get())

    def _target(self, p, colour, k):
        x, y, _, _ = self.spot
        own = self.s["own"][p]
        return own.at[on(x, k)] if colour == 0 else own.at[:, on(y, k)]

    def _a(self):
        copies = []
        for p, i, lo, w, colour in self._each():
            for n, k in BOTH:
                copies.append(remote(self._target(p, colour, 2).at[pl.ds(2 * n, 2)], self.s["h1"][p].at[n], pair(self.s["a"], p), Ring(colour == 0).to(k)))
        return copies

    def _a2(self):
        return [remote(self._target(p, colour, k), self.s["f1"][p].at[n], pair(self.s["a2"], p), Ring(colour == 0).to(k))
                for p, i, lo, w, colour in self._each() for n, k in BOTH]

    def _of(self, copies, p):
        n = len(copies) // len(self.pieces)
        return copies[n * p : n * p + n]

    def _done(self, stage, which, p):
        ref = self.s[{"over": "other", "a": "h1", "a2": "f1", "b": "h2", "b2": "f2"}[stage]][p]
        settle(ref.at[pl.ds(0, len(self._ways()))] if stage == "b2" else ref, self.s[stage][which].at[p])

    def near(self):
        a = self._a()
        get = None if self.in_vmem else self._get()
        for p, i, lo, w, colour in self._each():
            if get:
                get[p].wait()
            self._done("over", CAME, p)
            own, other = self.s["own"][p], self.s["other"][p]
            mine = self._view(i, lo, w, self.spot[3]) if self.in_vmem else own

            def add(n, _):
                at = n // Y, lax.rem(n, Y)
                own[at] = (mine[at].astype(F32) + other[at].astype(F32)).astype(BF)

            lax.fori_loop(0, X * Y, add, None)
            start(self._of(a, p))

    def near2(self):
        a2 = self._a2()
        for p, i, lo, w, colour in self._each():
            self._done("a", CAME, p)
            for n, k in BOTH:
                to, h = self._target(p, colour, k), self.s["h1"][p]
                for q in range(2):
                    to[2 * n + q] = (to[2 * n + q].astype(F32) + h[n, q].astype(F32)).astype(BF)
            start(self._of(a2, p))

    def _b(self):
        copies = []
        x, y, _, _ = self.spot
        for p, i, lo, w, colour in self._each():
            ring = Ring(colour == 1)
            for (n, k), part in zip(BOTH, self._parts(i)):
                copies.append(remote(self.s["t"][p].at[on(ring.at, 2), part], self.s["h2"][p].at[part], pair(self.s["b"], p), ring.to(k)))
        return copies

    def _b2(self):
        copies = []
        for p, i, lo, w, colour in self._each():
            ring = Ring(colour == 1)
            copies += [remote(self.s["t"][p].at[on(ring.at, k)], self.s["f2"][p].at[n], pair(self.s["b2"], p), ring.to(k)) for n, k in self._ways()]
        return copies

    def _ways(self):
        return BOTH + DIRECT if self.in_vmem else BOTH

    def far(self, *ps):
        b = self._b2() if self.in_vmem else self._b()
        for p, i, lo, w, colour in self._each(ps):
            self._done("a2", CAME, p)
            own, f, t = self._target(p, colour, 0), self.s["f1"][p], self.s["t"][p]

            def add(n, _):
                t[n] = (own[n].astype(F32) + f[0, n].astype(F32) + f[1, n].astype(F32)).astype(BF)

            lax.fori_loop(0, 4, add, None)
            start(self._of(b, p))

    def far2(self, *ps):
        b2 = self._b2()
        for p, i, lo, w, colour in self._each(ps):
            self._done("b", CAME, p)
            ring, t = Ring(colour == 1), self.s["t"][p]
            for (_, k), part in zip(BOTH, self._parts(i)):
                at = on(ring.at, k), part
                t[at] = (t[at].astype(F32) + self.s["h2"][p][part].astype(F32)).astype(BF)
            start(self._of(b2, p))

    def _line(self):
        x, y, slot, _ = self.spot

        def each(k, _):
            to = on(slot, k, LINE)
            start([remote(zs.at[to], zr.at[slot], pair(self.s["line"], i), device(x, y, to)) for i, (zs, zr) in enumerate(zip(self.s["zs"], self.s["zr"]))])

        lax.fori_loop(1, LINE, each, None)

    def _all_of(self, i, which):
        settle(self.s["zr"][i].at[pl.ds(0, LINE - 1)], self.s["line"][which].at[i])

    def line(self):
        slot = self.spot[2]
        for p, i, lo, w, colour in self._each():
            self._done("b2", CAME, p)
            f = self.s["f2"][p]
            total = self.s["t"][p][Ring(colour == 1).at].astype(F32)
            for n, _ in self._ways():
                total += f[n].astype(F32)
            zs = self.s["zs"][i]
            if self.arrays[i][0] == THIN:
                total = total.reshape(TALL, w)
                for d in range(LINE):
                    zs[d, :, lo : lo + w] = total[THIN * d : THIN * d + THIN].astype(BF)
            else:
                zs[:, :, lo : lo + w] = total.reshape(LINE, -1, w).astype(BF)
        self._line()
        for zs, zr in zip(self.s["zs"], self.s["zr"]):
            zr[slot] = zs[slot]

    def finish(self):
        n = 0
        for i, (r, width, parts) in enumerate(self.arrays):
            zr = self.s["zr"][i]
            self._all_of(i, CAME)
            sums = []
            for core in range(C):
                total = zr[core].astype(F32)
                for k in range(1, Z):
                    total += zr[C * k + core].astype(F32)
                sums.append(total.astype(BF))
            whole = jnp.concatenate(sums, axis=1)
            for first, w in parts or [(0, width)]:
                self.res[n][0] = whole[:, first : first + w]
                n += 1
            self._all_of(i, SENT)
        for stage in ("over", "a", "a2", "b2") if self.in_vmem else ("over", "a", "a2", "b", "b2"):
            for p in range(len(self.pieces)):
                self._done(stage, SENT, p)


QKV = ([(THIN, WIDTH + 2 * HEAD, [(0, WIDTH), (WIDTH, HEAD), (WIDTH + HEAD, HEAD)])], [(0, 0, 256, 0), (0, 256, 256, 1)])
REST = (
    [(THIN, WIDTH, ()), (THIN, HIDDEN_UNITS, ()), (THIN, HIDDEN_UNITS, ()), (8, WIDTH, ())],
    [(1, 0, 1024, 0), (2, 0, 1024, 1), (0, 0, 384, 0), (3, 0, 128, 0), (3, 128, 256, 1)],
)


THETA = 10000
NAMES = ("wq", "wk", "wv", "wo", "w_gate", "w_up", "w_down")
G = 6
TB = 512
NT = 4
MB, MT, FJ, MJ = 1024, 2, 512, 4
BLOCKS = NT * (NT + 1) // 2
NEG = -1e30
HIDDEN = 2 * NEG
LOG2E = 1.4426950408889634
VMEM = 56 * 2**20
EPS = 1e-6


def mm(a, b):
    return lax.dot_general(a, b, (((1,), (0,)), ((), ())), preferred_element_type=F32)


def mm_t(a, b):
    return lax.dot_general(a, b, (((1,), (1,)), ((), ())), preferred_element_type=F32)


def norm(h):
    scale = lax.rsqrt(jnp.mean(h * h, -1, keepdims=True) + EPS)
    return (h * scale).astype(BF), scale


def norm_back(h, g):
    scale = lax.rsqrt(jnp.mean(h * h, -1, keepdims=True) + EPS)
    return scale * (g - h * (scale * scale * jnp.mean(g * h, -1, keepdims=True)))


def turn_table(tokens):
    half = HEAD // 2
    freq = np.float64(THETA) ** (-np.arange(half) / half)
    place = np.concatenate([HEAD * np.arange(tokens // HEAD), np.arange(HEAD)]) * 1.0
    angle = place[:, None] * np.concatenate([freq, freq])
    return jnp.asarray(np.stack([np.cos(angle), np.sin(angle)]).astype(np.float32))


def turner(table, n):
    far, near = pl.ds(n, 1), slice(-HEAD, None)
    fc, fs, nc, ns = table[0, far, :], table[1, far, :], table[0, near, :], table[1, near, :]
    sin = fs * nc + fc * ns
    return fc * nc - fs * ns, jnp.where(lax.broadcasted_iota(jnp.int32, sin.shape, 1) < HEAD // 2, -sin, sin)


def swap(t):
    return pltpu.roll(t, HEAD // 2, 1)


def whole(shape):
    return pl.BlockSpec(shape, lambda *_: (0,) * len(shape))


def stage(n, plan):
    for at, todo in plan.items():

        @pl.when(n == at)
        def _():
            for do in todo:
                do()


def block_of(m):
    i = sum((m >= (r * (r + 1)) // 2).astype(jnp.int32) for r in range(1, NT))
    return i, m - (i * (i + 1)) // 2


def rows(b, size=TB, first=0):
    return pl.ds(pl.multiple_of(b * TB + first, HEAD), size)


def wait(copies):
    for cp in copies:
        cp.wait()


HALVES = ((0, 0), (TB // 2, TB // 2))


def masked(s, key, query):
    return lax.broadcasted_iota(jnp.int32, s.shape, 0) + key <= lax.broadcasted_iota(jnp.int32, s.shape, 1) + query


def _front(x_ref, table_ref, *rest, gq, gr):
    weights, rest = rest[: len(NAMES)], rest[len(NAMES) :]
    hbm, outs, (ours, qkv_s, lse_s, table_s, vt_s, top_s, mix_s, w_s, sems, o_sem, sq, sr) = rest[:6], rest[6:11], rest[11:]
    q_s, k_s, v_s, at_s, o_s, x_s = ours
    n = pl.program_id(0)
    gq.bind(qkv_s, (w_s,), sq, own=weights[:3])
    gr.bind(weights[3:], outs[1:], sr)
    fetch = [pltpu.make_async_copy(a, b, sems.at[len(ours) + m]) for m, (a, b) in enumerate([*zip(weights, qkv_s), (x_ref, x_s), (table_ref, table_s)])]
    lse_out = pltpu.make_async_copy(lse_s, hbm[5], sems.at[5])
    keep = [pltpu.make_async_copy(a, b, sems.at[m]) for m, (a, b) in enumerate(zip((q_s, k_s, v_s, at_s, w_s), (*hbm[:4], outs[0])))]
    o_out = lambda b: pltpu.make_async_copy(o_s.at[:, rows(b)], hbm[4].at[:, rows(b)], o_sem.at[b])

    def normed(first, last):
        for b in range(first, last):
            at = slice(b * TB, b * TB + TB)
            a, _ = norm(x_s[at, :].astype(F32))
            x_s[at, :] = a
            at_s[:, at] = a.T

    def early():
        start(fetch)
        hello()
        wait(fetch)
        normed(0, NT // 2)

    def late():
        normed(NT // 2, NT)

    def keep_all():
        start(keep)

    stage(n, {
        0: [early, meet, gq.down, gr.down, late, gq.lay, gq.near, gq.far, gr.lay, gq.far2, gr.near, gq.over, gq.finish],
        1: [gr.near2],
        NT: [gr.far, keep_all],
        10: [functools.partial(gr.far2, 0, 1)],
        11: [functools.partial(gr.far2, 2, 3, 4)],
        13: [functools.partial(gr.over, 0, 1)],
    })

    @pl.when(n < NT)
    def _():
        a = x_s[rows(n), :]
        y = mm(a, w_s[...].reshape(a.shape[1], -1)).astype(BF)
        for i in range(TB // HEAD):
            here, there = slice(HEAD * i, HEAD * i + HEAD), rows(n, HEAD, HEAD * i)
            cos, sin = turner(table_s, n * (TB // HEAD) + i)
            for h in range(G + 1):
                t = y[here, HEAD * h : HEAD * h + HEAD].astype(F32)
                t = (t * cos + swap(t) * sin).astype(BF)
                if h < G:
                    q_s[h, there, :] = t
                else:
                    k_s[there, :] = t
        v = y[:, (G + 1) * HEAD :]
        v_s[rows(n), :] = v
        vt_s[n] = jnp.concatenate([v.T, jnp.ones((8, TB), BF)], axis=0)

    i, j = block_of(n - NT)
    e = HEAD**-0.5 * LOG2E

    @pl.when((n >= NT) & (j == 0))
    def _():
        top_s[...] = jnp.full(top_s.shape, NEG, F32)
        mix_s[...] = jnp.zeros(mix_s.shape, F32)

    def block(key, keys, query, mask):
        k = k_s[rows(j, keys, key), :]
        scores = [mm_t(k, q_s[h, rows(i, TB - query, query), :]) for h in range(G)]
        weights, keeps = [], []
        for h, s in enumerate(scores):
            if mask:
                s = jnp.where(masked(s, key, query), s, HIDDEN)
            old = top_s[h : h + 1, query:]
            top = jnp.maximum(old, s.max(axis=0, keepdims=True))
            top_s[h : h + 1, query:] = top
            weights.append(jnp.exp2((s - top) * e).astype(BF))
            keeps.append(jnp.exp2((old - top) * e))
        for h in range(G):
            mix_s[h, :, query:] = mix_s[h, :, query:] * keeps[h] + mm(vt_s[j, :, key : key + keys], weights[h])

    @pl.when((n >= NT) & (j < i))
    def _():
        block(0, TB, 0, False)

    @pl.when((n >= NT) & (j == i))
    def _():
        for key, query in HALVES:
            block(key, TB // 2, query, True)
        for h in range(G):
            total = mix_s[h, HEAD : HEAD + 1, :]
            o_s[h, rows(i), :] = (mix_s[h, :HEAD, :] * (1 / total)).T.astype(BF)
            lse_s[h : h + 1, rows(i)] = top_s[h : h + 1, :] * HEAD**-0.5 + jnp.log(total)
        o_out(i).start()

    def finish():
        lse_out.start()
        gr.over(2, 3, 4)
        gr.finish()
        lse_out.wait()
        wait(keep)
        wait([o_out(b) for b in range(NT)])

    stage(n, {NT + BLOCKS - 1: [finish]})


def front(x, table, weights, gq, gr):
    T, D = x.shape
    hbm = pl.BlockSpec(memory_space=pltpu.HBM)
    mine = [(G, T, HEAD), (T, HEAD), (T, HEAD), (D, T), (G, T, HEAD)]
    outs = [jax.ShapeDtypeStruct(s, BF) for s in mine] + [jax.ShapeDtypeStruct((8, T), F32)] + gq.outs() + gr.outs()
    return pl.pallas_call(
        functools.partial(_front, gq=gq, gr=gr),
        grid=(NT + BLOCKS,),
        in_specs=[hbm] * (2 + len(weights)),
        out_specs=[hbm] * len(outs),
        out_shape=outs,
        scratch_shapes=[[pltpu.VMEM(s, BF) for s in (*mine, (T, D))], [pltpu.VMEM(a.shape, BF) for a in weights[:3]], pltpu.VMEM((8, T), F32), pltpu.VMEM(table.shape, F32),
                        pltpu.VMEM((NT, HEAD + 8, TB), BF), pltpu.VMEM((8, TB), F32), pltpu.VMEM((G, HEAD + 8, TB), F32),
                        pltpu.VMEM((X, Y, TALL, 1024), BF), DMA((11,)), DMA((NT,)), gq.scratch(), gr.scratch()],
        compiler_params=pltpu.CompilerParams(dimension_semantics=("arbitrary",), vmem_limit_bytes=VMEM, collective_id=1, has_side_effects=True),
        name="front",
    )(x, table, *weights)


def _back(*refs, sq, sr):
    hbm, then, grads, dx_ref, outs, rest = refs[:5], refs[5:11], refs[11:15], refs[15], refs[16:23], refs[23:]
    ours, more, sems, more_sem, dq_s, dk_s, dv_s, d_s, acc, dw_s, rq, rr = rest
    q_s, do_s, k_s, v_s, at_s = ours
    lse_ref, delta_ref, table_s, w_s, x_s, dh_s = more
    n = pl.program_id(0)
    sq.bind((dw_s,), outs[:3], rq)
    sr.bind(grads, outs[3:], rr)

    def fetch(b):
        at = [(ALL, rows(b)), (ALL, rows(b)), (rows(b),), (rows(b),), (ALL, rows(b))]
        return [pltpu.make_async_copy(src.at[a], dst.at[a], sems.at[m, b]) for m, (src, dst, a) in enumerate(zip(hbm, ours, at))]

    whole_ones = [pltpu.make_async_copy(src, dst, more_sem.at[m]) for m, (src, dst) in enumerate(zip(then, more))]

    def fetch_first():
        start(whole_ones[:3] + fetch(0))

    def fetch_more():
        for b in range(1, NT):
            start(fetch(b))

    def fetch_last():
        start(whole_ones[3:])

    def rest_here():
        wait(whole_ones[3:])

    i, j = block_of(n)
    stage(n, {0: [fetch_first, hello]})

    @pl.when((n < BLOCKS) & (j == 0))
    def _():
        wait(fetch(i))

        @pl.when(n == 0)
        def _():
            wait(whole_ones[:3])
            fetch_more()

    stage(n, {1: [meet, sr.down], 3: [fetch_last, sr.near], 5: [sr.near2], 8: [functools.partial(sr.far, 0, 1)], 9: [functools.partial(sr.far, 2, 3, 4), functools.partial(sr.far2, 0, 1)]})
    scale = HEAD**-0.5
    e = scale * LOG2E

    @pl.when(n == 0)
    def _():
        dk_s[...] = jnp.zeros_like(dk_s)
        dv_s[...] = jnp.zeros_like(dv_s)
        acc[...] = jnp.zeros_like(acc)

    @pl.when((n < BLOCKS) & (j == 0))
    def _():
        dq_s[...] = jnp.zeros_like(dq_s)

    def block(key, keys, query, mask):
        here, there = rows(j, keys, key), rows(i, TB - query, query)
        k, v = k_s[here, :], v_s[here, :]
        kt = k.T
        qs = [q_s[h, there, :] for h in range(G)]
        dos = [do_s[h, there, :] for h in range(G)]
        scores = [mm_t(k, q) for q in qs]
        dps = [mm_t(v, do) for do in dos]
        for h in range(G):
            p = jnp.exp2(scores[h] * e - lse_ref[h : h + 1, there] * LOG2E)
            if mask:
                p = jnp.where(masked(p, key, query), p, 0.0)
            ds = (p * (dps[h] - delta_ref[h : h + 1, there])).astype(BF)
            dv_s[j, key : key + keys] += mm(p.astype(BF), dos[h])
            dk_s[j, key : key + keys] += mm(ds, qs[h])
            dq_s[h, :, query:] += mm(kt, ds)

    def turn_back(t, b, r):
        cos, sin = turner(table_s, b * (TB // HEAD) + r)
        t = t[HEAD * r : HEAD * r + HEAD].astype(F32)
        return (t * cos - swap(t) * sin).astype(BF)

    @pl.when((n < BLOCKS) & (j < i))
    def _():
        block(0, TB, 0, False)

    @pl.when((n < BLOCKS) & (j == i))
    def _():
        for key, query in HALVES:
            block(key, TB // 2, query, True)

    stage(n, {BLOCKS - 1: [functools.partial(sr.far2, 2, 3, 4)]})

    @pl.when((n < BLOCKS) & (j == i))
    def _():
        for h in range(G):
            dq = (dq_s[h] * scale).T.astype(BF)
            for r in range(TB // HEAD):
                d_s[i, HEAD * r : HEAD * r + HEAD, HEAD * h : HEAD * h + HEAD] = turn_back(dq, i, r)
        acc[:, : G * HEAD] += mm(at_s[:, rows(i)], d_s[i, :, : G * HEAD])

    def last():
        for b in range(NT):
            dk = (dk_s[b] * scale).astype(BF)
            for r in range(TB // HEAD):
                d_s[b, HEAD * r : HEAD * r + HEAD, G * HEAD : (G + 1) * HEAD] = turn_back(dk, b, r)
            d_s[b, :, (G + 1) * HEAD :] = dv_s[b].astype(BF)
            acc[:, G * HEAD :] += mm(at_s[:, rows(b)], d_s[b, :, G * HEAD :])
        dw_s[...] = acc[...].astype(BF).reshape(dw_s.shape)

    stage(n, {BLOCKS: [last, sq.down, rest_here], BLOCKS + 1: [sq.near, sr.line], BLOCKS + 2: [sq.near2], BLOCKS + 3: [sq.far]})

    @pl.when(n >= BLOCKS)
    def _():
        da = mm_t(d_s[n - BLOCKS], w_s[...])
        at = rows(n - BLOCKS)
        dx_ref[...] = (dh_s[at, :].astype(F32) + norm_back(x_s[at, :].astype(F32), da)).astype(BF)

    stage(n, {BLOCKS + NT - 1: [sq.line, sr.finish, sq.finish]})


def back(q, k, v, do, lse, delta, at, x, dh, w, table, grads, sq, sr):
    T, D = x.shape
    hbm = pl.BlockSpec(memory_space=pltpu.HBM)
    outs = sq.outs() + sr.outs()
    ins, then = (q, do, k, v, at), (lse, delta, table, w, x, dh)
    return pl.pallas_call(
        functools.partial(_back, sq=sq, sr=sr),
        grid=(BLOCKS + NT,),
        in_specs=[hbm] * (len(ins) + len(then) + len(grads)),
        out_specs=[pl.BlockSpec((TB, D), lambda n: (jnp.maximum(n - BLOCKS, 0), 0))] + [whole(o.shape) for o in outs],
        out_shape=[jax.ShapeDtypeStruct((T, D), BF)] + outs,
        scratch_shapes=[[pltpu.VMEM(a.shape, BF) for a in ins], [pltpu.VMEM(a.shape, a.dtype) for a in then], DMA((len(ins), NT)), DMA((len(then),)),
                        pltpu.VMEM((G, HEAD, TB), F32), pltpu.VMEM((NT, TB, HEAD), F32), pltpu.VMEM((NT, TB, HEAD), F32),
                        pltpu.VMEM((NT, TB, 1024), BF), pltpu.VMEM(w.shape, F32), pltpu.VMEM((X, Y, THIN, LINE, 1024), BF), sq.scratch(), sr.scratch()],
        compiler_params=pltpu.CompilerParams(dimension_semantics=("arbitrary",), vmem_limit_bytes=63 * 2**20, collective_id=2, has_side_effects=True),
        name="back",
    )(*ins, *then, *grads)


def _middle(x_ref, o_ref, wo_ref, dy_hbm, wg_hbm, wu_hbm, wd_hbm, dh_ref, do_ref, delta_ref, dwo_ref, dwg_hbm, dwu_hbm, dwd_hbm,
            h_s, b_s, bt_s, db_s, dy_s, wg_s, wu_s, wd_s, ao, ag, au, ad, tg, tu, td, dy_sem, in_sem, out_sem):
    n = pl.program_id(0)
    m = n - NT
    j, t = m // MT, lax.rem(m, MT)
    is_main = (m >= 0) & (m < MJ * MT)
    dy_in = pltpu.make_async_copy(dy_hbm, dy_s, dy_sem)

    def chunk(j):
        at, to = cols(j * FJ, FJ), lax.rem(j, 2)
        pairs = [(wg_hbm.at[:, at], wg_s), (wu_hbm.at[:, at], wu_s), (wd_hbm.at[at, :], wd_s)]
        return [pltpu.make_async_copy(src, dst.at[to], in_sem.at[i, to]) for i, (src, dst) in enumerate(pairs)]

    def grads(j):
        at = cols(j * FJ, FJ)
        pairs = [(tg, dwg_hbm.at[:, at]), (tu, dwu_hbm.at[:, at]), (td, dwd_hbm.at[at, :])]
        return [pltpu.make_async_copy(src, dst, out_sem.at[i]) for i, (src, dst) in enumerate(pairs)]

    @pl.when(n == 0)
    def _():
        start(chunk(0))
        dy_in.start()

    @pl.when(n < NT)
    def _():
        o = jnp.concatenate([o_ref[h] for h in range(G)], axis=1)
        h = (x_ref[...].astype(F32) + mm(o, wo_ref[...]).astype(BF).astype(F32)).astype(BF)
        h_s[rows(n), :] = h
        b, _ = norm(h.astype(F32))
        b_s[rows(n), :] = b
        bt_s[:, rows(n)] = b.T
        db_s[rows(n), :] = jnp.zeros((TB, db_s.shape[1]), F32)

    @pl.when(m == 0)
    def _():
        dy_in.wait()

    @pl.when(is_main & (t == 0))
    def _():
        wait(chunk(j))
        ag[...] = jnp.zeros_like(ag)
        au[...] = jnp.zeros_like(au)
        ad[...] = jnp.zeros_like(ad)

        @pl.when(j + 1 < MJ)
        def _():
            start(chunk(j + 1))

    @pl.when(is_main)
    def _():
        these, slot = pl.ds(pl.multiple_of(t * MB, MB), MB), lax.rem(j, 2)
        b, bt, dy = b_s[these, :], bt_s[:, these], dy_s[these, :]

        def into(c):
            return mm(b, wg_s[slot, :, c]), mm(b, wu_s[slot, :, c]), mm_t(dy, wd_s[slot, c, :])

        def point(gate, up, dact):
            dact = dact.astype(BF).astype(F32)
            sig = 0.5 + 0.5 * jnp.tanh(0.5 * gate)
            silu = gate * sig
            return (silu * up).astype(BF), (dact * up * (sig + silu * (1 - sig))).astype(BF), (dact * silu).astype(BF)

        strips = [slice(a, a + 256) for a in range(0, FJ, 256)]
        ahead, dbs = into(strips[0]), []
        for i, c in enumerate(strips):
            now, ahead = ahead, into(strips[i + 1]) if i + 1 < len(strips) else ()
            act, dgate, dup = point(*now)
            dbs.append(mm_t(dgate, wg_s[slot, :, c]) + mm_t(dup, wu_s[slot, :, c]))
            ag[:, c] += mm(bt, dgate)
            au[:, c] += mm(bt, dup)
            ad[c, :] += mm(act.T, dy)
        db_s[these, :] += sum(dbs[1:], dbs[0])

        @pl.when(t == MT - 1)
        def _():
            @pl.when(j > 0)
            def _():
                wait(grads(j - 1))

            tg[...] = ag[...].astype(BF)
            tu[...] = au[...].astype(BF)
            td[...] = ad[...].astype(BF)
            start(grads(j))

    last = m - MJ * MT

    @pl.when(last == 0)
    def _():
        ao[...] = jnp.zeros_like(ao)

    @pl.when(last >= 0)
    def _():
        at = rows(jnp.maximum(last, 0))
        dh = (dy_s[at, :].astype(F32) + norm_back(h_s[at, :].astype(F32), db_s[at, :]).astype(BF).astype(F32)).astype(BF)
        dh_ref[...] = dh
        do = mm_t(dh, wo_ref[...]).astype(BF)
        o = jnp.concatenate([o_ref[h] for h in range(G)], axis=1)
        prod = do.astype(F32) * o.astype(F32)
        for h in range(G):
            do_ref[h] = do[:, HEAD * h : HEAD * h + HEAD]
        delta_ref[...] = jnp.concatenate([prod[:, HEAD * h : HEAD * h + HEAD].sum(-1, keepdims=True) for h in range(G)]
                                         + [jnp.zeros((TB, 8 - G), F32)], axis=1).T
        ao[...] += mm(o.T, dh)

    @pl.when(last == NT - 1)
    def _():
        dwo_ref[...] = ao[...].astype(BF)
        wait(grads(MJ - 1))


def middle(x, dy, o, wo, wg, wu, wd):
    T, D = x.shape
    end = NT + MJ * MT
    late = lambda n: jnp.maximum(n - end, 0)
    ends = lambda n: jnp.where(n < NT, n, jnp.where(n < end, NT - 1, n - end))
    once = pl.BlockSpec(wo.shape, lambda n: (0, 0), pipeline_mode=pl.Buffered(1))
    hbm = pl.BlockSpec(memory_space=pltpu.HBM)
    buf = lambda *s, dtype=BF: pltpu.VMEM(s, dtype)
    return pl.pallas_call(
        _middle,
        grid=(end + NT,),
        in_specs=[pl.BlockSpec((TB, D), lambda n: (jnp.minimum(n, NT - 1), 0)), pl.BlockSpec((G, TB, HEAD), lambda n: (0, ends(n), 0)), once,
                  hbm, hbm, hbm, hbm],
        out_specs=[pl.BlockSpec((TB, D), lambda n: (late(n), 0)), pl.BlockSpec((G, TB, HEAD), lambda n: (0, late(n), 0)),
                   pl.BlockSpec((8, TB), lambda n: (0, late(n))), once, hbm, hbm, hbm],
        out_shape=[jax.ShapeDtypeStruct((T, D), BF), jax.ShapeDtypeStruct((G, T, HEAD), BF), jax.ShapeDtypeStruct((8, T), F32),
                   *(jax.ShapeDtypeStruct(a.shape, BF) for a in (wo, wg, wu, wd))],
        scratch_shapes=[buf(T, D), buf(T, D), buf(D, T), buf(T, D, dtype=F32), buf(T, D), buf(2, D, FJ), buf(2, D, FJ), buf(2, FJ, D),
                        buf(D, D, dtype=F32), buf(D, FJ, dtype=F32), buf(D, FJ, dtype=F32), buf(FJ, D, dtype=F32), buf(D, FJ), buf(D, FJ), buf(FJ, D),
                        DMA(()), DMA((3, 2)), DMA((3,))],
        compiler_params=pltpu.CompilerParams(dimension_semantics=("arbitrary",), vmem_limit_bytes=67043328), name="middle",
    )(x, o, wo, dy, wg, wu, wd)


def _hand_over(*refs):
    *ends, bufs, big, sems = refs
    srcs, dsts = ends[: len(bufs)], ends[len(bufs) :]

    def pairs(src, dst, buf, sem):
        return pltpu.make_async_copy(src, buf, sem.at[0]), pltpu.make_async_copy(buf, dst, sem.at[1])

    copies = [pairs(s, d, b, sems.at[m]) for m, (s, d, b) in enumerate(zip(srcs, dsts, bufs))]
    some = [pl.ds(i * MB // NT, MB // NT) for i in range(srcs[0].shape[1] * NT // MB)]
    copies = [pairs(srcs[0].at[:, at], dsts[0].at[:, at], bufs[0].at[:, at], big.at[m]) for m, at in enumerate(some)] + copies[1:]
    start([get for get, _ in copies])
    for get, put in copies:
        get.wait()
        put.start()
    wait([put for _, put in copies])


def hand_over(results):
    hbm, n = pl.BlockSpec(memory_space=pltpu.HBM), len(results)
    return pl.pallas_call(
        _hand_over, in_specs=[hbm] * n, out_specs=[hbm] * n, out_shape=[jax.ShapeDtypeStruct(a.shape, BF) for a in results],
        scratch_shapes=[[pltpu.VMEM(a.shape, BF) for a in results], DMA((NT * NT, 2)), DMA((n, 2))],
        compiler_params=pltpu.CompilerParams(vmem_limit_bytes=VMEM), name="hand_over",
    )(*results)


def solution(mesh):
    gq, gr, sq, sr = Gather(*QKV, in_vmem=True), Gather(*REST), Scatter(*QKV, in_vmem=True), Scatter(*REST)

    def step(x, dy, *weights):
        x, dy = x[0], dy[0]
        T, D = x.shape
        table = turn_table(T)
        q, k, v, at, o, lse, w, *rest = front(x, table, weights, gq, gr)
        rest = [a.reshape(D, -1) for a in rest[:3]] + [rest[3].reshape(-1, D)]
        dh, do, delta, *grads = middle(x, dy, o, *rest)
        grads = [g.reshape(X, Y, -1, LINE, g.shape[1]) for g in grads]
        dx, *by_w = back(q, k, v, do, lse, delta, at, x, dh, w.reshape(D, -1), table, grads, sq, sr)
        return hand_over([dx[None], *by_w])

    states, cut = P(("rep", "dp"), None, None), P(None, "dp", None)
    return jax.shard_map(
        step,
        mesh=mesh,
        in_specs=(states, states) + (cut,) * 7,
        out_specs=(states,) + (P("rep", "dp", None),) * 7,
        check_vma=False,
    )
```
